128 devices in a mesh: py: 16 (over y, x_hi, core), px: 8 (over z, x_lo).
Axes of the slice: x: 4 (x_hi: 2, x_lo: 2; x = x_hi * 2 + x_lo), y: 4, z: 4, core: 2. Of those that a mesh axis runs over, the one named last changes fastest.
Arguments:
- load_terms: float32 [1024, 512, 256], P('py', 'px'), may hold values from -6 to 6
- start_values: float32 [1024, 512, 256], P('py', 'px'), may hold values from -6 to 6
- reaction_rate: float32 [1024, 512, 256], P('py', 'px'), may hold values from 0.1 to 0.9
Outputs:
- corrected: float32 [1024, 512, 256], P('py', 'px')
The draws below stay inside these ranges and needn't reach their ends.
All inputs are finite; a program needn't handle non-finite values.
Results may differ from the reference program's by a relative error of at most 0.00002.
Values sent between devices are 32-bit elements; how exact they have to be, the bound alone decides.
No kernel may reach another device: no remote copies, remote signals or barrier semaphores. Data moves between devices by JAX's collectives and lax.ppermute only.
A program may use at most 128 MiB of HBM per device.

```python
import jax
import jax.numpy as jnp
from jax import lax

MEMBERS = 256
RATIO = 4
BEFORE = 2
AFTER = 2
INNER = 7
GRID_Y = 1024
GRID_X = 512


def shard_levels(stream_key, extent, shards, smallest, high):
    gain = 1.0
    for axis_at, blocks in shards:
        steps = jax.random.uniform(jax.random.fold_in(jax.random.fold_in(stream_key, 6), axis_at), (blocks,), jnp.float32, smallest / len(shards), high / len(shards))
        gain = gain * jnp.repeat(jnp.exp(steps), extent[axis_at] // blocks).reshape((-1,) + (1,) * (len(extent) - 1 - axis_at))
    return gain


def normal_values(stream_key, dims, width, limit, shards=(), kind=jnp.bfloat16):
    gain = shard_levels(stream_key, dims, shards, -0.22, 0.18) if shards else 1.0
    entries = jax.random.normal(stream_key, dims, jnp.float32) * width * gain
    return jnp.minimum(jnp.maximum(entries, -limit), limit).astype(kind)


def setup_inputs(seed: int = 0) -> dict:
    arg_keys = jax.random.split(jax.random.key(seed), 4)
    return {
        "load_terms": normal_values(arg_keys[0], (GRID_Y, GRID_X, MEMBERS), 1.0, 6.0, ((0, 16), (1, 8)), jnp.float32),
        "start_values": normal_values(arg_keys[1], (GRID_Y, GRID_X, MEMBERS), 1.0, 6.0, ((0, 16), (1, 8)), jnp.float32),
        "reaction_rate": jnp.clip(0.1 + 0.79999997 * jax.random.uniform(arg_keys[2], (GRID_Y, GRID_X, MEMBERS), jnp.float32) ** shard_levels(arg_keys[2], (GRID_Y, GRID_X, MEMBERS), ((0, 16), (1, 8)), -0.2, 0.2), 0.1, 0.9),
    }


def around_sum(padded):
    inner_y, inner_x = padded.shape[0] - 2, padded.shape[1] - 2
    middle_rows = lax.slice_in_dim(padded, 1, 1 + inner_y, axis=0)
    middle_columns = lax.slice_in_dim(padded, 1, 1 + inner_x, axis=1)
    return (lax.slice_in_dim(middle_columns, 0, inner_y, axis=0) + lax.slice_in_dim(middle_columns, 2, 2 + inner_y, axis=0)
            + lax.slice_in_dim(middle_rows, 0, inner_x, axis=1) + lax.slice_in_dim(middle_rows, 2, 2 + inner_x, axis=1))


def relax_once(padded, values, load, mass_here):
    return values + 0.8 * (load + around_sum(padded) - (4.0 + mass_here) * values) / (4.0 + mass_here)


def block_means(values):
    cut = values.reshape(values.shape[0] // RATIO, RATIO, values.shape[1] // RATIO, RATIO, values.shape[2])
    return jnp.mean(cut, axis=(1, 3))


def spread_blocks(values):
    return jnp.repeat(jnp.repeat(values, RATIO, axis=0), RATIO, axis=1)


def reference(load_terms, start_values, reaction_rate):
    values = start_values
    for sweep in range(BEFORE):
        values = relax_once(jnp.pad(values, ((1, 1), (1, 1), (0, 0)), mode="wrap"), values, load_terms, reaction_rate)
    defect = load_terms + around_sum(jnp.pad(values, ((1, 1), (1, 1), (0, 0)), mode="wrap")) - (4.0 + reaction_rate) * values
    coarse_load, coarse_mass = block_means(defect) * RATIO, block_means(reaction_rate) * RATIO
    coarse_values = jnp.zeros_like(coarse_load)
    for sweep in range(INNER):
        coarse_values = relax_once(jnp.pad(coarse_values, ((1, 1), (1, 1), (0, 0)), mode="wrap"), coarse_values, coarse_load, coarse_mass)
    values = values + spread_blocks(coarse_values)
    for sweep in range(AFTER):
        values = relax_once(jnp.pad(values, ((1, 1), (1, 1), (0, 0)), mode="wrap"), values, load_terms, reaction_rate)
    corrected = values
    return corrected
```

```python
import jax
import jax.numpy as jnp
from jax import lax
from jax.experimental import pallas as pl
from jax.experimental.pallas import tpu as pltpu
from jax.sharding import PartitionSpec as P

F = jnp.float32
T = 64
R = 4
NB = T // R
INNER = 7
DEPTH = INNER
LANES = 128
HALVES = 2
PR, PC = T + 2, T + 16
PLANE = PR * PC
CW = 32
CR = NB + 2 * DEPTH
QX = 2 * DEPTH * NB + 2 * T + 16
QY = 2 * DEPTH * CW + CW + 2 * T + 8
QX_U2, QX_D, QX_S = 2 * DEPTH * NB, 2 * DEPTH * NB + T, 2 * DEPTH * NB + 2 * T
QY_M, QY_S = DEPTH * CW, 2 * DEPTH * CW
QY_U2, QY_D, QY_DIAG = QY_S + CW, QY_S + CW + T, QY_S + CW + 2 * T
MIB = 2**20


def at(refs, *names):
    return [refs[n] for n in names]


def rows(start, size, stride=1):
    return pl.ds(start, size, stride=stride)


def mid():
    return pl.ds(8, T)


def left():
    return pl.ds(7, T)


def right():
    return pl.ds(9, T)


def around(ref, h, y):
    return (ref[h, y, mid(), :] + ref[h, y + 2, mid(), :]) + (
        ref[h, y + 1, left(), :] + ref[h, y + 1, right(), :]
    )


def each_row(body, n=T, unroll=2):
    for h in range(HALVES):
        lax.fori_loop(0, n, lambda y, c, h=h: (body(h, y), c)[1], 0, unroll=unroll)


def clear_border(ref):
    for h in range(HALVES):
        ref[h, 0] = jnp.zeros((PC, LANES), F)
        ref[h, PR - 1] = jnp.zeros((PC, LANES), F)
        for x in (0, PC - 8):
            ref[h, pl.ds(1, T), pl.ds(x, 8), :] = jnp.zeros((T, 8, LANES), F)


def column(ref2, h, x):
    return rows(h * PLANE + PC + 8 + x, T, PC)


def block_sums(part, out):
    n = HALVES * NB * NB

    def body(j, c):
        total = part[rows(j * 4 * T, T, R), :]
        for k in range(1, R):
            total = total + part[rows(j * 4 * T + k, T, R), :]
        out[pl.ds(j * T, T), :] = total * (1.0 / R)
        return c

    lax.fori_loop(0, n // T, body, 0)


def first_kernel(load_h, u_h, m_h, pxl, pxh, pyl, pyh, u1p, b, ld, m, mo, up, part, sems):
    copies = []
    for h in range(HALVES):
        lanes = pl.ds(h * LANES, LANES)
        copies.append(pltpu.make_async_copy(m_h.at[:, :, lanes], m.at[h], sems.at[0, h]))
        copies.append(
            pltpu.make_async_copy(u_h.at[:, :, lanes], up.at[h, pl.ds(1, T), pl.ds(8, T), :], sems.at[1, h])
        )
        copies.append(pltpu.make_async_copy(load_h.at[:, :, lanes], ld.at[h], sems.at[2, h]))
    for c in copies:
        c.start()
    clear_border(up)
    for c in copies:
        c.wait()

    def sweep(h, y):
        bb = 0.8 / (4.0 + m[h, y])
        b[h, y] = bb
        u1p[h, y + 1, mid(), :] = 0.2 * up[h, y + 1, mid(), :] + bb * (ld[h, y] + around(up, h, y))

    each_row(sweep)

    def sums(h, y):
        part[pl.ds(pl.multiple_of((h * NB + y) * T, T), T), :] = (m[h, R * y] + m[h, R * y + 1]) + (
            m[h, R * y + 2] + m[h, R * y + 3]
        )

    each_row(sums, NB)
    block_sums(part, mo)

    up2, u1p2, b2 = up.reshape(HALVES * PLANE, LANES), u1p.reshape(HALVES * PLANE, LANES), b.reshape(
        HALVES * T * T, LANES
    )
    for h in range(HALVES):
        for x, p in ((0, pxl), (T - 1, pxh)):
            p[h, pl.ds(0, T), :] = up2[column(up2, h, x), :]
            p[h, pl.ds(T, T), :] = u1p2[column(u1p2, h, x), :]
            p[h, pl.ds(2 * T, T), :] = b2[rows(h * T * T + x, T, T), :]
        for y, p in ((0, pyl), (T - 1, pyh)):
            p[h, pl.ds(0, T), :] = up[h, y + 1, mid(), :]
            p[h, pl.ds(T, T), :] = u1p[h, y + 1, mid(), :]
            p[h, pl.ds(2 * T, T), :] = b[h, y]


def second_kernel(u1p_in, b, ld, m, mo, pxl, pxh, pyl, pyh, hxl, hxh, hyl, hyh, u1p, u2p, lp, qxl, qxh, part):
    del u1p_in
    u1p2 = u1p.reshape(HALVES * PLANE, LANES)
    U, A, B = pl.ds(0, T), pl.ds(T, T), pl.ds(2 * T, T)
    clear_border(u2p)
    for h in range(HALVES):
        for x, p, g in ((0, pxl, hxl), (T - 1, pxh, hxh)):
            inner = column(u1p2, h, x)
            outer = column(u1p2, h, -1 if x == 0 else T)
            u1p2[inner, :] = u1p2[inner, :] + p[h, B, :] * g[h, U, :]
            u1p2[outer, :] = g[h, A, :] + g[h, B, :] * p[h, U, :]
        for y, p, g in ((0, pyl, hyl), (T - 1, pyh, hyh)):
            u1p[h, y + 1, mid(), :] = u1p[h, y + 1, mid(), :] + p[h, B, :] * g[h, U, :]
            u1p[h, 0 if y == 0 else T + 1, mid(), :] = g[h, A, :] + g[h, B, :] * p[h, U, :]

    def sweep(h, y):
        u2p[h, y + 1, mid(), :] = 0.2 * u1p[h, y + 1, mid(), :] + b[h, y] * (ld[h, y] + around(u1p, h, y))

    each_row(sweep)

    def sums(h, y):
        total = None
        for k in range(R):
            c = R * y + k
            d = (ld[h, c] + around(u2p, h, c)) - (4.0 + m[h, c]) * u2p[h, c + 1, mid(), :]
            total = d if total is None else total + d
        part[pl.ds(pl.multiple_of((h * NB + y) * T, T), T), :] = total

    each_row(sums, NB, unroll=1)
    block_sums(part, lp)

    u2p2, ld2 = u2p.reshape(HALVES * PLANE, LANES), ld.reshape(HALVES * T * T, LANES)
    for h in range(HALVES):
        for x, first, s, q in ((0, 0, 0, qxl), (T - 1, NB - DEPTH, 8, qxh)):
            for k in range(DEPTH):
                q[h, pl.ds(k * NB, NB), :] = lp[rows(h * NB * NB + first + k, NB, NB), :]
                q[h, pl.ds((DEPTH + k) * NB, NB), :] = mo[rows(h * NB * NB + first + k, NB, NB), :]
            q[h, pl.ds(QX_U2, T), :] = u2p2[column(u2p2, h, x), :]
            q[h, pl.ds(QX_D, T), :] = (
                ld2[rows(h * T * T + x, T, T), :] + u2p2[column(u2p2, h, 1 if x == 0 else T - 2), :]
            )
            for i, y in enumerate((0, T - 1)):
                total = None
                for k in range(R):
                    v = u2p2[rows(h * PLANE + (y + 1) * PC + 8 + R * s + k, 8, R), :]
                    total = v if total is None else total + v
                q[h, pl.ds(QX_S + 8 * i, 8), :] = total


def third_kernel(lp, mo, u2p, ld, qxl, qxh, gxl, gxh, hxl, hxh, lx, mx, s0, s1, qyl, qyh):
    lx2, mx2 = lx.reshape(HALVES * NB * CW, LANES), mx.reshape(HALVES * NB * CW, LANES)
    flat = lambda r: r.reshape(HALVES * QX, LANES)
    qxl2, qxh2, gxl2, gxh2 = flat(qxl), flat(qxh), flat(gxl), flat(gxh)

    def quarter(ref, h):
        total = ref[rows(h * QX + QX_U2, NB, R), :]
        for k in range(1, R):
            total = total + ref[rows(h * QX + QX_U2 + k, NB, R), :]
        return total * (1.0 / R)

    for h in range(HALVES):
        col = lambda c: rows(h * NB * CW + c, NB, CW)
        for y in range(NB):
            lx[h, y, pl.ds(8, NB), :] = lp[pl.ds(h * NB * NB + y * NB, NB), :]
            mx[h, y, pl.ds(8, NB), :] = mo[pl.ds(h * NB * NB + y * NB, NB), :]
        for c in (0, CW - 1):
            lx2[col(c), :] = jnp.zeros((NB, LANES), F)
            mx2[col(c), :] = jnp.zeros((NB, LANES), F)
        for c, g in ((1, gxl), (8 + NB, gxh)):
            for k in range(DEPTH):
                lx2[col(c + k), :] = g[h, pl.ds(k * NB, NB), :]
                mx2[col(c + k), :] = g[h, pl.ds((DEPTH + k) * NB, NB), :]
        for c, ref in ((8, gxl2), (7, qxl2), (7 + NB, gxh2), (8 + NB, qxh2)):
            lx2[col(c), :] = lx2[col(c), :] + quarter(ref, h)
        for i, s in enumerate((s0, s1)):
            for c, ref in ((0, gxl), (8, qxl), (16, qxh), (24, gxh)):
                s[h, pl.ds(c, 8), :] = ref[h, pl.ds(QX_S + 8 * i, 8), :]
        for y, first, inside, s, q in ((0, 0, 1, s0, qyl), (T - 1, NB - DEPTH, T - 2, s1, qyh)):
            for k in range(DEPTH):
                q[h, pl.ds(k * CW, CW), :] = lx[h, first + k]
                q[h, pl.ds(QY_M + k * CW, CW), :] = mx[h, first + k]
            q[h, pl.ds(QY_S, CW), :] = s[h]
            q[h, pl.ds(QY_U2, T), :] = u2p[h, y + 1, mid(), :]
            q[h, pl.ds(QY_D, T), :] = ld[h, y] + u2p[h, inside + 1, mid(), :]
            for j, (g1, g2) in enumerate(((hxl, gxl), (hxh, gxh))):
                q[h, pl.ds(QY_DIAG + 3 * j, 1), :] = g1[h, pl.ds(y, 1), :]
                q[h, pl.ds(QY_DIAG + 3 * j + 1, 1), :] = g1[h, pl.ds(2 * T + y, 1), :]
                q[h, pl.ds(QY_DIAG + 3 * j + 2, 1), :] = g2[h, pl.ds(QX_U2 + y, 1), :]
            q[h, pl.ds(QY_DIAG + 6, 2), :] = jnp.zeros((2, LANES), F)


def last_kernel(
    lx, mx, s0, s1, gyl, gyh, gxl, gxh, hxl, hxh, hyl, hyh, pxl, pxh, u2p, b, ld,
    out, lg, bc, ca, cb, sp, w0, w1, wh, sh, sems,
):
    one = lambda r: pl.ds(r, 1)
    for h in range(HALVES):
        for k in range(DEPTH):
            for base, g in ((0, gyl), (DEPTH + NB, gyh)):
                lg[h, base + k] = g[h, pl.ds(k * CW, CW), :]
                bc[h, base + k] = 0.8 / (4.0 + g[h, pl.ds(QY_M + k * CW, CW), :])
        for y in range(NB):
            lg[h, DEPTH + y] = lx[h, y]
            bc[h, DEPTH + y] = 0.8 / (4.0 + mx[h, y])
        quarter = 1.0 / R
        for r, v in (
            (DEPTH - 1, s0[h]),
            (DEPTH, gyl[h, pl.ds(QY_S, CW), :]),
            (DEPTH + NB - 1, gyh[h, pl.ds(QY_S, CW), :]),
            (DEPTH + NB, s1[h]),
        ):
            lg[h, r] = lg[h, r] + quarter * v

    bumps = {}
    for h in range(HALVES):
        for j, (px, hx) in enumerate(((pxl, hxl), (pxh, hxh))):
            for i, (hy, gy) in enumerate(((hyl, gyl), (hyh, gyh))):
                y, x = (0, T - 1)[i], (0, T - 1)[j]
                ua, ba = px[h, one(y), :], px[h, one(2 * T + y), :]
                ux, bx = hx[h, one(y), :], hx[h, one(2 * T + y), :]
                uy, by = hy[h, one(x), :], hy[h, one(2 * T + x), :]
                ud, bd = gy[h, one(QY_DIAG + 3 * j), :], gy[h, one(QY_DIAG + 3 * j + 1), :]
                ea, ed = ba * (bx + by) * ud, bd * (bx + by) * ua
                ex, ey = bx * (ba + bd) * uy, by * (ba + bd) * ux
                ya, yo = (DEPTH, DEPTH - 1) if i == 0 else (DEPTH + NB - 1, DEPTH + NB)
                xa, xo = (8, 7) if j == 0 else (7 + NB, 8 + NB)
                for yy, xx, e, bb, e1, e2 in (
                    (ya, xa, ea, ba, ex, ey),
                    (ya, xo, ex, bx, ea, ed),
                    (yo, xa, ey, by, ea, ed),
                    (yo, xo, ed, bd, ex, ey),
                ):
                    lg[h, yy, one(xx), :] = lg[h, yy, one(xx), :] + quarter * (
                        (2.0 - 0.8 / bb) * e + (e1 + e2)
                    )
                bumps[h, i, j] = (ea, ex, ey, ed + gy[h, one(QY_DIAG + 3 * j + 2), :])

    def start(h, y):
        v = bc[h, y] * lg[h, y]
        lg[h, y] = v
        ca[h, y] = v

    each_row(start, CR)
    old, new = ca, cb
    for s in range(1, INNER):

        def inner(h, i, old=old, new=new, s=s):
            y = i + s
            c = old[h, y]
            around_c = (old[h, y - 1] + old[h, y + 1]) + (pltpu.roll(c, 1, 0) + pltpu.roll(c, CW - 1, 0))
            new[h, y] = (0.2 * c + lg[h, y]) + bc[h, y] * around_c

        each_row(inner, CR - 2 * s)
        old, new = new, old
    cv = old
    cv2 = cv.reshape(HALVES * CR * CW, LANES)

    def correct(h, y):
        base = pl.multiple_of((h * NB + y) * T, T)
        c = cv[h, y + DEPTH, pl.ds(8, NB), :]
        for k in range(R):
            sp[rows(base + k, NB, R), :] = c
        add = sp[pl.ds(base, T), :]
        for k in range(R):
            w0[h, R * y + k + 1, mid(), :] = u2p[h, R * y + k + 1, mid(), :] + add

    each_row(correct, NB)

    w02, w12 = w0.reshape(HALVES * PLANE, LANES), w1.reshape(HALVES * PLANE, LANES)
    for h in range(HALVES):
        for i in range(2):
            for j in range(2):
                r, x = (1, T)[i], (8, T + 7)[j]
                w0[h, r, one(x), :] = w0[h, r, one(x), :] + bumps[h, i, j][0]
    U2X, DX, U2Y, DY, BH = pl.ds(QX_U2, T), pl.ds(QX_D, T), pl.ds(QY_U2, T), pl.ds(QY_D, T), pl.ds(2 * T, T)
    n = 0
    for h in range(HALVES):
        diag = {}
        for i in range(2):
            for j in range(2):
                diag[i, j] = (
                    bumps[h, i, j][3] + cv[h, (DEPTH - 1, DEPTH + NB)[i], one((7, 8 + NB)[j]), :]
                )
        for j, (g, hx) in enumerate(((gxl, hxl), (gxh, hxh))):
            c = cv2[rows(h * CR * CW + DEPTH * CW + (7, 8 + NB)[j], NB, CW), :]
            for k in range(R):
                sh[n, rows(k, NB, R), :] = c
            add = sh[n]
            wh[n, mid(), :] = g[h, U2X, :] + add
            wh[n, one(7), :], wh[n, one(8 + T), :] = diag[0, j], diag[1, j]
            wh[n, one(8), :] = wh[n, one(8), :] + bumps[h, 0, j][1]
            wh[n, one(7 + T), :] = wh[n, one(7 + T), :] + bumps[h, 1, j][1]
            v = wh[n, mid(), :]
            x = (-1, T)[j]
            w02[column(w02, h, x), :] = v
            w12[column(w12, h, x), :] = 0.2 * v + hx[h, BH, :] * (
                (g[h, DX, :] + add)
                + (wh[n, left(), :] + wh[n, right(), :])
                + w02[column(w02, h, (0, T - 1)[j]), :]
            )
            n += 1
        for i, (g, hy) in enumerate(((gyl, hyl), (gyh, hyh))):
            c = cv[h, (DEPTH - 1, DEPTH + NB)[i], pl.ds(8, NB), :]
            for k in range(R):
                sh[n, rows(k, NB, R), :] = c
            add = sh[n]
            wh[n, mid(), :] = g[h, U2Y, :] + add
            wh[n, one(7), :], wh[n, one(8 + T), :] = diag[i, 0], diag[i, 1]
            wh[n, one(8), :] = wh[n, one(8), :] + bumps[h, i, 0][2]
            wh[n, one(7 + T), :] = wh[n, one(7 + T), :] + bumps[h, i, 1][2]
            v = wh[n, mid(), :]
            r = (0, T + 1)[i]
            w0[h, r, mid(), :] = v
            w1[h, r, mid(), :] = 0.2 * v + hy[h, BH, :] * (
                (g[h, DY, :] + add)
                + (wh[n, left(), :] + wh[n, right(), :])
                + w0[h, (1, T)[i], mid(), :]
            )
            n += 1

    copies = []
    for h in range(HALVES):

        def one_more(y, c, h=h):
            w1[h, y + 1, mid(), :] = 0.2 * w0[h, y + 1, mid(), :] + b[h, y] * (ld[h, y] + around(w0, h, y))
            return c

        def last(y, c, h=h):
            w0[h, y + 1, mid(), :] = 0.2 * w1[h, y + 1, mid(), :] + b[h, y] * (ld[h, y] + around(w1, h, y))
            return c

        lax.fori_loop(0, T, one_more, 0, unroll=2)
        step = T // 4
        for q in range(4):
            lax.fori_loop(q * step, (q + 1) * step, last, 0, unroll=2)
            copies.append(
                pltpu.make_async_copy(
                    w0.at[h, pl.ds(1 + q * step, step), mid(), :],
                    out.at[pl.ds(q * step, step), :, pl.ds(h * LANES, LANES)],
                    sems.at[h, q],
                )
            )
            copies[-1].start()
    for c in copies:
        c.wait()


def vmem(*shape):
    return pltpu.VMEM(shape, F)


V = pl.BlockSpec(memory_space=pltpu.VMEM)
H = pl.BlockSpec(memory_space=pltpu.HBM)


def shifted(value, axis, step):
    size = lax.axis_size(axis)
    return lax.ppermute(value, axis, [(i, (i + step) % size) for i in range(size)])


def per_device(load_terms, start_values, reaction_rate):
    tile, padded = (HALVES, T, T, LANES), (HALVES, PR, PC, LANES)
    coarse = (HALVES * NB * NB, LANES)
    edge = (HALVES, 3 * T, LANES)
    part = vmem(HALVES * NB * T, LANES)
    pxl, pxh, pyl, pyh, u1p, b, ld, m, mo = pl.pallas_call(
        first_kernel,
        in_specs=[H] * 3,
        out_specs=[V] * 9,
        out_shape=[vmem(*edge)] * 4 + [vmem(*padded)] + [vmem(*tile)] * 3 + [vmem(*coarse)],
        scratch_shapes=[vmem(*padded), part, pltpu.SemaphoreType.DMA((3, HALVES))],
        compiler_params=pltpu.CompilerParams(vmem_limit_bytes=12 * MIB),
        name="first",
    )(*(pltpu.with_memory_space_constraint(v, pltpu.HBM) for v in (load_terms, start_values, reaction_rate)))
    hyl, hyh = shifted(pyh, "py", 1), shifted(pyl, "py", -1)
    hxl, hxh = shifted(pxh, "px", 1), shifted(pxl, "px", -1)
    _, u2p, lp, qxl, qxh = pl.pallas_call(
        second_kernel,
        in_specs=[V] * 13,
        out_specs=[V] * 5,
        out_shape=[vmem(*padded)] * 2 + [vmem(*coarse)] + [vmem(HALVES, QX, LANES)] * 2,
        scratch_shapes=[part],
        input_output_aliases={0: 0},
        compiler_params=pltpu.CompilerParams(vmem_limit_bytes=8 * MIB),
        name="second",
    )(u1p, b, ld, m, mo, pxl, pxh, pyl, pyh, hxl, hxh, hyl, hyh)
    gxl, gxh = shifted(qxh, "px", 1), shifted(qxl, "px", -1)
    lx, mx, s0, s1, qyl, qyh = pl.pallas_call(
        third_kernel,
        in_specs=[V] * 10,
        out_specs=[V] * 6,
        out_shape=[vmem(HALVES, NB, CW, LANES)] * 2
        + [vmem(HALVES, CW, LANES)] * 2
        + [vmem(HALVES, QY, LANES)] * 2,
        compiler_params=pltpu.CompilerParams(vmem_limit_bytes=8 * MIB),
        name="third",
    )(lp, mo, u2p, ld, qxl, qxh, gxl, gxh, hxl, hxh)
    gyl, gyh = shifted(qyh, "py", 1), shifted(qyl, "py", -1)
    grid = vmem(HALVES, CR, CW, LANES)
    return pl.pallas_call(
        last_kernel,
        in_specs=[V] * 17,
        out_specs=H,
        out_shape=jax.ShapeDtypeStruct(load_terms.shape, F),
        scratch_shapes=[grid] * 4
        + [part, vmem(*padded), vmem(*padded)]
        + [vmem(8, PC, LANES), vmem(8, T, LANES), pltpu.SemaphoreType.DMA((HALVES, 4))],
        compiler_params=pltpu.CompilerParams(vmem_limit_bytes=20 * MIB),
        name="last",
    )(lx, mx, s0, s1, gyl, gyh, gxl, gxh, hxl, hxh, hyl, hyh, pxl, pxh, u2p, b, ld)


def solution(mesh):
    return jax.shard_map(
        per_device,
        mesh=mesh,
        in_specs=(P("py", "px", None), P("py", "px", None), P("py", "px", None)),
        out_specs=P("py", "px", None),
        check_vma=False,
    )
```

```python
import jax
import jax.numpy as jnp
from jax import lax
from jax.experimental import pallas as pl
from jax.experimental.pallas import tpu as pltpu
from jax.sharding import PartitionSpec as P

F = jnp.float32
T = 64
R = 4
NB = T // R
INNER = 7
DEPTH = INNER
LANES = 128
HALVES = 2
PR, PC = T + 2, T + 16
PLANE = PR * PC
CW = 32
CR = NB + 2 * DEPTH
KX = DEPTH * NB
KY = sum(CW - 2 * i for i in range(1, DEPTH + 1))
QX_U2, QX_D, QX_S = KX, KX + T, KX + 2 * T
QX = QX_S + 16
QY_S = KY
QY_U2, QY_D, QY_DIAG = QY_S + CW, QY_S + CW + T, QY_S + CW + 2 * T
QY = QY_DIAG + 8
MIB = 2**20


def rows(start, size, stride=1):
    return pl.ds(start, size, stride=stride)


def mid():
    return pl.ds(8, T)


def left():
    return pl.ds(7, T)


def right():
    return pl.ds(9, T)


def around(ref, h, y):
    return (ref[h, y, mid(), :] + ref[h, y + 2, mid(), :]) + (
        ref[h, y + 1, left(), :] + ref[h, y + 1, right(), :]
    )


def each_row(body, n=T, unroll=2):
    for h in range(HALVES):
        lax.fori_loop(0, n, lambda y, c, h=h: (body(h, y), c)[1], 0, unroll=unroll)


def clear_border(ref):
    for h in range(HALVES):
        ref[h, 0] = jnp.zeros((PC, LANES), F)
        ref[h, PR - 1] = jnp.zeros((PC, LANES), F)
        for x in (0, PC - 8):
            ref[h, pl.ds(1, T), pl.ds(x, 8), :] = jnp.zeros((T, 8, LANES), F)


def column(h, x):
    return rows(h * PLANE + PC + 8 + x, T, PC)


def block_sums(part, out):
    n = HALVES * NB * NB

    def body(j, c):
        total = part[rows(j * 4 * T, T, R), :]
        for k in range(1, R):
            total = total + part[rows(j * 4 * T + k, T, R), :]
        out[pl.ds(j * T, T), :] = total * (1.0 / R)
        return c

    lax.fori_loop(0, n // T, body, 0)


def edge_kernel(load_h, u_h, m_h, pxl, pxh, pyl, pyh, uc, lc, mc, ur, lr, mr, sems):
    copies = []
    for h in range(HALVES):
        lanes = pl.ds(h * LANES, LANES)
        for i in range(2):
            x, y, yy = (0, T - 8)[i], (0, T - 1)[i], (0, T - 2)[i]
            for src, dst, n in (
                (u_h.at[:, pl.ds(x, 8), lanes], uc.at[h, i, pl.ds(1, T)], 0),
                (load_h.at[:, pl.ds(x, 8), lanes], lc.at[h, i], 1),
                (m_h.at[:, pl.ds(x, 8), lanes], mc.at[h, i], 2),
                (u_h.at[pl.ds(yy, 2), :, lanes], ur.at[h, i, :, mid(), :], 3),
                (load_h.at[pl.ds(y, 1), :, lanes], lr.at[h, i], 4),
                (m_h.at[pl.ds(y, 1), :, lanes], mr.at[h, i], 5),
            ):
                copies.append(pltpu.make_async_copy(src, dst, sems.at[h, i, n]))
    for c in copies:
        c.start()
    for h in range(HALVES):
        for i in range(2):
            uc[h, i, 0] = jnp.zeros((8, LANES), F)
            uc[h, i, T + 1] = jnp.zeros((8, LANES), F)
            for k in range(2):
                ur[h, i, k, pl.ds(0, 8), :] = jnp.zeros((8, LANES), F)
                ur[h, i, k, pl.ds(8 + T, 8), :] = jnp.zeros((8, LANES), F)
    for c in copies:
        c.wait()
    uc2 = uc.reshape(HALVES * 2 * (T + 2) * 8, LANES)
    lc2, mc2 = lc.reshape(HALVES * 2 * T * 8, LANES), mc.reshape(HALVES * 2 * T * 8, LANES)
    for h in range(HALVES):
        for i in range(2):
            px, py = (pxl, pxh)[i], (pyl, pyh)[i]
            ub, lb = (h * 2 + i) * (T + 2) * 8, (h * 2 + i) * T * 8
            x, xi = (0, 7)[i], (1, 6)[i]
            u = uc2[rows(ub + 8 + x, T, 8), :]
            bb = 0.8 / (4.0 + mc2[rows(lb + x, T, 8), :])
            near = uc2[rows(ub + 8 + xi, T, 8), :] + (uc2[rows(ub + x, T, 8), :] + uc2[rows(ub + 16 + x, T, 8), :])
            px[h, pl.ds(0, T), :] = u
            px[h, pl.ds(T, T), :] = 0.2 * u + bb * (lc2[rows(lb + x, T, 8), :] + near)
            px[h, pl.ds(2 * T, T), :] = bb
            k = i
            u = ur[h, i, k, mid(), :]
            bb = 0.8 / (4.0 + mr[h, i, 0])
            near = ur[h, i, 1 - k, mid(), :] + (ur[h, i, k, left(), :] + ur[h, i, k, right(), :])
            py[h, pl.ds(0, T), :] = u
            py[h, pl.ds(T, T), :] = 0.2 * u + bb * (lr[h, i, 0] + near)
            py[h, pl.ds(2 * T, T), :] = bb


CHUNKS = 4


def first_kernel(load_h, u_h, m_h, u1p, b, ld, m, mo, kxl, kxh, up, part, sems):
    step = T // CHUNKS
    copies = {}
    for h in range(HALVES):
        lanes = pl.ds(h * LANES, LANES)
        for q in range(CHUNKS):
            y = pl.ds(q * step, step)
            copies[h, q] = [
                pltpu.make_async_copy(m_h.at[y, :, lanes], m.at[h, y], sems.at[0, h, q]),
                pltpu.make_async_copy(
                    u_h.at[y, :, lanes], up.at[h, pl.ds(q * step + 1, step), pl.ds(8, T), :], sems.at[1, h, q]
                ),
                pltpu.make_async_copy(load_h.at[y, :, lanes], ld.at[h, y], sems.at[2, h, q]),
            ]
            for c in copies[h, q]:
                c.start()
    clear_border(up)

    for h in range(HALVES):

        def sweep(y, c, h=h):
            bb = 0.8 / (4.0 + m[h, y])
            b[h, y] = bb
            u1p[h, y + 1, mid(), :] = 0.2 * up[h, y + 1, mid(), :] + bb * (ld[h, y] + around(up, h, y))
            return c

        def sums(y, c, h=h):
            part[pl.ds(pl.multiple_of((h * NB + y) * T, T), T), :] = (m[h, R * y] + m[h, R * y + 1]) + (
                m[h, R * y + 2] + m[h, R * y + 3]
            )
            return c

        for q in range(CHUNKS):
            for c in copies[h, q]:
                c.wait()
            lax.fori_loop(q * step // R, (q + 1) * step // R, sums, 0, unroll=2)
            lax.fori_loop(max(q * step - 1, 0), T if q == CHUNKS - 1 else (q + 1) * step - 1, sweep, 0, unroll=2 if q else 1)
    block_sums(part, mo)
    for h in range(HALVES):
        for first, q in ((0, kxl), (NB - DEPTH, kxh)):
            for k in range(DEPTH):
                q[h, pl.ds(k * NB, NB), :] = mo[rows(h * NB * NB + first + k, NB, NB), :]


def spread_x(inner, low, high, ext):
    ext2 = ext.reshape(HALVES * NB * CW, LANES)
    for h in range(HALVES):
        for y in range(NB):
            ext[h, y, pl.ds(8, NB), :] = inner[pl.ds(h * NB * NB + y * NB, NB), :]
        for c, g in ((1, low), (8 + NB, high)):
            for k in range(DEPTH):
                ext2[rows(h * NB * CW + c + k, NB, CW), :] = g[h, pl.ds(k * NB, NB), :]


def wedge(i):
    return i, CW - 2 * i, sum(CW - 2 * k for k in range(1, i))


def cut_wedges(ext, h, low, high):
    for i in range(1, DEPTH + 1):
        c, n, at = wedge(i)
        low[h, pl.ds(at, n), :] = ext[h, i - 1, pl.ds(c, n), :]
        high[h, pl.ds(at, n), :] = ext[h, NB - i, pl.ds(c, n), :]


def mass_kernel(mo, gml, gmh, mx, kyl, kyh):
    spread_x(mo, gml, gmh, mx)
    for h in range(HALVES):
        cut_wedges(mx, h, kyl, kyh)


def second_kernel(u1p_in, b, ld, m, pxl, pxh, pyl, pyh, hxl, hxh, hyl, hyh, u1p, u2p, lp, qxl, qxh, part):
    del u1p_in
    u1p2 = u1p.reshape(HALVES * PLANE, LANES)
    U, A, B = pl.ds(0, T), pl.ds(T, T), pl.ds(2 * T, T)
    clear_border(u2p)
    for h in range(HALVES):
        for x, p, g in ((0, pxl, hxl), (T - 1, pxh, hxh)):
            inner = column(h, x)
            outer = column(h, -1 if x == 0 else T)
            u1p2[inner, :] = u1p2[inner, :] + p[h, B, :] * g[h, U, :]
            u1p2[outer, :] = g[h, A, :] + g[h, B, :] * p[h, U, :]
        for y, p, g in ((0, pyl, hyl), (T - 1, pyh, hyh)):
            u1p[h, y + 1, mid(), :] = u1p[h, y + 1, mid(), :] + p[h, B, :] * g[h, U, :]
            u1p[h, 0 if y == 0 else T + 1, mid(), :] = g[h, A, :] + g[h, B, :] * p[h, U, :]

    def sweep(h, y):
        u2p[h, y + 1, mid(), :] = 0.2 * u1p[h, y + 1, mid(), :] + b[h, y] * (ld[h, y] + around(u1p, h, y))

    each_row(sweep)

    def sums(h, y):
        total = None
        for k in range(R):
            c = R * y + k
            d = (ld[h, c] + around(u2p, h, c)) - (4.0 + m[h, c]) * u2p[h, c + 1, mid(), :]
            total = d if total is None else total + d
        part[pl.ds(pl.multiple_of((h * NB + y) * T, T), T), :] = total

    each_row(sums, NB, unroll=1)
    block_sums(part, lp)

    u2p2, ld2 = u2p.reshape(HALVES * PLANE, LANES), ld.reshape(HALVES * T * T, LANES)
    for h in range(HALVES):
        for x, first, s, q in ((0, 0, 0, qxl), (T - 1, NB - DEPTH, 8, qxh)):
            for k in range(DEPTH):
                q[h, pl.ds(k * NB, NB), :] = lp[rows(h * NB * NB + first + k, NB, NB), :]
            q[h, pl.ds(QX_U2, T), :] = u2p2[column(h, x), :]
            q[h, pl.ds(QX_D, T), :] = ld2[rows(h * T * T + x, T, T), :] + u2p2[column(h, 1 if x == 0 else T - 2), :]
            for i, y in enumerate((0, T - 1)):
                total = None
                for k in range(R):
                    v = u2p2[rows(h * PLANE + (y + 1) * PC + 8 + R * s + k, 8, R), :]
                    total = v if total is None else total + v
                q[h, pl.ds(QX_S + 8 * i, 8), :] = total


def third_kernel(lp, u2p, ld, qxl, qxh, gxl, gxh, hxl, hxh, lx, s0, s1, qyl, qyh):
    lx2 = lx.reshape(HALVES * NB * CW, LANES)
    flat = lambda r: r.reshape(HALVES * QX, LANES)
    qxl2, qxh2, gxl2, gxh2 = flat(qxl), flat(qxh), flat(gxl), flat(gxh)

    def quarter(ref, h):
        total = ref[rows(h * QX + QX_U2, NB, R), :]
        for k in range(1, R):
            total = total + ref[rows(h * QX + QX_U2 + k, NB, R), :]
        return total * (1.0 / R)

    spread_x(lp, gxl, gxh, lx)
    for h in range(HALVES):
        col = lambda c: rows(h * NB * CW + c, NB, CW)
        for c, ref in ((8, gxl2), (7, qxl2), (7 + NB, gxh2), (8 + NB, qxh2)):
            lx2[col(c), :] = lx2[col(c), :] + quarter(ref, h)
        for i, s in enumerate((s0, s1)):
            for c, ref in ((0, gxl), (8, qxl), (16, qxh), (24, gxh)):
                s[h, pl.ds(c, 8), :] = ref[h, pl.ds(QX_S + 8 * i, 8), :]
        cut_wedges(lx, h, qyl, qyh)
        for y, inside, s, q in ((0, 1, s0, qyl), (T - 1, T - 2, s1, qyh)):
            q[h, pl.ds(QY_S, CW), :] = s[h]
            q[h, pl.ds(QY_U2, T), :] = u2p[h, y + 1, mid(), :]
            q[h, pl.ds(QY_D, T), :] = ld[h, y] + u2p[h, inside + 1, mid(), :]
            for j, (g1, g2) in enumerate(((hxl, gxl), (hxh, gxh))):
                q[h, pl.ds(QY_DIAG + 3 * j, 1), :] = g1[h, pl.ds(y, 1), :]
                q[h, pl.ds(QY_DIAG + 3 * j + 1, 1), :] = g1[h, pl.ds(2 * T + y, 1), :]
                q[h, pl.ds(QY_DIAG + 3 * j + 2, 1), :] = g2[h, pl.ds(QX_U2 + y, 1), :]
            q[h, pl.ds(QY_DIAG + 6, 2), :] = jnp.zeros((2, LANES), F)


def last_kernel(
    lx, mx, gkl, gkh, s0, s1, gyl, gyh, gxl, gxh, hxl, hxh, hyl, hyh, pxl, pxh, u2p, b, ld,
    out, lg, bc, ca, cb, sp, w0, w1, wh, sh, sems,
):
    one = lambda r: pl.ds(r, 1)
    for h in range(HALVES):
        for i in range(1, DEPTH + 1):
            c, n, at = wedge(i)
            for r, g, gk in ((DEPTH - i, gyl, gkl), (DEPTH + NB - 1 + i, gyh, gkh)):
                lg[h, r, pl.ds(c, n), :] = g[h, pl.ds(at, n), :]
                bc[h, r, pl.ds(c, n), :] = 0.8 / (4.0 + gk[h, pl.ds(at, n), :])
        for y in range(NB):
            lg[h, DEPTH + y] = lx[h, y]
            bc[h, DEPTH + y] = 0.8 / (4.0 + mx[h, y])
        quarter = 1.0 / R
        for r, v in (
            (DEPTH - 1, s0[h]),
            (DEPTH, gyl[h, pl.ds(QY_S, CW), :]),
            (DEPTH + NB - 1, gyh[h, pl.ds(QY_S, CW), :]),
            (DEPTH + NB, s1[h]),
        ):
            lg[h, r] = lg[h, r] + quarter * v

    bumps = {}
    for h in range(HALVES):
        for j, (px, hx) in enumerate(((pxl, hxl), (pxh, hxh))):
            for i, (hy, gy) in enumerate(((hyl, gyl), (hyh, gyh))):
                y, x = (0, T - 1)[i], (0, T - 1)[j]
                ua, ba = px[h, one(y), :], px[h, one(2 * T + y), :]
                ux, bx = hx[h, one(y), :], hx[h, one(2 * T + y), :]
                uy, by = hy[h, one(x), :], hy[h, one(2 * T + x), :]
                ud, bd = gy[h, one(QY_DIAG + 3 * j), :], gy[h, one(QY_DIAG + 3 * j + 1), :]
                ea, ed = ba * (bx + by) * ud, bd * (bx + by) * ua
                ex, ey = bx * (ba + bd) * uy, by * (ba + bd) * ux
                ya, yo = (DEPTH, DEPTH - 1) if i == 0 else (DEPTH + NB - 1, DEPTH + NB)
                xa, xo = (8, 7) if j == 0 else (7 + NB, 8 + NB)
                for yy, xx, e, bb, e1, e2 in (
                    (ya, xa, ea, ba, ex, ey),
                    (ya, xo, ex, bx, ea, ed),
                    (yo, xa, ey, by, ea, ed),
                    (yo, xo, ed, bd, ex, ey),
                ):
                    lg[h, yy, one(xx), :] = lg[h, yy, one(xx), :] + quarter * (
                        (2.0 - 0.8 / bb) * e + (e1 + e2)
                    )
                bumps[h, i, j] = (ea, ex, ey, ed + gy[h, one(QY_DIAG + 3 * j + 2), :])

    def start(h, y):
        v = bc[h, y] * lg[h, y]
        lg[h, y] = v
        ca[h, y] = v

    each_row(start, CR)
    old, new = ca, cb
    for s in range(1, INNER):

        def inner(h, i, old=old, new=new, s=s):
            y = i + s
            c = old[h, y]
            around_c = (old[h, y - 1] + old[h, y + 1]) + (pltpu.roll(c, 1, 0) + pltpu.roll(c, CW - 1, 0))
            new[h, y] = (0.2 * c + lg[h, y]) + bc[h, y] * around_c

        each_row(inner, CR - 2 * s)
        old, new = new, old
    cv = old
    cv2 = cv.reshape(HALVES * CR * CW, LANES)

    def correct(h, y):
        base = pl.multiple_of((h * NB + y) * T, T)
        c = cv[h, y + DEPTH, pl.ds(8, NB), :]
        for k in range(R):
            sp[rows(base + k, NB, R), :] = c
        add = sp[pl.ds(base, T), :]
        for k in range(R):
            w0[h, R * y + k + 1, mid(), :] = u2p[h, R * y + k + 1, mid(), :] + add

    each_row(correct, NB)

    w02, w12 = w0.reshape(HALVES * PLANE, LANES), w1.reshape(HALVES * PLANE, LANES)
    for h in range(HALVES):
        for i in range(2):
            for j in range(2):
                r, x = (1, T)[i], (8, T + 7)[j]
                w0[h, r, one(x), :] = w0[h, r, one(x), :] + bumps[h, i, j][0]
    U2X, DX, U2Y, DY, BH = pl.ds(QX_U2, T), pl.ds(QX_D, T), pl.ds(QY_U2, T), pl.ds(QY_D, T), pl.ds(2 * T, T)
    n = 0
    for h in range(HALVES):
        diag = {}
        for i in range(2):
            for j in range(2):
                diag[i, j] = (
                    bumps[h, i, j][3] + cv[h, (DEPTH - 1, DEPTH + NB)[i], one((7, 8 + NB)[j]), :]
                )
        for j, (g, hx) in enumerate(((gxl, hxl), (gxh, hxh))):
            c = cv2[rows(h * CR * CW + DEPTH * CW + (7, 8 + NB)[j], NB, CW), :]
            for k in range(R):
                sh[n, rows(k, NB, R), :] = c
            add = sh[n]
            wh[n, mid(), :] = g[h, U2X, :] + add
            wh[n, one(7), :], wh[n, one(8 + T), :] = diag[0, j], diag[1, j]
            wh[n, one(8), :] = wh[n, one(8), :] + bumps[h, 0, j][1]
            wh[n, one(7 + T), :] = wh[n, one(7 + T), :] + bumps[h, 1, j][1]
            v = wh[n, mid(), :]
            x = (-1, T)[j]
            w02[column(h, x), :] = v
            w12[column(h, x), :] = 0.2 * v + hx[h, BH, :] * (
                (g[h, DX, :] + add)
                + (wh[n, left(), :] + wh[n, right(), :])
                + w02[column(h, (0, T - 1)[j]), :]
            )
            n += 1
        for i, (g, hy) in enumerate(((gyl, hyl), (gyh, hyh))):
            c = cv[h, (DEPTH - 1, DEPTH + NB)[i], pl.ds(8, NB), :]
            for k in range(R):
                sh[n, rows(k, NB, R), :] = c
            add = sh[n]
            wh[n, mid(), :] = g[h, U2Y, :] + add
            wh[n, one(7), :], wh[n, one(8 + T), :] = diag[i, 0], diag[i, 1]
            wh[n, one(8), :] = wh[n, one(8), :] + bumps[h, i, 0][2]
            wh[n, one(7 + T), :] = wh[n, one(7 + T), :] + bumps[h, i, 1][2]
            v = wh[n, mid(), :]
            r = (0, T + 1)[i]
            w0[h, r, mid(), :] = v
            w1[h, r, mid(), :] = 0.2 * v + hy[h, BH, :] * (
                (g[h, DY, :] + add)
                + (wh[n, left(), :] + wh[n, right(), :])
                + w0[h, (1, T)[i], mid(), :]
            )
            n += 1

    copies = []
    for h in range(HALVES):

        def one_more(y, c, h=h):
            w1[h, y + 1, mid(), :] = 0.2 * w0[h, y + 1, mid(), :] + b[h, y] * (ld[h, y] + around(w0, h, y))
            return c

        def last(y, c, h=h):
            w0[h, y + 1, mid(), :] = 0.2 * w1[h, y + 1, mid(), :] + b[h, y] * (ld[h, y] + around(w1, h, y))
            return c

        lax.fori_loop(0, T, one_more, 0, unroll=2)
        step = T // 4
        for q in range(4):
            lax.fori_loop(q * step, (q + 1) * step, last, 0, unroll=2)
            copies.append(
                pltpu.make_async_copy(
                    w0.at[h, pl.ds(1 + q * step, step), mid(), :],
                    out.at[pl.ds(q * step, step), :, pl.ds(h * LANES, LANES)],
                    sems.at[h, q],
                )
            )
            copies[-1].start()
    for c in copies:
        c.wait()


def vmem(*shape):
    return pltpu.VMEM(shape, F)


V = pl.BlockSpec(memory_space=pltpu.VMEM)
H = pl.BlockSpec(memory_space=pltpu.HBM)


def swapped(axis, low, high):
    size = lax.axis_size(axis)
    up = [(i, (i + 1) % size) for i in range(size)]
    return lax.ppermute(high, axis, up), lax.ppermute(low, axis, [(b, a) for a, b in up])


def estimate(flops, size):
    return pl.CostEstimate(flops=flops, bytes_accessed=size, transcendentals=0)


def per_device(load_terms, start_values, reaction_rate):
    tile, padded = (HALVES, T, T, LANES), (HALVES, PR, PC, LANES)
    coarse = (HALVES * NB * NB, LANES)
    edge = (HALVES, 3 * T, LANES)
    part = vmem(HALVES * NB * T, LANES)
    inputs = tuple(
        pltpu.with_memory_space_constraint(v, pltpu.HBM) for v in (load_terms, start_values, reaction_rate)
    )
    strip, line = vmem(HALVES, 2, T, 8, LANES), vmem(HALVES, 2, 1, T, LANES)
    pxl, pxh, pyl, pyh = pl.pallas_call(
        edge_kernel,
        in_specs=[H] * 3,
        out_specs=[V] * 4,
        out_shape=[vmem(*edge)] * 4,
        scratch_shapes=[vmem(HALVES, 2, T + 2, 8, LANES), strip, strip, vmem(HALVES, 2, 2, PC, LANES), line, line]
        + [pltpu.SemaphoreType.DMA((HALVES, 2, 6))],
        compiler_params=pltpu.CompilerParams(vmem_limit_bytes=8 * MIB),
        name="edges",
    )(*inputs)
    hxl, hxh = swapped("px", pxl, pxh)
    hyl, hyh = swapped("py", pyl, pyh)
    u1p, b, ld, m, mo, kxl, kxh = pl.pallas_call(
        first_kernel,
        in_specs=[H] * 3,
        out_specs=[V] * 7,
        out_shape=[vmem(*padded)] + [vmem(*tile)] * 3 + [vmem(*coarse)] + [vmem(HALVES, KX, LANES)] * 2,
        scratch_shapes=[vmem(*padded), part, pltpu.SemaphoreType.DMA((3, HALVES, CHUNKS))],
        compiler_params=pltpu.CompilerParams(vmem_limit_bytes=12 * MIB),
        cost_estimate=estimate(10**7, 12 * MIB),
        name="first",
    )(*inputs)
    gml, gmh = swapped("px", kxl, kxh)
    _, u2p, lp, qxl, qxh = pl.pallas_call(
        second_kernel,
        in_specs=[V] * 12,
        out_specs=[V] * 5,
        out_shape=[vmem(*padded)] * 2 + [vmem(*coarse)] + [vmem(HALVES, QX, LANES)] * 2,
        scratch_shapes=[part],
        input_output_aliases={0: 0},
        compiler_params=pltpu.CompilerParams(vmem_limit_bytes=8 * MIB),
        name="second",
    )(u1p, b, ld, m, pxl, pxh, pyl, pyh, hxl, hxh, hyl, hyh)
    gxl, gxh = swapped("px", qxl, qxh)
    mx, kyl, kyh = pl.pallas_call(
        mass_kernel,
        in_specs=[V] * 3,
        out_specs=[V] * 3,
        out_shape=[vmem(HALVES, NB, CW, LANES)] + [vmem(HALVES, KY, LANES)] * 2,
        compiler_params=pltpu.CompilerParams(vmem_limit_bytes=8 * MIB),
        name="mass",
    )(mo, gml, gmh)
    gkl, gkh = swapped("py", kyl, kyh)
    lx, s0, s1, qyl, qyh = pl.pallas_call(
        third_kernel,
        in_specs=[V] * 9,
        out_specs=[V] * 5,
        out_shape=[vmem(HALVES, NB, CW, LANES)]
        + [vmem(HALVES, CW, LANES)] * 2
        + [vmem(HALVES, QY, LANES)] * 2,
        compiler_params=pltpu.CompilerParams(vmem_limit_bytes=8 * MIB),
        name="third",
    )(lp, u2p, ld, qxl, qxh, gxl, gxh, hxl, hxh)
    gyl, gyh = swapped("py", qyl, qyh)
    grid = vmem(HALVES, CR, CW, LANES)
    return pl.pallas_call(
        last_kernel,
        in_specs=[V] * 19,
        out_specs=H,
        out_shape=jax.ShapeDtypeStruct(load_terms.shape, F),
        scratch_shapes=[grid] * 4
        + [part, vmem(*padded), vmem(*padded)]
        + [vmem(8, PC, LANES), vmem(8, T, LANES), pltpu.SemaphoreType.DMA((HALVES, 4))],
        compiler_params=pltpu.CompilerParams(vmem_limit_bytes=20 * MIB),
        name="last",
    )(lx, mx, gkl, gkh, s0, s1, gyl, gyh, gxl, gxh, hxl, hxh, hyl, hyh, pxl, pxh, u2p, b, ld)


def solution(mesh):
    return jax.shard_map(
        per_device,
        mesh=mesh,
        in_specs=(P("py", "px", None), P("py", "px", None), P("py", "px", None)),
        out_specs=P("py", "px", None),
        check_vma=False,
    )
```

```python
import jax
import jax.numpy as jnp
from jax import lax
from jax.experimental import pallas as pl
from jax.experimental.pallas import tpu as pltpu
from jax.sharding import PartitionSpec as P

F = jnp.float32
T = 64
R = 4
NB = T // R
INNER = 7
DEPTH = INNER
LANES = 128
HALVES = 2
PR, PC = T + 2, T + 16
PLANE = PR * PC
CW = 32
CR = NB + 2 * DEPTH
KX = DEPTH * NB
KY = sum(CW - 2 * i for i in range(1, DEPTH + 1))
QX_S, QX_Q = KX, KX + 16
QX = QX_Q + NB
QY_S, QY_DIAG = KY, KY + CW
QY = QY_DIAG + 8
MIB = 2**20


def rows(start, size, stride=1):
    return pl.ds(start, size, stride=stride)


def mid():
    return pl.ds(8, T)


def left():
    return pl.ds(7, T)


def right():
    return pl.ds(9, T)


def around(ref, h, y):
    return (ref[h, y, mid(), :] + ref[h, y + 2, mid(), :]) + (
        ref[h, y + 1, left(), :] + ref[h, y + 1, right(), :]
    )


def each_row(body, n=T, unroll=2):
    for h in range(HALVES):
        lax.fori_loop(0, n, lambda y, c, h=h: (body(h, y), c)[1], 0, unroll=unroll)


def carried(h, first, last, src, point, unroll=2):
    def body(y, c):
        above, here = c
        below = src[h, y + 2, mid(), :]
        point(y, here, (above + below) + (src[h, y + 1, left(), :] + src[h, y + 1, right(), :]))
        return here, below

    lax.fori_loop(first, last, body, (src[h, first, mid(), :], src[h, first + 1, mid(), :]), unroll=unroll)


def clear_border(ref):
    for h in range(HALVES):
        ref[h, 0] = jnp.zeros((PC, LANES), F)
        ref[h, PR - 1] = jnp.zeros((PC, LANES), F)
        for x in (0, PC - 8):
            ref[h, pl.ds(1, T), pl.ds(x, 8), :] = jnp.zeros((T, 8, LANES), F)


def column(h, x):
    return rows(h * PLANE + PC + 8 + x, T, PC)


SWAPPED = ("py",)


def is_even(axis):
    return lax.rem(lax.axis_index(axis), 2) == 0


def order(axis, first, second, a, b):
    even = is_even(axis) if axis in SWAPPED else False
    n = first.shape[1]
    for h in range(HALVES):
        for r in range(0, n, T):
            part = pl.ds(r, min(T, n - r))
            va, vb = a[h, part, :], b[h, part, :]
            first[h, part, :] = va if even is False else jnp.where(even, vb, va)
            second[h, part, :] = vb if even is False else jnp.where(even, va, vb)


def block_sums(part, out):
    n = HALVES * NB * NB

    def body(j, c):
        total = part[rows(j * 4 * T, T, R), :]
        for k in range(1, R):
            total = total + part[rows(j * 4 * T + k, T, R), :]
        out[pl.ds(j * T, T), :] = total * (1.0 / R)
        return c

    lax.fori_loop(0, n // T, body, 0)


def edge_kernel(load_h, u_h, m_h, pxl, pxh, pyl, pyh, pxe, pxo, pye, pyo, uc, lc, mc, ur, lr, mr, sems):
    copies = []
    for h in range(HALVES):
        lanes = pl.ds(h * LANES, LANES)
        for i in range(2):
            x, y, yy = (0, T - 8)[i], (0, T - 1)[i], (0, T - 2)[i]
            for src, dst, n in (
                (u_h.at[:, pl.ds(x, 8), lanes], uc.at[h, i, pl.ds(1, T)], 0),
                (load_h.at[:, pl.ds(x, 8), lanes], lc.at[h, i], 1),
                (m_h.at[:, pl.ds(x, 8), lanes], mc.at[h, i], 2),
                (u_h.at[pl.ds(yy, 2), :, lanes], ur.at[h, i, :, mid(), :], 3),
                (load_h.at[pl.ds(y, 1), :, lanes], lr.at[h, i], 4),
                (m_h.at[pl.ds(y, 1), :, lanes], mr.at[h, i], 5),
            ):
                copies.append(pltpu.make_async_copy(src, dst, sems.at[h, i, n]))
    for c in copies:
        c.start()
    for h in range(HALVES):
        for i in range(2):
            uc[h, i, 0] = jnp.zeros((8, LANES), F)
            uc[h, i, T + 1] = jnp.zeros((8, LANES), F)
            for k in range(2):
                ur[h, i, k, pl.ds(0, 8), :] = jnp.zeros((8, LANES), F)
                ur[h, i, k, pl.ds(8 + T, 8), :] = jnp.zeros((8, LANES), F)
    for c in copies:
        c.wait()
    uc2 = uc.reshape(HALVES * 2 * (T + 2) * 8, LANES)
    lc2, mc2 = lc.reshape(HALVES * 2 * T * 8, LANES), mc.reshape(HALVES * 2 * T * 8, LANES)
    for h in range(HALVES):
        for i in range(2):
            px, py = (pxl, pxh)[i], (pyl, pyh)[i]
            ub, lb = (h * 2 + i) * (T + 2) * 8, (h * 2 + i) * T * 8
            x, xi = (0, 7)[i], (1, 6)[i]
            u = uc2[rows(ub + 8 + x, T, 8), :]
            bb = 0.8 / (4.0 + mc2[rows(lb + x, T, 8), :])
            near = uc2[rows(ub + 8 + xi, T, 8), :] + (uc2[rows(ub + x, T, 8), :] + uc2[rows(ub + 16 + x, T, 8), :])
            px[h, pl.ds(0, T), :] = u
            px[h, pl.ds(T, T), :] = 0.2 * u + bb * (lc2[rows(lb + x, T, 8), :] + near)
            px[h, pl.ds(2 * T, T), :] = bb
            k = i
            u = ur[h, i, k, mid(), :]
            bb = 0.8 / (4.0 + mr[h, i, 0])
            near = ur[h, i, 1 - k, mid(), :] + (ur[h, i, k, left(), :] + ur[h, i, k, right(), :])
            py[h, pl.ds(0, T), :] = u
            py[h, pl.ds(T, T), :] = 0.2 * u + bb * (lr[h, i, 0] + near)
            py[h, pl.ds(2 * T, T), :] = bb
    order("px", pxe, pxo, pxl, pxh)
    order("py", pye, pyo, pyl, pyh)


CHUNKS = 4


def first_kernel(load_h, u_h, m_h, u1p, b, ld, m, mo, kxe, kxo, up, part, kxl, kxh, sems):
    step = T // CHUNKS
    copies = {}
    for h in range(HALVES):
        lanes = pl.ds(h * LANES, LANES)
        for q in range(CHUNKS):
            y = pl.ds(q * step, step)
            copies[h, q] = [
                pltpu.make_async_copy(m_h.at[y, :, lanes], m.at[h, y], sems.at[0, h, q]),
                pltpu.make_async_copy(
                    u_h.at[y, :, lanes], up.at[h, pl.ds(q * step + 1, step), pl.ds(8, T), :], sems.at[1, h, q]
                ),
                pltpu.make_async_copy(load_h.at[y, :, lanes], ld.at[h, y], sems.at[2, h, q]),
            ]
            for c in copies[h, q]:
                c.start()
    clear_border(up)

    for h in range(HALVES):

        def sweep(y, c, h=h):
            bb = 0.8 / (4.0 + m[h, y])
            b[h, y] = bb
            u1p[h, y + 1, mid(), :] = 0.2 * up[h, y + 1, mid(), :] + bb * (ld[h, y] + around(up, h, y))
            return c

        def sums(y, c, h=h):
            part[pl.ds(pl.multiple_of((h * NB + y) * T, T), T), :] = (m[h, R * y] + m[h, R * y + 1]) + (
                m[h, R * y + 2] + m[h, R * y + 3]
            )
            return c

        for q in range(CHUNKS):
            for c in copies[h, q]:
                c.wait()
            lax.fori_loop(q * step // R, (q + 1) * step // R, sums, 0, unroll=2)
            lax.fori_loop(max(q * step - 1, 0), T if q == CHUNKS - 1 else (q + 1) * step - 1, sweep, 0, unroll=2 if q else 1)
    block_sums(part, mo)
    for h in range(HALVES):
        for first, q in ((0, kxl), (NB - DEPTH, kxh)):
            for k in range(DEPTH):
                q[h, pl.ds(k * NB, NB), :] = mo[rows(h * NB * NB + first + k, NB, NB), :]
    order("px", kxe, kxo, kxl, kxh)


def spread_x(inner, low, high, ext):
    ext2 = ext.reshape(HALVES * NB * CW, LANES)
    for h in range(HALVES):
        for y in range(NB):
            ext[h, y, pl.ds(8, NB), :] = inner[pl.ds(h * NB * NB + y * NB, NB), :]
        for c, g in ((1, low), (8 + NB, high)):
            for k in range(DEPTH):
                ext2[rows(h * NB * CW + c + k, NB, CW), :] = g[h, pl.ds(k * NB, NB), :]


def wedge(i):
    return i, CW - 2 * i, sum(CW - 2 * k for k in range(1, i))


def cut_wedges(ext, h, low, high):
    for i in range(1, DEPTH + 1):
        c, n, at = wedge(i)
        low[h, pl.ds(at, n), :] = ext[h, i - 1, pl.ds(c, n), :]
        high[h, pl.ds(at, n), :] = ext[h, NB - i, pl.ds(c, n), :]


def mass_kernel(mo, gme, gmo, mx, kye, kyo, gml, gmh, kyl, kyh):
    order("px", gml, gmh, gme, gmo)
    spread_x(mo, gml, gmh, mx)
    for h in range(HALVES):
        cut_wedges(mx, h, kyl, kyh)
    order("py", kye, kyo, kyl, kyh)


def bulk_kernel(u1p, b, ld, m, u2p, part):
    clear_border(u2p)
    for h in range(HALVES):

        def sweep(y, c, near, h=h):
            u2p[h, y + 1, mid(), :] = 0.2 * c + b[h, y] * (ld[h, y] + near)

        carried(h, 0, T, u1p, sweep)
    each_row(lambda h, y: defect_rows(h, y, u2p, ld, m, part), NB, unroll=1)


def defect_rows(h, y, u2p, ld, m, part):
    total = None
    for k in range(R):
        c = R * y + k
        d = (ld[h, c] + around(u2p, h, c)) - (4.0 + m[h, c]) * u2p[h, c + 1, mid(), :]
        total = d if total is None else total + d
    part[pl.ds(pl.multiple_of((h * NB + y) * T, T), T), :] = total


def near_tile(ref, h, y, x):
    return (ref[h, pl.ds(y, 8), pl.ds(x + 8, 8), :] + ref[h, pl.ds(y + 2, 8), pl.ds(x + 8, 8), :]) + (
        ref[h, pl.ds(y + 1, 8), pl.ds(x + 7, 8), :] + ref[h, pl.ds(y + 1, 8), pl.ds(x + 9, 8), :]
    )


def second_kernel(
    u1p_in, u2p_in, part_in, b, ld, m, pxl, pxh, pyl, pyh, hxe, hxo, hye, hyo,
    u1p, u2p, part, lp, own, qxl, qxh, qxe, qxo, vxe, vxo, vye, vyo, hxl, hxh, hyl, hyh,
    vxl, vxh, vyl, vyh,
):
    del u1p_in, u2p_in, part_in
    order("px", hxl, hxh, hxe, hxo)
    order("py", hyl, hyh, hye, hyo)
    u1p2 = u1p.reshape(HALVES * PLANE, LANES)
    U, A, B = pl.ds(0, T), pl.ds(T, T), pl.ds(2 * T, T)
    for h in range(HALVES):
        for x, p, g in ((0, pxl, hxl), (T - 1, pxh, hxh)):
            inner = column(h, x)
            outer = column(h, -1 if x == 0 else T)
            u1p2[inner, :] = u1p2[inner, :] + p[h, B, :] * g[h, U, :]
            u1p2[outer, :] = g[h, A, :] + g[h, B, :] * p[h, U, :]
        for y, p, g in ((0, pyl, hyl), (T - 1, pyh, hyh)):
            u1p[h, y + 1, mid(), :] = u1p[h, y + 1, mid(), :] + p[h, B, :] * g[h, U, :]
            u1p[h, 0 if y == 0 else T + 1, mid(), :] = g[h, A, :] + g[h, B, :] * p[h, U, :]

    for h in range(HALVES):
        for y in (0, 1, T - 2, T - 1):
            u2p[h, y + 1, mid(), :] = 0.2 * u1p[h, y + 1, mid(), :] + b[h, y] * (ld[h, y] + around(u1p, h, y))

    def sweep(j, c):
        y = pl.multiple_of(j * 8, 8)
        for h in range(HALVES):
            for x in (0, T - 8):
                here = (h, pl.ds(y + 1, 8), pl.ds(8 + x, 8))
                tile = (h, pl.ds(y, 8), pl.ds(x, 8))
                u2p[here] = 0.2 * u1p[here] + b[tile] * (ld[tile] + near_tile(u1p, h, y, x))
        return c

    lax.fori_loop(0, T // 8, sweep, 0)

    def sums(j, c):
        y = pl.multiple_of(j * 8, 8)
        for h in range(HALVES):
            for x in (0, T - 8):
                here = (h, pl.ds(y + 1, 8), pl.ds(8 + x, 8))
                tile = (h, pl.ds(y, 8), pl.ds(x, 8))
                d = (ld[tile] + near_tile(u2p, h, y, x)) - (4.0 + m[tile]) * u2p[here]
                for k in range(2):
                    at = pl.multiple_of((h * NB + 2 * j + k) * T, T) + x
                    part[pl.ds(at, 8), :] = (d[R * k] + d[R * k + 1]) + (d[R * k + 2] + d[R * k + 3])
        return c

    lax.fori_loop(0, T // 8, sums, 0)
    for h in range(HALVES):
        for y in (0, NB - 1):
            defect_rows(h, y, u2p, ld, m, part)
    block_sums(part, lp)

    u2p2, ld2 = u2p.reshape(HALVES * PLANE, LANES), ld.reshape(HALVES * T * T, LANES)
    for h in range(HALVES):
        for x, first, s, q, v in ((0, 0, 0, qxl, vxl), (T - 1, NB - DEPTH, 8, qxh, vxh)):
            for k in range(DEPTH):
                q[h, pl.ds(k * NB, NB), :] = lp[rows(h * NB * NB + first + k, NB, NB), :]
            for i, y in enumerate((0, T - 1)):
                total = None
                for k in range(R):
                    e = u2p2[rows(h * PLANE + (y + 1) * PC + 8 + R * s + k, 8, R), :]
                    total = e if total is None else total + e
                q[h, pl.ds(QX_S + 8 * i, 8), :] = total
                own[h, i, pl.ds(s, 8), :] = total
                free = QX_S + 8 * i + (7 if x == 0 else 0)
                q[h, pl.ds(free, 1), :] = u2p[h, y + 1, pl.ds(8 + x, 1), :]
            total = None
            for k in range(R):
                e = u2p2[rows(h * PLANE + (k + 1) * PC + 8 + x, NB, R * PC), :]
                total = e if total is None else total + e
            q[h, pl.ds(QX_Q, NB), :] = total * (1.0 / R)
            v[h, pl.ds(0, T), :] = u2p2[column(h, x), :]
            v[h, pl.ds(T, T), :] = ld2[rows(h * T * T + x, T, T), :] + u2p2[column(h, 1 if x == 0 else T - 2), :]
        for y, inside, v in ((0, 1, vyl), (T - 1, T - 2, vyh)):
            v[h, pl.ds(0, T), :] = u2p[h, y + 1, mid(), :]
            v[h, pl.ds(T, T), :] = ld[h, y] + u2p[h, inside + 1, mid(), :]
    order("px", qxe, qxo, qxl, qxh)
    order("px", vxe, vxo, vxl, vxh)
    order("py", vye, vyo, vyl, vyh)


def third_kernel(lp, own, qxl, qxh, gxe, gxo, hxl, hxh, lx, s0, s1, qye, qyo, gxl, gxh, qyl, qyh):
    order("px", gxl, gxh, gxe, gxo)
    lx2 = lx.reshape(HALVES * NB * CW, LANES)
    spread_x(lp, gxl, gxh, lx)
    for h in range(HALVES):
        for c, ref in ((8, gxl), (7, qxl), (7 + NB, gxh), (8 + NB, qxh)):
            col = rows(h * NB * CW + c, NB, CW)
            lx2[col, :] = lx2[col, :] + ref[h, pl.ds(QX_Q, NB), :]
        for i, s in enumerate((s0, s1)):
            for c, ref in ((0, gxl), (24, gxh)):
                s[h, pl.ds(c, 8), :] = ref[h, pl.ds(QX_S + 8 * i, 8), :]
            s[h, pl.ds(8, NB), :] = own[h, i]
        cut_wedges(lx, h, qyl, qyh)
        for i, s, q in ((0, s0, qyl), (1, s1, qyh)):
            y = i * (T - 1)
            q[h, pl.ds(QY_S, CW), :] = s[h]
            for j, (g1, g2) in enumerate(((hxl, gxl), (hxh, gxh))):
                q[h, pl.ds(QY_DIAG + 3 * j, 1), :] = g1[h, pl.ds(y, 1), :]
                q[h, pl.ds(QY_DIAG + 3 * j + 1, 1), :] = g1[h, pl.ds(2 * T + y, 1), :]
                q[h, pl.ds(QY_DIAG + 3 * j + 2, 1), :] = g2[h, pl.ds(QX_S + 8 * i + 7 * j, 1), :]
            q[h, pl.ds(QY_DIAG + 6, 2), :] = jnp.zeros((2, LANES), F)
    order("py", qye, qyo, qyl, qyh)


def rate_kernel(mx, gke, gko, bc, gkl, gkh):
    order("py", gkl, gkh, gke, gko)
    for h in range(HALVES):
        for i in range(1, DEPTH + 1):
            c, n, at = wedge(i)
            for r, gk in ((DEPTH - i, gkl), (DEPTH + NB - 1 + i, gkh)):
                bc[h, r, pl.ds(c, n), :] = 0.8 / (4.0 + gk[h, pl.ds(at, n), :])
        for y in range(NB):
            bc[h, DEPTH + y] = 0.8 / (4.0 + mx[h, y])


def coarse_kernel(
    lx, bc, s0, s1, gye, gyo, hxl, hxh, hyl, hyh, pxl, pxh,
    cv, bumps, gyl, gyh, lg, ca, cb,
):
    order("py", gyl, gyh, gye, gyo)
    one = lambda r: pl.ds(r, 1)
    for h in range(HALVES):
        for i in range(1, DEPTH + 1):
            c, n, at = wedge(i)
            for r, g in ((DEPTH - i, gyl), (DEPTH + NB - 1 + i, gyh)):
                lg[h, r, pl.ds(c, n), :] = g[h, pl.ds(at, n), :]
        for y in range(NB):
            lg[h, DEPTH + y] = lx[h, y]
        quarter = 1.0 / R
        for r, v in (
            (DEPTH - 1, s0[h]),
            (DEPTH, gyl[h, pl.ds(QY_S, CW), :]),
            (DEPTH + NB - 1, gyh[h, pl.ds(QY_S, CW), :]),
            (DEPTH + NB, s1[h]),
        ):
            lg[h, r] = lg[h, r] + quarter * v

    for h in range(HALVES):
        for j, (px, hx) in enumerate(((pxl, hxl), (pxh, hxh))):
            for i, (hy, gy) in enumerate(((hyl, gyl), (hyh, gyh))):
                y, x = (0, T - 1)[i], (0, T - 1)[j]
                ua, ba = px[h, one(y), :], px[h, one(2 * T + y), :]
                ux, bx = hx[h, one(y), :], hx[h, one(2 * T + y), :]
                uy, by = hy[h, one(x), :], hy[h, one(2 * T + x), :]
                ud, bd = gy[h, one(QY_DIAG + 3 * j), :], gy[h, one(QY_DIAG + 3 * j + 1), :]
                ea, ed = ba * (bx + by) * ud, bd * (bx + by) * ua
                ex, ey = bx * (ba + bd) * uy, by * (ba + bd) * ux
                ya, yo = (DEPTH, DEPTH - 1) if i == 0 else (DEPTH + NB - 1, DEPTH + NB)
                xa, xo = (8, 7) if j == 0 else (7 + NB, 8 + NB)
                for yy, xx, e, bb, e1, e2 in (
                    (ya, xa, ea, ba, ex, ey),
                    (ya, xo, ex, bx, ea, ed),
                    (yo, xa, ey, by, ea, ed),
                    (yo, xo, ed, bd, ex, ey),
                ):
                    lg[h, yy, one(xx), :] = lg[h, yy, one(xx), :] + quarter * (
                        (2.0 - 0.8 / bb) * e + (e1 + e2)
                    )
                at = 4 * (2 * i + j)
                for k, e in enumerate((ea, ex, ey, ed + gy[h, one(QY_DIAG + 3 * j + 2), :])):
                    bumps[h, one(at + k), :] = e

    own = pl.ds(8, CW)

    def start(h, y):
        v = bc[h, y] * lg[h, y]
        lg[h, y] = v
        ca[h, y, own, :] = v

    each_row(start, CR)
    old, new = ca, cb
    for s in range(1, INNER):

        def inner(y, c, old=old, new=new, end=s == INNER - 1):
            kept = []
            for h in range(HALVES):
                above, here = c[h]
                below = old[h, y + 1, own, :]
                near = (above + below) + (old[h, y, pl.ds(7, CW), :] + old[h, y, pl.ds(9, CW), :])
                value = (0.2 * here + lg[h, y]) + bc[h, y] * near
                if end:
                    cv[h, y] = value
                else:
                    new[h, y, own, :] = value
                kept.append((here, below))
            return tuple(kept)

        lax.fori_loop(
            s, CR - s, inner, tuple((old[h, s - 1, own, :], old[h, s, own, :]) for h in range(HALVES)), unroll=2
        )
        old, new = new, old


def last_kernel(
    cv, bumps, vxl, vxh, vye, vyo, hxl, hxh, hyl, hyh, u2p, b, ld,
    out, vyl, vyh, sp, w0, w1, wh, sh, sems,
):
    order("py", vyl, vyh, vye, vyo)
    one = lambda r: pl.ds(r, 1)
    bump = lambda h, i, j, k: bumps[h, one(4 * (2 * i + j) + k), :]
    cv2 = cv.reshape(HALVES * CR * CW, LANES)

    def correct(h, y):
        base = pl.multiple_of((h * NB + y) * T, T)
        c = cv[h, y + DEPTH, pl.ds(8, NB), :]
        for k in range(R):
            sp[rows(base + k, NB, R), :] = c
        add = sp[pl.ds(base, T), :]
        for k in range(R):
            w0[h, R * y + k + 1, mid(), :] = u2p[h, R * y + k + 1, mid(), :] + add

    each_row(correct, NB)

    w02, w12 = w0.reshape(HALVES * PLANE, LANES), w1.reshape(HALVES * PLANE, LANES)
    for h in range(HALVES):
        for i in range(2):
            for j in range(2):
                r, x = (1, T)[i], (8, T + 7)[j]
                w0[h, r, one(x), :] = w0[h, r, one(x), :] + bump(h, i, j, 0)
    U2, D, BH = pl.ds(0, T), pl.ds(T, T), pl.ds(2 * T, T)
    n = 0
    for h in range(HALVES):
        diag = {}
        for i in range(2):
            for j in range(2):
                diag[i, j] = (
                    bump(h, i, j, 3) + cv[h, (DEPTH - 1, DEPTH + NB)[i], one((7, 8 + NB)[j]), :]
                )
        for j, (g, hx) in enumerate(((vxl, hxl), (vxh, hxh))):
            c = cv2[rows(h * CR * CW + DEPTH * CW + (7, 8 + NB)[j], NB, CW), :]
            for k in range(R):
                sh[n, rows(k, NB, R), :] = c
            add = sh[n]
            wh[n, mid(), :] = g[h, U2, :] + add
            wh[n, one(7), :], wh[n, one(8 + T), :] = diag[0, j], diag[1, j]
            wh[n, one(8), :] = wh[n, one(8), :] + bump(h, 0, j, 1)
            wh[n, one(7 + T), :] = wh[n, one(7 + T), :] + bump(h, 1, j, 1)
            v = wh[n, mid(), :]
            x = (-1, T)[j]
            w02[column(h, x), :] = v
            w12[column(h, x), :] = 0.2 * v + hx[h, BH, :] * (
                (g[h, D, :] + add)
                + (wh[n, left(), :] + wh[n, right(), :])
                + w02[column(h, (0, T - 1)[j]), :]
            )
            n += 1
        for i, (g, hy) in enumerate(((vyl, hyl), (vyh, hyh))):
            c = cv[h, (DEPTH - 1, DEPTH + NB)[i], pl.ds(8, NB), :]
            for k in range(R):
                sh[n, rows(k, NB, R), :] = c
            add = sh[n]
            wh[n, mid(), :] = g[h, U2, :] + add
            wh[n, one(7), :], wh[n, one(8 + T), :] = diag[i, 0], diag[i, 1]
            wh[n, one(8), :] = wh[n, one(8), :] + bump(h, i, 0, 2)
            wh[n, one(7 + T), :] = wh[n, one(7 + T), :] + bump(h, i, 1, 2)
            v = wh[n, mid(), :]
            r = (0, T + 1)[i]
            w0[h, r, mid(), :] = v
            w1[h, r, mid(), :] = 0.2 * v + hy[h, BH, :] * (
                (g[h, D, :] + add)
                + (wh[n, left(), :] + wh[n, right(), :])
                + w0[h, (1, T)[i], mid(), :]
            )
            n += 1

    copies = []
    for h in range(HALVES):

        def one_more(y, c, near, h=h):
            w1[h, y + 1, mid(), :] = 0.2 * c + b[h, y] * (ld[h, y] + near)

        def last(y, c, near, h=h):
            w0[h, y + 1, mid(), :] = 0.2 * c + b[h, y] * (ld[h, y] + near)

        carried(h, 0, T, w0, one_more)
        step = T // 4
        for q in range(4):
            carried(h, q * step, (q + 1) * step, w1, last)
            copies.append(
                pltpu.make_async_copy(
                    w0.at[h, pl.ds(1 + q * step, step), mid(), :],
                    out.at[pl.ds(q * step, step), :, pl.ds(h * LANES, LANES)],
                    sems.at[h, q],
                )
            )
            copies[-1].start()
    for c in copies:
        c.wait()


def vmem(*shape):
    return pltpu.VMEM(shape, F)


V = pl.BlockSpec(memory_space=pltpu.VMEM)
H = pl.BlockSpec(memory_space=pltpu.HBM)


def swapped(axis, even, odd):
    size = lax.axis_size(axis)
    got = []
    if axis not in SWAPPED:
        up = [(i, (i + 1) % size) for i in range(size)]
        return lax.ppermute(odd, axis, up), lax.ppermute(even, axis, [(b, a) for a, b in up])
    for first, value in ((0, even), (1, odd)):
        pairs = []
        for k in range(first, size, 2):
            pairs += [(k, (k + 1) % size), ((k + 1) % size, k)]
        got.append(lax.ppermute(value, axis, pairs))
    return got


def estimate(flops, size):
    return pl.CostEstimate(flops=flops, bytes_accessed=size, transcendentals=0)


def per_device(load_terms, start_values, reaction_rate):
    tile, padded = (HALVES, T, T, LANES), (HALVES, PR, PC, LANES)
    coarse = (HALVES * NB * NB, LANES)
    edge = (HALVES, 3 * T, LANES)
    part = vmem(HALVES * NB * T, LANES)
    inputs = tuple(
        pltpu.with_memory_space_constraint(v, pltpu.HBM) for v in (load_terms, start_values, reaction_rate)
    )
    strip, line = vmem(HALVES, 2, T, 8, LANES), vmem(HALVES, 2, 1, T, LANES)
    pxl, pxh, pyl, pyh, pxe, pxo, pye, pyo = pl.pallas_call(
        edge_kernel,
        in_specs=[H] * 3,
        out_specs=[V] * 8,
        out_shape=[vmem(*edge)] * 8,
        scratch_shapes=[vmem(HALVES, 2, T + 2, 8, LANES), strip, strip, vmem(HALVES, 2, 2, PC, LANES), line, line]
        + [pltpu.SemaphoreType.DMA((HALVES, 2, 6))],
        compiler_params=pltpu.CompilerParams(vmem_limit_bytes=8 * MIB),
        name="edges",
    )(*inputs)
    hxe, hxo = swapped("px", pxe, pxo)
    hye, hyo = swapped("py", pye, pyo)
    u1p, b, ld, m, mo, kxe, kxo = pl.pallas_call(
        first_kernel,
        in_specs=[H] * 3,
        out_specs=[V] * 7,
        out_shape=[vmem(*padded)] + [vmem(*tile)] * 3 + [vmem(*coarse)] + [vmem(HALVES, KX, LANES)] * 2,
        scratch_shapes=[vmem(*padded), part]
        + [vmem(HALVES, KX, LANES)] * 2
        + [pltpu.SemaphoreType.DMA((3, HALVES, CHUNKS))],
        compiler_params=pltpu.CompilerParams(vmem_limit_bytes=12 * MIB),
        cost_estimate=estimate(10**7, 12 * MIB),
        name="first",
    )(*inputs)
    gme, gmo = swapped("px", kxe, kxo)
    outer = vmem(HALVES, 2 * T, LANES)
    u2p, part_sums = pl.pallas_call(
        bulk_kernel,
        in_specs=[V] * 4,
        out_specs=[V] * 2,
        out_shape=[vmem(*padded), part],
        compiler_params=pltpu.CompilerParams(vmem_limit_bytes=4 * MIB),
        cost_estimate=estimate(10**7, 12 * MIB),
        name="bulk",
    )(u1p, b, ld, m)
    _, u2p, _, lp, own, qxl, qxh, qxe, qxo, vxe, vxo, vye, vyo, hxl, hxh, hyl, hyh = pl.pallas_call(
        second_kernel,
        in_specs=[V] * 14,
        out_specs=[V] * 17,
        out_shape=[vmem(*padded)] * 2
        + [part, vmem(*coarse), vmem(HALVES, 2, NB, LANES)]
        + [vmem(HALVES, QX, LANES)] * 4
        + [outer] * 4
        + [vmem(*edge)] * 4,
        scratch_shapes=[outer] * 4,
        input_output_aliases={0: 0, 1: 1, 2: 2},
        compiler_params=pltpu.CompilerParams(vmem_limit_bytes=8 * MIB),
        name="second",
    )(u1p, u2p, part_sums, b, ld, m, pxl, pxh, pyl, pyh, hxe, hxo, hye, hyo)
    gxe, gxo = swapped("px", qxe, qxo)
    vxl, vxh = swapped("px", vxe, vxo)
    mx, kye, kyo = pl.pallas_call(
        mass_kernel,
        in_specs=[V] * 3,
        out_specs=[V] * 3,
        out_shape=[vmem(HALVES, NB, CW, LANES)] + [vmem(HALVES, KY, LANES)] * 2,
        scratch_shapes=[vmem(HALVES, KX, LANES)] * 2 + [vmem(HALVES, KY, LANES)] * 2,
        compiler_params=pltpu.CompilerParams(vmem_limit_bytes=8 * MIB),
        name="mass",
    )(mo, gme, gmo)
    gke, gko = swapped("py", kye, kyo)
    lx, s0, s1, qye, qyo = pl.pallas_call(
        third_kernel,
        in_specs=[V] * 8,
        out_specs=[V] * 5,
        out_shape=[vmem(HALVES, NB, CW, LANES)]
        + [vmem(HALVES, CW, LANES)] * 2
        + [vmem(HALVES, QY, LANES)] * 2,
        scratch_shapes=[vmem(HALVES, QX, LANES)] * 2 + [vmem(HALVES, QY, LANES)] * 2,
        compiler_params=pltpu.CompilerParams(vmem_limit_bytes=8 * MIB),
        name="third",
    )(lp, own, qxl, qxh, gxe, gxo, hxl, hxh)
    gye, gyo = swapped("py", qye, qyo)
    vye, vyo = swapped("py", vye, vyo)
    grid = vmem(HALVES, CR, CW, LANES)
    bc = pl.pallas_call(
        rate_kernel,
        in_specs=[V] * 3,
        out_specs=V,
        out_shape=grid,
        scratch_shapes=[vmem(HALVES, KY, LANES)] * 2,
        compiler_params=pltpu.CompilerParams(vmem_limit_bytes=8 * MIB),
        name="rate",
    )(mx, gke, gko)
    wide = vmem(HALVES, CR, CW + 16, LANES)
    cv, bumps = pl.pallas_call(
        coarse_kernel,
        in_specs=[V] * 12,
        out_specs=[V] * 2,
        out_shape=[grid, vmem(HALVES, 16, LANES)],
        scratch_shapes=[vmem(HALVES, QY, LANES)] * 2 + [grid, wide, wide],
        compiler_params=pltpu.CompilerParams(vmem_limit_bytes=8 * MIB),
        cost_estimate=estimate(10**7, 4 * MIB),
        name="coarse",
    )(lx, bc, s0, s1, gye, gyo, hxl, hxh, hyl, hyh, pxl, pxh)
    return pl.pallas_call(
        last_kernel,
        in_specs=[V] * 13,
        out_specs=H,
        out_shape=jax.ShapeDtypeStruct(load_terms.shape, F),
        scratch_shapes=[outer] * 2
        + [part, vmem(*padded), vmem(*padded)]
        + [vmem(8, PC, LANES), vmem(8, T, LANES), pltpu.SemaphoreType.DMA((HALVES, 4))],
        compiler_params=pltpu.CompilerParams(vmem_limit_bytes=20 * MIB),
        name="last",
    )(cv, bumps, vxl, vxh, vye, vyo, hxl, hxh, hyl, hyh, u2p, b, ld)


def solution(mesh):
    return jax.shard_map(
        per_device,
        mesh=mesh,
        in_specs=(P("py", "px", None), P("py", "px", None), P("py", "px", None)),
        out_specs=P("py", "px", None),
        check_vma=False,
    )
```

```python
import jax
import jax.numpy as jnp
from jax import lax
from jax.experimental import pallas as pl
from jax.experimental.pallas import tpu as pltpu
from jax.sharding import PartitionSpec as P

F = jnp.float32
T = 64
R = 4
NB = T // R
INNER = 7
DEPTH = INNER
LANES = 128
HALVES = 2
PR, PC = T + 2, T + 16
PLANE = PR * PC
CW = 32
CR = NB + 2 * DEPTH
KX = DEPTH * NB
KY = sum(CW - 2 * i for i in range(1, DEPTH + 1))
QX_S, QX_Q = KX, KX + 16
QX = QX_Q + NB
QY_S, QY_DIAG = KY, KY + CW
QY = QY_DIAG + 8
MIB = 2**20


def rows(start, size, stride=1):
    return pl.ds(start, size, stride=stride)


def mid():
    return pl.ds(8, T)


def left():
    return pl.ds(7, T)


def right():
    return pl.ds(9, T)


def around(ref, h, y):
    return (ref[h, y, mid(), :] + ref[h, y + 2, mid(), :]) + (
        ref[h, y + 1, left(), :] + ref[h, y + 1, right(), :]
    )


def each_row(body, n=T, unroll=2):
    for h in range(HALVES):
        lax.fori_loop(0, n, lambda y, c, h=h: (body(h, y), c)[1], 0, unroll=unroll)


def carried(h, first, last, src, point, unroll=2):
    def body(y, c):
        above, here = c
        below = src[h, y + 2, mid(), :]
        point(y, here, (above + below) + (src[h, y + 1, left(), :] + src[h, y + 1, right(), :]))
        return here, below

    lax.fori_loop(first, last, body, (src[h, first, mid(), :], src[h, first + 1, mid(), :]), unroll=unroll)


def clear_border(ref):
    for h in range(HALVES):
        ref[h, 0] = jnp.zeros((PC, LANES), F)
        ref[h, PR - 1] = jnp.zeros((PC, LANES), F)
        for x in (0, PC - 8):
            ref[h, pl.ds(1, T), pl.ds(x, 8), :] = jnp.zeros((T, 8, LANES), F)


def column(h, x):
    return rows(h * PLANE + PC + 8 + x, T, PC)


SWAPPED = ("py",)


def is_even(axis):
    return lax.rem(lax.axis_index(axis), 2) == 0


def order(axis, first, second, a, b):
    even = is_even(axis) if axis in SWAPPED else False
    n = first.shape[1]
    for h in range(HALVES):
        for r in range(0, n, T):
            part = pl.ds(r, min(T, n - r))
            va, vb = a[h, part, :], b[h, part, :]
            first[h, part, :] = va if even is False else jnp.where(even, vb, va)
            second[h, part, :] = vb if even is False else jnp.where(even, va, vb)


def block_sums(part, out):
    n = HALVES * NB * NB

    def body(j, c):
        total = part[rows(j * 4 * T, T, R), :]
        for k in range(1, R):
            total = total + part[rows(j * 4 * T + k, T, R), :]
        out[pl.ds(j * T, T), :] = total * (1.0 / R)
        return c

    lax.fori_loop(0, n // T, body, 0)


def column_edges(load_h, u_h, m_h, pxl, pxh, pxe, pxo, uc, lc, mc, sems):
    copies = []
    for h in range(HALVES):
        lanes = pl.ds(h * LANES, LANES)
        for i in range(2):
            x = (0, T - 8)[i]
            for n, (src, dst) in enumerate(
                (
                    (u_h.at[:, pl.ds(x, 8), lanes], uc.at[h, i, pl.ds(1, T)]),
                    (load_h.at[:, pl.ds(x, 8), lanes], lc.at[h, i]),
                    (m_h.at[:, pl.ds(x, 8), lanes], mc.at[h, i]),
                )
            ):
                copies.append(pltpu.make_async_copy(src, dst, sems.at[h, i, n]))
    for c in copies:
        c.start()
    for h in range(HALVES):
        for i in range(2):
            uc[h, i, 0] = jnp.zeros((8, LANES), F)
            uc[h, i, T + 1] = jnp.zeros((8, LANES), F)
    for c in copies:
        c.wait()
    uc2 = uc.reshape(HALVES * 2 * (T + 2) * 8, LANES)
    lc2, mc2 = lc.reshape(HALVES * 2 * T * 8, LANES), mc.reshape(HALVES * 2 * T * 8, LANES)
    for h in range(HALVES):
        for i in range(2):
            px = (pxl, pxh)[i]
            ub, lb = (h * 2 + i) * (T + 2) * 8, (h * 2 + i) * T * 8
            x, xi = (0, 7)[i], (1, 6)[i]
            u = uc2[rows(ub + 8 + x, T, 8), :]
            bb = 0.8 / (4.0 + mc2[rows(lb + x, T, 8), :])
            near = uc2[rows(ub + 8 + xi, T, 8), :] + (uc2[rows(ub + x, T, 8), :] + uc2[rows(ub + 16 + x, T, 8), :])
            px[h, pl.ds(0, T), :] = u
            px[h, pl.ds(T, T), :] = 0.2 * u + bb * (lc2[rows(lb + x, T, 8), :] + near)
            px[h, pl.ds(2 * T, T), :] = bb
    order("px", pxe, pxo, pxl, pxh)


def row_edges(load_h, u_h, m_h, pyl, pyh, pye, pyo, ur, lr, mr, sems):
    copies = []
    for h in range(HALVES):
        lanes = pl.ds(h * LANES, LANES)
        for i in range(2):
            y, yy = (0, T - 1)[i], (0, T - 2)[i]
            for n, (src, dst) in enumerate(
                (
                    (u_h.at[pl.ds(yy, 2), :, lanes], ur.at[h, i, :, mid(), :]),
                    (load_h.at[pl.ds(y, 1), :, lanes], lr.at[h, i]),
                    (m_h.at[pl.ds(y, 1), :, lanes], mr.at[h, i]),
                )
            ):
                copies.append(pltpu.make_async_copy(src, dst, sems.at[h, i, n]))
    for c in copies:
        c.start()
    for h in range(HALVES):
        for i in range(2):
            for k in range(2):
                ur[h, i, k, pl.ds(0, 8), :] = jnp.zeros((8, LANES), F)
                ur[h, i, k, pl.ds(8 + T, 8), :] = jnp.zeros((8, LANES), F)
    for c in copies:
        c.wait()
    for h in range(HALVES):
        for k in range(2):
            py = (pyl, pyh)[k]
            u = ur[h, k, k, mid(), :]
            bb = 0.8 / (4.0 + mr[h, k, 0])
            near = ur[h, k, 1 - k, mid(), :] + (ur[h, k, k, left(), :] + ur[h, k, k, right(), :])
            py[h, pl.ds(0, T), :] = u
            py[h, pl.ds(T, T), :] = 0.2 * u + bb * (lr[h, k, 0] + near)
            py[h, pl.ds(2 * T, T), :] = bb
    order("py", pye, pyo, pyl, pyh)


CHUNKS = 4


def first_kernel(load_h, u_h, m_h, u1p, b, ld, m, mo, kxe, kxo, up, part, kxl, kxh, sems):
    step = T // CHUNKS
    copies = {}
    for h in range(HALVES):
        lanes = pl.ds(h * LANES, LANES)
        for q in range(CHUNKS):
            y = pl.ds(q * step, step)
            copies[h, q] = [
                pltpu.make_async_copy(m_h.at[y, :, lanes], m.at[h, y], sems.at[0, h, q]),
                pltpu.make_async_copy(
                    u_h.at[y, :, lanes], up.at[h, pl.ds(q * step + 1, step), pl.ds(8, T), :], sems.at[1, h, q]
                ),
                pltpu.make_async_copy(load_h.at[y, :, lanes], ld.at[h, y], sems.at[2, h, q]),
            ]
            for c in copies[h, q]:
                c.start()
    clear_border(up)

    for h in range(HALVES):

        def sweep(y, c, h=h):
            bb = 0.8 / (4.0 + m[h, y])
            b[h, y] = bb
            u1p[h, y + 1, mid(), :] = 0.2 * up[h, y + 1, mid(), :] + bb * (ld[h, y] + around(up, h, y))
            return c

        def sums(y, c, h=h):
            part[pl.ds(pl.multiple_of((h * NB + y) * T, T), T), :] = (m[h, R * y] + m[h, R * y + 1]) + (
                m[h, R * y + 2] + m[h, R * y + 3]
            )
            return c

        for q in range(CHUNKS):
            for c in copies[h, q]:
                c.wait()
            lax.fori_loop(q * step // R, (q + 1) * step // R, sums, 0, unroll=2)
            lax.fori_loop(max(q * step - 1, 0), T if q == CHUNKS - 1 else (q + 1) * step - 1, sweep, 0, unroll=2 if q else 1)
    block_sums(part, mo)
    for h in range(HALVES):
        for first, q in ((0, kxl), (NB - DEPTH, kxh)):
            for k in range(DEPTH):
                q[h, pl.ds(k * NB, NB), :] = mo[rows(h * NB * NB + first + k, NB, NB), :]
    order("px", kxe, kxo, kxl, kxh)


def spread_x(inner, low, high, ext):
    ext2 = ext.reshape(HALVES * NB * CW, LANES)
    for h in range(HALVES):
        for y in range(NB):
            ext[h, y, pl.ds(8, NB), :] = inner[pl.ds(h * NB * NB + y * NB, NB), :]
        for c, g in ((1, low), (8 + NB, high)):
            for k in range(DEPTH):
                ext2[rows(h * NB * CW + c + k, NB, CW), :] = g[h, pl.ds(k * NB, NB), :]


def wedge(i):
    return i, CW - 2 * i, sum(CW - 2 * k for k in range(1, i))


def cut_wedges(ext, h, low, high):
    for i in range(1, DEPTH + 1):
        c, n, at = wedge(i)
        low[h, pl.ds(at, n), :] = ext[h, i - 1, pl.ds(c, n), :]
        high[h, pl.ds(at, n), :] = ext[h, NB - i, pl.ds(c, n), :]


def mass_kernel(mo, gme, gmo, mx, kye, kyo, gml, gmh, kyl, kyh):
    order("px", gml, gmh, gme, gmo)
    spread_x(mo, gml, gmh, mx)
    for h in range(HALVES):
        cut_wedges(mx, h, kyl, kyh)
    order("py", kye, kyo, kyl, kyh)


def bulk_kernel(u1p, b, ld, m, u2p, part):
    clear_border(u2p)
    for h in range(HALVES):

        def sweep(y, c, near, h=h):
            u2p[h, y + 1, mid(), :] = 0.2 * c + b[h, y] * (ld[h, y] + near)

        carried(h, 0, T, u1p, sweep)
    each_row(lambda h, y: defect_rows(h, y, u2p, ld, m, part), NB, unroll=1)


def defect_rows(h, y, u2p, ld, m, part):
    total = None
    for k in range(R):
        c = R * y + k
        d = (ld[h, c] + around(u2p, h, c)) - (4.0 + m[h, c]) * u2p[h, c + 1, mid(), :]
        total = d if total is None else total + d
    part[pl.ds(pl.multiple_of((h * NB + y) * T, T), T), :] = total


def near_tile(ref, h, y, x):
    return (ref[h, pl.ds(y, 8), pl.ds(x + 8, 8), :] + ref[h, pl.ds(y + 2, 8), pl.ds(x + 8, 8), :]) + (
        ref[h, pl.ds(y + 1, 8), pl.ds(x + 7, 8), :] + ref[h, pl.ds(y + 1, 8), pl.ds(x + 9, 8), :]
    )


def second_kernel(
    u1p_in, u2p_in, part_in, b, ld, m, pxl, pxh, pyl, pyh, hxe, hxo, hye, hyo,
    u1p, u2p, part, lp, own, qxl, qxh, qxe, qxo, vxe, vxo, vye, vyo, hxl, hxh, hyl, hyh,
    vxl, vxh, vyl, vyh,
):
    del u1p_in, u2p_in, part_in
    order("px", hxl, hxh, hxe, hxo)
    order("py", hyl, hyh, hye, hyo)
    u1p2 = u1p.reshape(HALVES * PLANE, LANES)
    U, A, B = pl.ds(0, T), pl.ds(T, T), pl.ds(2 * T, T)
    for h in range(HALVES):
        for x, p, g in ((0, pxl, hxl), (T - 1, pxh, hxh)):
            inner = column(h, x)
            outer = column(h, -1 if x == 0 else T)
            u1p2[inner, :] = u1p2[inner, :] + p[h, B, :] * g[h, U, :]
            u1p2[outer, :] = g[h, A, :] + g[h, B, :] * p[h, U, :]
        for y, p, g in ((0, pyl, hyl), (T - 1, pyh, hyh)):
            u1p[h, y + 1, mid(), :] = u1p[h, y + 1, mid(), :] + p[h, B, :] * g[h, U, :]
            u1p[h, 0 if y == 0 else T + 1, mid(), :] = g[h, A, :] + g[h, B, :] * p[h, U, :]

    for h in range(HALVES):
        for y in (0, 1, T - 2, T - 1):
            u2p[h, y + 1, mid(), :] = 0.2 * u1p[h, y + 1, mid(), :] + b[h, y] * (ld[h, y] + around(u1p, h, y))

    def sweep(j, c):
        y = pl.multiple_of(j * 8, 8)
        for h in range(HALVES):
            for x in (0, T - 8):
                here = (h, pl.ds(y + 1, 8), pl.ds(8 + x, 8))
                tile = (h, pl.ds(y, 8), pl.ds(x, 8))
                u2p[here] = 0.2 * u1p[here] + b[tile] * (ld[tile] + near_tile(u1p, h, y, x))
        return c

    lax.fori_loop(0, T // 8, sweep, 0)

    def sums(j, c):
        y = pl.multiple_of(j * 8, 8)
        for h in range(HALVES):
            for x in (0, T - 8):
                here = (h, pl.ds(y + 1, 8), pl.ds(8 + x, 8))
                tile = (h, pl.ds(y, 8), pl.ds(x, 8))
                d = (ld[tile] + near_tile(u2p, h, y, x)) - (4.0 + m[tile]) * u2p[here]
                for k in range(2):
                    at = pl.multiple_of((h * NB + 2 * j + k) * T, T) + x
                    part[pl.ds(at, 8), :] = (d[R * k] + d[R * k + 1]) + (d[R * k + 2] + d[R * k + 3])
        return c

    lax.fori_loop(0, T // 8, sums, 0)
    for h in range(HALVES):
        for y in (0, NB - 1):
            defect_rows(h, y, u2p, ld, m, part)
    block_sums(part, lp)

    u2p2, ld2 = u2p.reshape(HALVES * PLANE, LANES), ld.reshape(HALVES * T * T, LANES)
    for h in range(HALVES):
        for x, first, s, q, v in ((0, 0, 0, qxl, vxl), (T - 1, NB - DEPTH, 8, qxh, vxh)):
            for k in range(DEPTH):
                q[h, pl.ds(k * NB, NB), :] = lp[rows(h * NB * NB + first + k, NB, NB), :]
            for i, y in enumerate((0, T - 1)):
                total = None
                for k in range(R):
                    e = u2p2[rows(h * PLANE + (y + 1) * PC + 8 + R * s + k, 8, R), :]
                    total = e if total is None else total + e
                q[h, pl.ds(QX_S + 8 * i, 8), :] = total
                own[h, i, pl.ds(s, 8), :] = total
                free = QX_S + 8 * i + (7 if x == 0 else 0)
                q[h, pl.ds(free, 1), :] = u2p[h, y + 1, pl.ds(8 + x, 1), :]
            total = None
            for k in range(R):
                e = u2p2[rows(h * PLANE + (k + 1) * PC + 8 + x, NB, R * PC), :]
                total = e if total is None else total + e
            q[h, pl.ds(QX_Q, NB), :] = total * (1.0 / R)
            v[h, pl.ds(0, T), :] = u2p2[column(h, x), :]
            v[h, pl.ds(T, T), :] = ld2[rows(h * T * T + x, T, T), :] + u2p2[column(h, 1 if x == 0 else T - 2), :]
        for y, inside, v in ((0, 1, vyl), (T - 1, T - 2, vyh)):
            v[h, pl.ds(0, T), :] = u2p[h, y + 1, mid(), :]
            v[h, pl.ds(T, T), :] = ld[h, y] + u2p[h, inside + 1, mid(), :]
    order("px", qxe, qxo, qxl, qxh)
    order("px", vxe, vxo, vxl, vxh)
    order("py", vye, vyo, vyl, vyh)


def third_kernel(lp, own, qxl, qxh, gxe, gxo, hxl, hxh, lx, s0, s1, qye, qyo, gxl, gxh, qyl, qyh):
    order("px", gxl, gxh, gxe, gxo)
    lx2 = lx.reshape(HALVES * NB * CW, LANES)
    spread_x(lp, gxl, gxh, lx)
    for h in range(HALVES):
        for c, ref in ((8, gxl), (7, qxl), (7 + NB, gxh), (8 + NB, qxh)):
            col = rows(h * NB * CW + c, NB, CW)
            lx2[col, :] = lx2[col, :] + ref[h, pl.ds(QX_Q, NB), :]
        for i, s in enumerate((s0, s1)):
            for c, ref in ((0, gxl), (24, gxh)):
                s[h, pl.ds(c, 8), :] = ref[h, pl.ds(QX_S + 8 * i, 8), :]
            s[h, pl.ds(8, NB), :] = own[h, i]
        cut_wedges(lx, h, qyl, qyh)
        for i, s, q in ((0, s0, qyl), (1, s1, qyh)):
            y = i * (T - 1)
            q[h, pl.ds(QY_S, CW), :] = s[h]
            for j, (g1, g2) in enumerate(((hxl, gxl), (hxh, gxh))):
                q[h, pl.ds(QY_DIAG + 3 * j, 1), :] = g1[h, pl.ds(y, 1), :]
                q[h, pl.ds(QY_DIAG + 3 * j + 1, 1), :] = g1[h, pl.ds(2 * T + y, 1), :]
                q[h, pl.ds(QY_DIAG + 3 * j + 2, 1), :] = g2[h, pl.ds(QX_S + 8 * i + 7 * j, 1), :]
            q[h, pl.ds(QY_DIAG + 6, 2), :] = jnp.zeros((2, LANES), F)
    order("py", qye, qyo, qyl, qyh)


def rate_kernel(mx, gke, gko, bc, gkl, gkh):
    order("py", gkl, gkh, gke, gko)
    for h in range(HALVES):
        for i in range(1, DEPTH + 1):
            c, n, at = wedge(i)
            for r, gk in ((DEPTH - i, gkl), (DEPTH + NB - 1 + i, gkh)):
                bc[h, r, pl.ds(c, n), :] = 0.8 / (4.0 + gk[h, pl.ds(at, n), :])
        for y in range(NB):
            bc[h, DEPTH + y] = 0.8 / (4.0 + mx[h, y])


def coarse_kernel(
    lx, bc, s0, s1, gye, gyo, hxl, hxh, hyl, hyh, pxl, pxh, b, w1_in,
    w1, sp, bumps, gyl, gyh, lg, ca, cb, cv,
):
    del w1_in
    order("py", gyl, gyh, gye, gyo)
    one = lambda r: pl.ds(r, 1)
    for h in range(HALVES):
        for i in range(1, DEPTH + 1):
            c, n, at = wedge(i)
            for r, g in ((DEPTH - i, gyl), (DEPTH + NB - 1 + i, gyh)):
                lg[h, r, pl.ds(c, n), :] = g[h, pl.ds(at, n), :]
        for y in range(NB):
            lg[h, DEPTH + y] = lx[h, y]
        quarter = 1.0 / R
        for r, v in (
            (DEPTH - 1, s0[h]),
            (DEPTH, gyl[h, pl.ds(QY_S, CW), :]),
            (DEPTH + NB - 1, gyh[h, pl.ds(QY_S, CW), :]),
            (DEPTH + NB, s1[h]),
        ):
            lg[h, r] = lg[h, r] + quarter * v

    for h in range(HALVES):
        for j, (px, hx) in enumerate(((pxl, hxl), (pxh, hxh))):
            for i, (hy, gy) in enumerate(((hyl, gyl), (hyh, gyh))):
                y, x = (0, T - 1)[i], (0, T - 1)[j]
                ua, ba = px[h, one(y), :], px[h, one(2 * T + y), :]
                ux, bx = hx[h, one(y), :], hx[h, one(2 * T + y), :]
                uy, by = hy[h, one(x), :], hy[h, one(2 * T + x), :]
                ud, bd = gy[h, one(QY_DIAG + 3 * j), :], gy[h, one(QY_DIAG + 3 * j + 1), :]
                ea, ed = ba * (bx + by) * ud, bd * (bx + by) * ua
                ex, ey = bx * (ba + bd) * uy, by * (ba + bd) * ux
                ya, yo = (DEPTH, DEPTH - 1) if i == 0 else (DEPTH + NB - 1, DEPTH + NB)
                xa, xo = (8, 7) if j == 0 else (7 + NB, 8 + NB)
                for yy, xx, e, bb, e1, e2 in (
                    (ya, xa, ea, ba, ex, ey),
                    (ya, xo, ex, bx, ea, ed),
                    (yo, xa, ey, by, ea, ed),
                    (yo, xo, ed, bd, ex, ey),
                ):
                    lg[h, yy, one(xx), :] = lg[h, yy, one(xx), :] + quarter * (
                        (2.0 - 0.8 / bb) * e + (e1 + e2)
                    )
                at = 4 * (2 * i + j)
                for k, e in enumerate((ea, ex, ey, ed + gy[h, one(QY_DIAG + 3 * j + 2), :])):
                    bumps[h, one(at + k), :] = e

    own = pl.ds(8, CW)

    def start(h, y):
        v = bc[h, y] * lg[h, y]
        lg[h, y] = v
        ca[h, y, own, :] = v

    each_row(start, CR)
    old, new = ca, cb
    for s in range(1, INNER):

        def inner(y, c, old=old, new=new, end=s == INNER - 1):
            kept = []
            for h in range(HALVES):
                above, here = c[h]
                below = old[h, y + 1, own, :]
                near = (above + below) + (old[h, y, pl.ds(7, CW), :] + old[h, y, pl.ds(9, CW), :])
                value = (0.2 * here + lg[h, y]) + bc[h, y] * near
                if end:
                    cv[h, y] = value
                else:
                    new[h, y, own, :] = value
                kept.append((here, below))
            return tuple(kept)

        lax.fori_loop(
            s, CR - s, inner, tuple((old[h, s - 1, own, :], old[h, s, own, :]) for h in range(HALVES)), unroll=2
        )
        old, new = new, old

    for h in range(HALVES):
        for y in range(NB + 2):
            c = cv[h, y + DEPTH - 1, pl.ds(6, NB + 4), :]
            for k in range(R):
                sp[h, y, rows(k, NB + 4, R), :] = c

    def correct(h, y):
        c = sp[h, y + 1, mid(), :]
        sides = sp[h, y + 1, left(), :] + sp[h, y + 1, right(), :]
        above, below = sp[h, y, mid(), :], sp[h, y + 2, mid(), :]
        base = 0.2 * c
        inside = sides + (c + c)
        for k, near in ((0, sides + (c + above)), (1, inside), (2, inside), (3, sides + (c + below))):
            r = R * y + k
            w1[h, r + 1, mid(), :] = w1[h, r + 1, mid(), :] + (base + b[h, r] * near)

    each_row(correct, NB, unroll=1)


def ahead_kernel(u2p, b, ld, w1):
    for h in range(HALVES):

        def sweep(y, c, near, h=h):
            w1[h, y + 1, mid(), :] = 0.2 * c + b[h, y] * (ld[h, y] + near)

        carried(h, 0, T, u2p, sweep)


def last_kernel(
    w1_in, sp, bumps, vxl, vxh, vye, vyo, hxl, hxh, hyl, hyh, u2p, b, ld,
    w1, out, vyl, vyh, w0, wh, sh, oh, sems,
):
    del w1_in
    order("py", vyl, vyh, vye, vyo)
    one = lambda r: pl.ds(r, 1)
    bump = lambda h, i, j, k: bumps[h, one(4 * (2 * i + j) + k), :]
    stride = (NB + 2) * PC
    sp2, b2 = sp.reshape(HALVES * stride, LANES), b.reshape(HALVES * T * T, LANES)
    w12, u2p2 = w1.reshape(HALVES * PLANE, LANES), u2p.reshape(HALVES * PLANE, LANES)
    U2, D, BH = pl.ds(0, T), pl.ds(T, T), pl.ds(2 * T, T)
    n = 0
    for h in range(HALVES):
        for i in range(2):
            for j in range(2):
                e, y, x = bump(h, i, j, 0), (0, T - 1)[i], (0, T - 1)[j]
                yi, xi = (1, T - 2)[i], (1, T - 2)[j]
                for yy, xx, f in ((y, x, None), (y, xi, b), (yi, x, b)):
                    f = 0.2 if f is None else b[h, yy, one(xx), :]
                    w1[h, yy + 1, one(xx + 8), :] = w1[h, yy + 1, one(xx + 8), :] + f * e
        diag = {
            (i, j): bump(h, i, j, 3) + sp[h, (0, NB + 1)[i], one((7, 8 + T)[j]), :] for i in range(2) for j in range(2)
        }

        def ring(n, v, bh, c, here, to, ends, corners, h=h):
            wh[n, mid(), :] = v[h, U2, :]
            for r, (outside, inside) in zip((0, T - 1), ends):
                wh[n, one(8 + r), :] = wh[n, one(8 + r), :] + outside
                oh[n, one(r), :] = oh[n, one(r), :] + inside
            u2h = wh[n, mid(), :]
            w0h = u2h + c
            wh[n, mid(), :] = w0h
            wh[n, one(7), :], wh[n, one(8 + T), :] = corners
            near = (wh[n, left(), :] + wh[n, right(), :]) + oh[n]
            here(u2h)
            to(0.2 * w0h + bh * ((v[h, D, :] + c) + near))

        for j, (v, hx) in enumerate(((vxl, hxl), (vxh, hxh))):
            x, xo = (0, T - 1)[j], (-1, T)[j]
            for k in range(R):
                sh[n, 0, rows(k, NB, R), :] = sp2[rows(h * stride + PC + 8 + xo, NB, PC), :]
                sh[n, 1, rows(k, NB, R), :] = sp2[rows(h * stride + PC + 8 + x, NB, PC), :]
            oh[n] = u2p2[column(h, x), :] + sh[n, 1]

            def here(u2h, h=h, x=x):
                at = column(h, x)
                w12[at, :] = w12[at, :] + b2[rows(h * T * T + x, T, T), :] * u2h

            def to(value, h=h, xo=xo):
                w12[column(h, xo), :] = value

            ring(
                n, v, hx[h, BH, :], sh[n, 0], here, to,
                [(bump(h, i, j, 1), bump(h, i, j, 0)) for i in range(2)], (diag[0, j], diag[1, j]),
            )
            n += 1
        for i, (v, hy) in enumerate(((vyl, hyl), (vyh, hyh))):
            y = (0, T - 1)[i]
            oh[n] = u2p[h, y + 1, mid(), :] + sp[h, (1, NB)[i], mid(), :]

            def here(u2h, h=h, y=y):
                w1[h, y + 1, mid(), :] = w1[h, y + 1, mid(), :] + b[h, y] * u2h

            def to(value, h=h, i=i):
                w1[h, (0, T + 1)[i], mid(), :] = value

            ring(
                n, v, hy[h, BH, :], sp[h, (0, NB + 1)[i], mid(), :], here, to,
                [(bump(h, i, j, 2), bump(h, i, j, 0)) for j in range(2)], (diag[i, 0], diag[i, 1]),
            )
            n += 1

    copies = []
    for h in range(HALVES):

        def last(y, c, near, h=h):
            w0[h, y + 1, mid(), :] = 0.2 * c + b[h, y] * (ld[h, y] + near)

        step = T // 4
        for q in range(4):
            carried(h, q * step, (q + 1) * step, w1, last)
            copies.append(
                pltpu.make_async_copy(
                    w0.at[h, pl.ds(1 + q * step, step), mid(), :],
                    out.at[pl.ds(q * step, step), :, pl.ds(h * LANES, LANES)],
                    sems.at[h, q],
                )
            )
            copies[-1].start()
    for c in copies:
        c.wait()


def vmem(*shape):
    return pltpu.VMEM(shape, F)


V = pl.BlockSpec(memory_space=pltpu.VMEM)
H = pl.BlockSpec(memory_space=pltpu.HBM)


def swapped(axis, even, odd):
    size = lax.axis_size(axis)
    got = []
    if axis not in SWAPPED:
        up = [(i, (i + 1) % size) for i in range(size)]
        return lax.ppermute(odd, axis, up), lax.ppermute(even, axis, [(b, a) for a, b in up])
    for first, value in ((0, even), (1, odd)):
        pairs = []
        for k in range(first, size, 2):
            pairs += [(k, (k + 1) % size), ((k + 1) % size, k)]
        got.append(lax.ppermute(value, axis, pairs))
    return got


def estimate(flops, size):
    return pl.CostEstimate(flops=flops, bytes_accessed=size, transcendentals=0)


def per_device(load_terms, start_values, reaction_rate):
    tile, padded = (HALVES, T, T, LANES), (HALVES, PR, PC, LANES)
    coarse = (HALVES * NB * NB, LANES)
    edge = (HALVES, 3 * T, LANES)
    part = vmem(HALVES * NB * T, LANES)
    inputs = tuple(
        pltpu.with_memory_space_constraint(v, pltpu.HBM) for v in (load_terms, start_values, reaction_rate)
    )
    strip, line = vmem(HALVES, 2, T, 8, LANES), vmem(HALVES, 2, 1, T, LANES)
    pyl, pyh, pye, pyo = pl.pallas_call(
        row_edges,
        in_specs=[H] * 3,
        out_specs=[V] * 4,
        out_shape=[vmem(*edge)] * 4,
        scratch_shapes=[vmem(HALVES, 2, 2, PC, LANES), line, line, pltpu.SemaphoreType.DMA((HALVES, 2, 3))],
        compiler_params=pltpu.CompilerParams(vmem_limit_bytes=4 * MIB),
        name="rowedges",
    )(*inputs)
    hye, hyo = swapped("py", pye, pyo)
    pxl, pxh, pxe, pxo = pl.pallas_call(
        column_edges,
        in_specs=[H] * 3,
        out_specs=[V] * 4,
        out_shape=[vmem(*edge)] * 4,
        scratch_shapes=[vmem(HALVES, 2, T + 2, 8, LANES), strip, strip, pltpu.SemaphoreType.DMA((HALVES, 2, 3))],
        compiler_params=pltpu.CompilerParams(vmem_limit_bytes=8 * MIB),
        name="columnedges",
    )(*inputs)
    hxe, hxo = swapped("px", pxe, pxo)
    u1p, b, ld, m, mo, kxe, kxo = pl.pallas_call(
        first_kernel,
        in_specs=[H] * 3,
        out_specs=[V] * 7,
        out_shape=[vmem(*padded)] + [vmem(*tile)] * 3 + [vmem(*coarse)] + [vmem(HALVES, KX, LANES)] * 2,
        scratch_shapes=[vmem(*padded), part]
        + [vmem(HALVES, KX, LANES)] * 2
        + [pltpu.SemaphoreType.DMA((3, HALVES, CHUNKS))],
        compiler_params=pltpu.CompilerParams(vmem_limit_bytes=12 * MIB),
        cost_estimate=estimate(10**7, 12 * MIB),
        name="first",
    )(*inputs)
    gme, gmo = swapped("px", kxe, kxo)
    outer = vmem(HALVES, 2 * T, LANES)
    u2p, part_sums = pl.pallas_call(
        bulk_kernel,
        in_specs=[V] * 4,
        out_specs=[V] * 2,
        out_shape=[vmem(*padded), part],
        compiler_params=pltpu.CompilerParams(vmem_limit_bytes=4 * MIB),
        cost_estimate=estimate(10**7, 12 * MIB),
        name="bulk",
    )(u1p, b, ld, m)
    _, u2p, _, lp, own, qxl, qxh, qxe, qxo, vxe, vxo, vye, vyo, hxl, hxh, hyl, hyh = pl.pallas_call(
        second_kernel,
        in_specs=[V] * 14,
        out_specs=[V] * 17,
        out_shape=[vmem(*padded)] * 2
        + [part, vmem(*coarse), vmem(HALVES, 2, NB, LANES)]
        + [vmem(HALVES, QX, LANES)] * 4
        + [outer] * 4
        + [vmem(*edge)] * 4,
        scratch_shapes=[outer] * 4,
        input_output_aliases={0: 0, 1: 1, 2: 2},
        compiler_params=pltpu.CompilerParams(vmem_limit_bytes=8 * MIB),
        name="second",
    )(u1p, u2p, part_sums, b, ld, m, pxl, pxh, pyl, pyh, hxe, hxo, hye, hyo)
    gxe, gxo = swapped("px", qxe, qxo)
    vxl, vxh = swapped("px", vxe, vxo)
    mx, kye, kyo = pl.pallas_call(
        mass_kernel,
        in_specs=[V] * 3,
        out_specs=[V] * 3,
        out_shape=[vmem(HALVES, NB, CW, LANES)] + [vmem(HALVES, KY, LANES)] * 2,
        scratch_shapes=[vmem(HALVES, KX, LANES)] * 2 + [vmem(HALVES, KY, LANES)] * 2,
        compiler_params=pltpu.CompilerParams(vmem_limit_bytes=8 * MIB),
        name="mass",
    )(mo, gme, gmo)
    gke, gko = swapped("py", kye, kyo)
    lx, s0, s1, qye, qyo = pl.pallas_call(
        third_kernel,
        in_specs=[V] * 8,
        out_specs=[V] * 5,
        out_shape=[vmem(HALVES, NB, CW, LANES)]
        + [vmem(HALVES, CW, LANES)] * 2
        + [vmem(HALVES, QY, LANES)] * 2,
        scratch_shapes=[vmem(HALVES, QX, LANES)] * 2 + [vmem(HALVES, QY, LANES)] * 2,
        compiler_params=pltpu.CompilerParams(vmem_limit_bytes=8 * MIB),
        name="third",
    )(lp, own, qxl, qxh, gxe, gxo, hxl, hxh)
    gye, gyo = swapped("py", qye, qyo)
    vye, vyo = swapped("py", vye, vyo)
    grid = vmem(HALVES, CR, CW, LANES)
    bc = pl.pallas_call(
        rate_kernel,
        in_specs=[V] * 3,
        out_specs=V,
        out_shape=grid,
        scratch_shapes=[vmem(HALVES, KY, LANES)] * 2,
        compiler_params=pltpu.CompilerParams(vmem_limit_bytes=8 * MIB),
        name="rate",
    )(mx, gke, gko)
    wide = vmem(HALVES, CR, CW + 16, LANES)
    u3 = pl.pallas_call(
        ahead_kernel,
        in_specs=[V] * 3,
        out_specs=V,
        out_shape=vmem(*padded),
        compiler_params=pltpu.CompilerParams(vmem_limit_bytes=4 * MIB),
        name="ahead",
    )(u2p, b, ld)
    w1, sp, bumps = pl.pallas_call(
        coarse_kernel,
        in_specs=[V] * 14,
        out_specs=[V] * 3,
        out_shape=[vmem(*padded), vmem(HALVES, NB + 2, PC, LANES), vmem(HALVES, 16, LANES)],
        scratch_shapes=[vmem(HALVES, QY, LANES)] * 2 + [grid, wide, wide, grid],
        input_output_aliases={13: 0},
        compiler_params=pltpu.CompilerParams(vmem_limit_bytes=8 * MIB),
        cost_estimate=estimate(10**7, 4 * MIB),
        name="coarse",
    )(lx, bc, s0, s1, gye, gyo, hxl, hxh, hyl, hyh, pxl, pxh, b, u3)
    _, corrected = pl.pallas_call(
        last_kernel,
        in_specs=[V] * 14,
        out_specs=[V, H],
        out_shape=[vmem(*padded), jax.ShapeDtypeStruct(load_terms.shape, F)],
        scratch_shapes=[outer] * 2
        + [vmem(*padded)]
        + [vmem(8, PC, LANES), vmem(8, 2, T, LANES), vmem(8, T, LANES), pltpu.SemaphoreType.DMA((HALVES, 4))],
        input_output_aliases={0: 0},
        compiler_params=pltpu.CompilerParams(vmem_limit_bytes=12 * MIB),
        name="last",
    )(w1, sp, bumps, vxl, vxh, vye, vyo, hxl, hxh, hyl, hyh, u2p, b, ld)
    return corrected


def solution(mesh):
    return jax.shard_map(
        per_device,
        mesh=mesh,
        in_specs=(P("py", "px", None), P("py", "px", None), P("py", "px", None)),
        out_specs=P("py", "px", None),
        check_vma=False,
    )
```

```python
import jax
import jax.numpy as jnp
from jax import lax
from jax.experimental import pallas as pl
from jax.experimental.pallas import tpu as pltpu
from jax.sharding import PartitionSpec as P

F = jnp.float32
T = 64
R = 4
NB = T // R
INNER = 7
DEPTH = INNER
LANES = 128
HALVES = 2
PR, PC = T + 2, T + 16
PLANE = PR * PC
CW = 32
CR = NB + 2 * DEPTH
KX = DEPTH * NB
KY = sum(CW - 2 * i for i in range(1, DEPTH + 1))
QX_S, QX_Q = KX, KX + 16
QX = QX_Q + NB
QY_S, QY_DIAG = KY, KY + CW
QY = QY_DIAG + 8
MIB = 2**20


def rows(start, size, stride=1):
    return pl.ds(start, size, stride=stride)


def mid():
    return pl.ds(8, T)


def left():
    return pl.ds(7, T)


def right():
    return pl.ds(9, T)


def around(ref, h, y):
    return (ref[h, y, mid(), :] + ref[h, y + 2, mid(), :]) + (
        ref[h, y + 1, left(), :] + ref[h, y + 1, right(), :]
    )


def each_row(body, n=T, unroll=2):
    for h in range(HALVES):
        lax.fori_loop(0, n, lambda y, c, h=h: (body(h, y), c)[1], 0, unroll=unroll)


def carried(h, first, last, src, point, x=0, n=T, unroll=2):
    here_x, left_x, right_x = pl.ds(8 + x, n), pl.ds(7 + x, n), pl.ds(9 + x, n)

    def body(y, c):
        above, here = c
        below = src[h, y + 2, here_x, :]
        point(y, here, (above + below) + (src[h, y + 1, left_x, :] + src[h, y + 1, right_x, :]))
        return here, below

    lax.fori_loop(first, last, body, (src[h, first, here_x, :], src[h, first + 1, here_x, :]), unroll=unroll)


def clear_border(ref):
    for h in range(HALVES):
        ref[h, 0] = jnp.zeros((PC, LANES), F)
        ref[h, PR - 1] = jnp.zeros((PC, LANES), F)
        for x in (0, PC - 8):
            ref[h, pl.ds(1, T), pl.ds(x, 8), :] = jnp.zeros((T, 8, LANES), F)


def column(h, x):
    return rows(h * PLANE + PC + 8 + x, T, PC)


AXIS = {"r1x": "px", "massx": "px", "r2x": "px", "u2x": "px", "r1y": "py", "massy": "py", "r2y": "py", "u2y": "py"}
SWAPPED = ("r1x", "massx", "r2x", "u2x", "r1y", "massy", "r2y", "u2y")


def is_even(axis):
    return lax.rem(lax.axis_index(axis), 2) == 0


def order(name, first, second, a, b):
    even = is_even(AXIS[name]) if name in SWAPPED else False
    n = first.shape[1]
    for h in range(HALVES):
        for r in range(0, n, T):
            part = pl.ds(r, min(T, n - r))
            va, vb = a[h, part, :], b[h, part, :]
            first[h, part, :] = va if even is False else jnp.where(even, vb, va)
            second[h, part, :] = vb if even is False else jnp.where(even, va, vb)


def block_sums(part, out):
    n = HALVES * NB * NB

    def body(j, c):
        total = part[rows(j * 4 * T, T, R), :]
        for k in range(1, R):
            total = total + part[rows(j * 4 * T + k, T, R), :]
        out[pl.ds(j * T, T), :] = total * (1.0 / R)
        return c

    lax.fori_loop(0, n // T, body, 0)


def column_edges(load_h, u_h, m_h, pxl, pxh, pxe, pxo, uc, lc, mc, sems):
    copies = []
    for h in range(HALVES):
        lanes = pl.ds(h * LANES, LANES)
        for i in range(2):
            x = (0, T - 8)[i]
            for n, (src, dst) in enumerate(
                (
                    (u_h.at[:, pl.ds(x, 8), lanes], uc.at[h, i, pl.ds(1, T)]),
                    (load_h.at[:, pl.ds(x, 8), lanes], lc.at[h, i]),
                    (m_h.at[:, pl.ds(x, 8), lanes], mc.at[h, i]),
                )
            ):
                copies.append(pltpu.make_async_copy(src, dst, sems.at[h, i, n]))
    for c in copies:
        c.start()
    for h in range(HALVES):
        for i in range(2):
            uc[h, i, 0] = jnp.zeros((8, LANES), F)
            uc[h, i, T + 1] = jnp.zeros((8, LANES), F)
    for c in copies:
        c.wait()
    uc2 = uc.reshape(HALVES * 2 * (T + 2) * 8, LANES)
    lc2, mc2 = lc.reshape(HALVES * 2 * T * 8, LANES), mc.reshape(HALVES * 2 * T * 8, LANES)
    for h in range(HALVES):
        for i in range(2):
            px = (pxl, pxh)[i]
            ub, lb = (h * 2 + i) * (T + 2) * 8, (h * 2 + i) * T * 8
            x, xi = (0, 7)[i], (1, 6)[i]
            u = uc2[rows(ub + 8 + x, T, 8), :]
            bb = 0.8 / (4.0 + mc2[rows(lb + x, T, 8), :])
            near = uc2[rows(ub + 8 + xi, T, 8), :] + (uc2[rows(ub + x, T, 8), :] + uc2[rows(ub + 16 + x, T, 8), :])
            px[h, pl.ds(0, T), :] = u
            px[h, pl.ds(T, T), :] = 0.2 * u + bb * (lc2[rows(lb + x, T, 8), :] + near)
            px[h, pl.ds(2 * T, T), :] = bb
    order("r1x", pxe, pxo, pxl, pxh)


def row_edges(load_h, u_h, m_h, pyl, pyh, pye, pyo, ur, lr, mr, sems):
    copies = []
    for h in range(HALVES):
        lanes = pl.ds(h * LANES, LANES)
        for i in range(2):
            y, yy = (0, T - 1)[i], (0, T - 2)[i]
            for n, (src, dst) in enumerate(
                (
                    (u_h.at[pl.ds(yy, 2), :, lanes], ur.at[h, i, :, mid(), :]),
                    (load_h.at[pl.ds(y, 1), :, lanes], lr.at[h, i]),
                    (m_h.at[pl.ds(y, 1), :, lanes], mr.at[h, i]),
                )
            ):
                copies.append(pltpu.make_async_copy(src, dst, sems.at[h, i, n]))
    for c in copies:
        c.start()
    for h in range(HALVES):
        for i in range(2):
            for k in range(2):
                ur[h, i, k, pl.ds(0, 8), :] = jnp.zeros((8, LANES), F)
                ur[h, i, k, pl.ds(8 + T, 8), :] = jnp.zeros((8, LANES), F)
    for c in copies:
        c.wait()
    for h in range(HALVES):
        for k in range(2):
            py = (pyl, pyh)[k]
            u = ur[h, k, k, mid(), :]
            bb = 0.8 / (4.0 + mr[h, k, 0])
            near = ur[h, k, 1 - k, mid(), :] + (ur[h, k, k, left(), :] + ur[h, k, k, right(), :])
            py[h, pl.ds(0, T), :] = u
            py[h, pl.ds(T, T), :] = 0.2 * u + bb * (lr[h, k, 0] + near)
            py[h, pl.ds(2 * T, T), :] = bb
    order("r1y", pye, pyo, pyl, pyh)


CHUNKS = 4


def first_kernel(load_h, u_h, m_h, u1p, b, ld, m, mo, kxe, kxo, up, part, kxl, kxh, sems):
    step = T // CHUNKS
    copies = {}
    for h in range(HALVES):
        lanes = pl.ds(h * LANES, LANES)
        for q in range(CHUNKS):
            y = pl.ds(q * step, step)
            copies[h, q] = [
                pltpu.make_async_copy(m_h.at[y, :, lanes], m.at[h, y], sems.at[0, h, q]),
                pltpu.make_async_copy(
                    u_h.at[y, :, lanes], up.at[h, pl.ds(q * step + 1, step), pl.ds(8, T), :], sems.at[1, h, q]
                ),
                pltpu.make_async_copy(load_h.at[y, :, lanes], ld.at[h, y], sems.at[2, h, q]),
            ]
            for c in copies[h, q]:
                c.start()
    clear_border(up)

    for h in range(HALVES):

        def sweep(y, c, h=h):
            bb = 0.8 / (4.0 + m[h, y])
            b[h, y] = bb
            u1p[h, y + 1, mid(), :] = 0.2 * up[h, y + 1, mid(), :] + bb * (ld[h, y] + around(up, h, y))
            return c

        def sums(y, c, h=h):
            part[pl.ds(pl.multiple_of((h * NB + y) * T, T), T), :] = (m[h, R * y] + m[h, R * y + 1]) + (
                m[h, R * y + 2] + m[h, R * y + 3]
            )
            return c

        for q in range(CHUNKS):
            for c in copies[h, q]:
                c.wait()
            lax.fori_loop(q * step // R, (q + 1) * step // R, sums, 0, unroll=2)
            lax.fori_loop(max(q * step - 1, 0), T if q == CHUNKS - 1 else (q + 1) * step - 1, sweep, 0, unroll=2 if q else 1)
    block_sums(part, mo)
    for h in range(HALVES):
        for first, q in ((0, kxl), (NB - DEPTH, kxh)):
            for k in range(DEPTH):
                q[h, pl.ds(k * NB, NB), :] = mo[rows(h * NB * NB + first + k, NB, NB), :]
    order("massx", kxe, kxo, kxl, kxh)


def spread_x(inner, low, high, ext):
    ext2 = ext.reshape(HALVES * NB * CW, LANES)
    for h in range(HALVES):
        for y in range(NB):
            ext[h, y, pl.ds(8, NB), :] = inner[pl.ds(h * NB * NB + y * NB, NB), :]
        for c, g in ((1, low), (8 + NB, high)):
            for k in range(DEPTH):
                ext2[rows(h * NB * CW + c + k, NB, CW), :] = g[h, pl.ds(k * NB, NB), :]


def wedge(i):
    return i, CW - 2 * i, sum(CW - 2 * k for k in range(1, i))


def cut_wedges(ext, h, low, high):
    for i in range(1, DEPTH + 1):
        c, n, at = wedge(i)
        low[h, pl.ds(at, n), :] = ext[h, i - 1, pl.ds(c, n), :]
        high[h, pl.ds(at, n), :] = ext[h, NB - i, pl.ds(c, n), :]


def mass_kernel(mo, gme, gmo, mx, kye, kyo, gml, gmh, kyl, kyh):
    order("massx", gml, gmh, gme, gmo)
    spread_x(mo, gml, gmh, mx)
    for h in range(HALVES):
        cut_wedges(mx, h, kyl, kyh)
    order("massy", kye, kyo, kyl, kyh)


def bulk_kernel(u1p, b, ld, m, u2p, part):
    clear_border(u2p)
    for h in range(HALVES):

        def sweep(y, c, near, h=h):
            u2p[h, y + 1, mid(), :] = 0.2 * c + b[h, y] * (ld[h, y] + near)

        carried(h, 0, T, u1p, sweep)
    for h in range(HALVES):

        def sums(y, c, h=h):
            above, here = c
            total = None
            for k in range(R):
                r = R * y + k
                below = u2p[h, r + 2, mid(), :]
                near = (above + below) + (u2p[h, r + 1, left(), :] + u2p[h, r + 1, right(), :])
                d = (ld[h, r] + near) - (4.0 + m[h, r]) * here
                total = d if total is None else total + d
                above, here = here, below
            part[pl.ds(pl.multiple_of((h * NB + y) * T, T), T), :] = total
            return above, here

        lax.fori_loop(0, NB, sums, (u2p[h, 0, mid(), :], u2p[h, 1, mid(), :]))


def defect_rows(h, y, u2p, ld, m, part):
    total = None
    for k in range(R):
        c = R * y + k
        d = (ld[h, c] + around(u2p, h, c)) - (4.0 + m[h, c]) * u2p[h, c + 1, mid(), :]
        total = d if total is None else total + d
    part[pl.ds(pl.multiple_of((h * NB + y) * T, T), T), :] = total


def near_tile(ref, h, y, x):
    return (ref[h, pl.ds(y, 8), pl.ds(x + 8, 8), :] + ref[h, pl.ds(y + 2, 8), pl.ds(x + 8, 8), :]) + (
        ref[h, pl.ds(y + 1, 8), pl.ds(x + 7, 8), :] + ref[h, pl.ds(y + 1, 8), pl.ds(x + 9, 8), :]
    )


def second_kernel(
    u1p_in, u2p_in, part_in, b, ld, m, pxl, pxh, pyl, pyh, hxe, hxo, hye, hyo,
    u1p, u2p, part, lp, own, qxl, qxh, qxe, qxo, vxe, vxo, vye, vyo, hxl, hxh, hyl, hyh,
    vxl, vxh, vyl, vyh,
):
    del u1p_in, u2p_in, part_in
    order("r1x", hxl, hxh, hxe, hxo)
    order("r1y", hyl, hyh, hye, hyo)
    u1p2 = u1p.reshape(HALVES * PLANE, LANES)
    U, A, B = pl.ds(0, T), pl.ds(T, T), pl.ds(2 * T, T)
    for h in range(HALVES):
        for x, p, g in ((0, pxl, hxl), (T - 1, pxh, hxh)):
            inner = column(h, x)
            outer = column(h, -1 if x == 0 else T)
            u1p2[inner, :] = u1p2[inner, :] + p[h, B, :] * g[h, U, :]
            u1p2[outer, :] = g[h, A, :] + g[h, B, :] * p[h, U, :]
        for y, p, g in ((0, pyl, hyl), (T - 1, pyh, hyh)):
            u1p[h, y + 1, mid(), :] = u1p[h, y + 1, mid(), :] + p[h, B, :] * g[h, U, :]
            u1p[h, 0 if y == 0 else T + 1, mid(), :] = g[h, A, :] + g[h, B, :] * p[h, U, :]

    for h in range(HALVES):
        for y in (0, 1, T - 2, T - 1):
            u2p[h, y + 1, mid(), :] = 0.2 * u1p[h, y + 1, mid(), :] + b[h, y] * (ld[h, y] + around(u1p, h, y))

    def sweep(j, c):
        y = pl.multiple_of(j * 8, 8)
        for h in range(HALVES):
            for x in (0, T - 8):
                here = (h, pl.ds(y + 1, 8), pl.ds(8 + x, 8))
                tile = (h, pl.ds(y, 8), pl.ds(x, 8))
                u2p[here] = 0.2 * u1p[here] + b[tile] * (ld[tile] + near_tile(u1p, h, y, x))
        return c

    lax.fori_loop(0, T // 8, sweep, 0)

    def sums(j, c):
        y = pl.multiple_of(j * 8, 8)
        for h in range(HALVES):
            for x in (0, T - 8):
                here = (h, pl.ds(y + 1, 8), pl.ds(8 + x, 8))
                tile = (h, pl.ds(y, 8), pl.ds(x, 8))
                d = (ld[tile] + near_tile(u2p, h, y, x)) - (4.0 + m[tile]) * u2p[here]
                for k in range(2):
                    at = pl.multiple_of((h * NB + 2 * j + k) * T, T) + x
                    part[pl.ds(at, 8), :] = (d[R * k] + d[R * k + 1]) + (d[R * k + 2] + d[R * k + 3])
        return c

    lax.fori_loop(0, T // 8, sums, 0)
    for h in range(HALVES):
        for y in (0, NB - 1):
            defect_rows(h, y, u2p, ld, m, part)
    block_sums(part, lp)

    u2p2, ld2 = u2p.reshape(HALVES * PLANE, LANES), ld.reshape(HALVES * T * T, LANES)
    for h in range(HALVES):
        for x, first, s, q, v in ((0, 0, 0, qxl, vxl), (T - 1, NB - DEPTH, 8, qxh, vxh)):
            for k in range(DEPTH):
                q[h, pl.ds(k * NB, NB), :] = lp[rows(h * NB * NB + first + k, NB, NB), :]
            for i, y in enumerate((0, T - 1)):
                total = None
                for k in range(R):
                    e = u2p2[rows(h * PLANE + (y + 1) * PC + 8 + R * s + k, 8, R), :]
                    total = e if total is None else total + e
                q[h, pl.ds(QX_S + 8 * i, 8), :] = total
                own[h, i, pl.ds(s, 8), :] = total
                free = QX_S + 8 * i + (7 if x == 0 else 0)
                q[h, pl.ds(free, 1), :] = u2p[h, y + 1, pl.ds(8 + x, 1), :]
            total = None
            for k in range(R):
                e = u2p2[rows(h * PLANE + (k + 1) * PC + 8 + x, NB, R * PC), :]
                total = e if total is None else total + e
            q[h, pl.ds(QX_Q, NB), :] = total * (1.0 / R)
            v[h, pl.ds(0, T), :] = u2p2[column(h, x), :]
            v[h, pl.ds(T, T), :] = ld2[rows(h * T * T + x, T, T), :] + u2p2[column(h, 1 if x == 0 else T - 2), :]
        for y, inside, v in ((0, 1, vyl), (T - 1, T - 2, vyh)):
            v[h, pl.ds(0, T), :] = u2p[h, y + 1, mid(), :]
            v[h, pl.ds(T, T), :] = ld[h, y] + u2p[h, inside + 1, mid(), :]
    order("r2x", qxe, qxo, qxl, qxh)
    order("u2x", vxe, vxo, vxl, vxh)
    order("u2y", vye, vyo, vyl, vyh)


def third_kernel(lp, own, qxl, qxh, gxe, gxo, hxl, hxh, lx, s0, s1, qye, qyo, gxl, gxh, qyl, qyh):
    order("r2x", gxl, gxh, gxe, gxo)
    lx2 = lx.reshape(HALVES * NB * CW, LANES)
    spread_x(lp, gxl, gxh, lx)
    for h in range(HALVES):
        for c, ref in ((8, gxl), (7, qxl), (7 + NB, gxh), (8 + NB, qxh)):
            col = rows(h * NB * CW + c, NB, CW)
            lx2[col, :] = lx2[col, :] + ref[h, pl.ds(QX_Q, NB), :]
        for i, s in enumerate((s0, s1)):
            for c, ref in ((0, gxl), (24, gxh)):
                s[h, pl.ds(c, 8), :] = ref[h, pl.ds(QX_S + 8 * i, 8), :]
            s[h, pl.ds(8, NB), :] = own[h, i]
        cut_wedges(lx, h, qyl, qyh)
        for i, s, q in ((0, s0, qyl), (1, s1, qyh)):
            y = i * (T - 1)
            q[h, pl.ds(QY_S, CW), :] = s[h]
            for j, (g1, g2) in enumerate(((hxl, gxl), (hxh, gxh))):
                q[h, pl.ds(QY_DIAG + 3 * j, 1), :] = g1[h, pl.ds(y, 1), :]
                q[h, pl.ds(QY_DIAG + 3 * j + 1, 1), :] = g1[h, pl.ds(2 * T + y, 1), :]
                q[h, pl.ds(QY_DIAG + 3 * j + 2, 1), :] = g2[h, pl.ds(QX_S + 8 * i + 7 * j, 1), :]
            q[h, pl.ds(QY_DIAG + 6, 2), :] = jnp.zeros((2, LANES), F)
    order("r2y", qye, qyo, qyl, qyh)


def rate_kernel(mx, gke, gko, bc, gkl, gkh):
    order("massy", gkl, gkh, gke, gko)
    for h in range(HALVES):
        for i in range(1, DEPTH + 1):
            c, n, at = wedge(i)
            for r, gk in ((DEPTH - i, gkl), (DEPTH + NB - 1 + i, gkh)):
                bc[h, r, pl.ds(c, n), :] = 0.8 / (4.0 + gk[h, pl.ds(at, n), :])
        for y in range(NB):
            bc[h, DEPTH + y] = 0.8 / (4.0 + mx[h, y])


def coarse_kernel(
    lx, bc, s0, s1, gye, gyo, hxl, hxh, hyl, hyh, pxl, pxh, b, w1_in,
    w1, sp, bumps, gyl, gyh, lg, ca, cb, cv,
):
    del w1_in
    order("r2y", gyl, gyh, gye, gyo)
    one = lambda r: pl.ds(r, 1)
    for h in range(HALVES):
        for i in range(1, DEPTH + 1):
            c, n, at = wedge(i)
            for r, g in ((DEPTH - i, gyl), (DEPTH + NB - 1 + i, gyh)):
                lg[h, r, pl.ds(c, n), :] = g[h, pl.ds(at, n), :]
        for y in range(NB):
            lg[h, DEPTH + y] = lx[h, y]
        quarter = 1.0 / R
        for r, v in (
            (DEPTH - 1, s0[h]),
            (DEPTH, gyl[h, pl.ds(QY_S, CW), :]),
            (DEPTH + NB - 1, gyh[h, pl.ds(QY_S, CW), :]),
            (DEPTH + NB, s1[h]),
        ):
            lg[h, r] = lg[h, r] + quarter * v

    for h in range(HALVES):
        for j, (px, hx) in enumerate(((pxl, hxl), (pxh, hxh))):
            for i, (hy, gy) in enumerate(((hyl, gyl), (hyh, gyh))):
                y, x = (0, T - 1)[i], (0, T - 1)[j]
                ua, ba = px[h, one(y), :], px[h, one(2 * T + y), :]
                ux, bx = hx[h, one(y), :], hx[h, one(2 * T + y), :]
                uy, by = hy[h, one(x), :], hy[h, one(2 * T + x), :]
                ud, bd = gy[h, one(QY_DIAG + 3 * j), :], gy[h, one(QY_DIAG + 3 * j + 1), :]
                ea, ed = ba * (bx + by) * ud, bd * (bx + by) * ua
                ex, ey = bx * (ba + bd) * uy, by * (ba + bd) * ux
                ya, yo = (DEPTH, DEPTH - 1) if i == 0 else (DEPTH + NB - 1, DEPTH + NB)
                xa, xo = (8, 7) if j == 0 else (7 + NB, 8 + NB)
                for yy, xx, e, bb, e1, e2 in (
                    (ya, xa, ea, ba, ex, ey),
                    (ya, xo, ex, bx, ea, ed),
                    (yo, xa, ey, by, ea, ed),
                    (yo, xo, ed, bd, ex, ey),
                ):
                    lg[h, yy, one(xx), :] = lg[h, yy, one(xx), :] + quarter * (
                        (2.0 - 0.8 / bb) * e + (e1 + e2)
                    )
                at = 4 * (2 * i + j)
                for k, e in enumerate((ea, ex, ey, ed + gy[h, one(QY_DIAG + 3 * j + 2), :])):
                    bumps[h, one(at + k), :] = e

    own = pl.ds(8, CW)

    def start(h, y):
        v = bc[h, y] * lg[h, y]
        lg[h, y] = v
        ca[h, y, own, :] = v

    each_row(start, CR)
    old, new = ca, cb
    for s in range(1, INNER):

        def inner(y, c, old=old, new=new, end=s == INNER - 1):
            kept = []
            for h in range(HALVES):
                above, here = c[h]
                below = old[h, y + 1, own, :]
                near = (above + below) + (old[h, y, pl.ds(7, CW), :] + old[h, y, pl.ds(9, CW), :])
                value = (0.2 * here + lg[h, y]) + bc[h, y] * near
                if end:
                    cv[h, y] = value
                else:
                    new[h, y, own, :] = value
                kept.append((here, below))
            return tuple(kept)

        lax.fori_loop(
            s, CR - s, inner, tuple((old[h, s - 1, own, :], old[h, s, own, :]) for h in range(HALVES)), unroll=2
        )
        old, new = new, old

    for h in range(HALVES):
        for y in range(NB + 2):
            c = cv[h, y + DEPTH - 1, pl.ds(6, NB + 4), :]
            for k in range(R):
                sp[h, y, rows(k, NB + 4, R), :] = c

    def correct(h, y):
        c = sp[h, y + 1, mid(), :]
        sides = sp[h, y + 1, left(), :] + sp[h, y + 1, right(), :]
        above, below = sp[h, y, mid(), :], sp[h, y + 2, mid(), :]
        base = 0.2 * c
        inside = sides + (c + c)
        for k, near in ((0, sides + (c + above)), (1, inside), (2, inside), (3, sides + (c + below))):
            r = R * y + k
            w1[h, r + 1, mid(), :] = w1[h, r + 1, mid(), :] + (base + b[h, r] * near)

    each_row(correct, NB, unroll=1)


def ahead_kernel(u2p, b, ld, w1):
    for h in range(HALVES):

        def sweep(y, c, near, h=h):
            w1[h, y + 1, mid(), :] = 0.2 * c + b[h, y] * (ld[h, y] + near)

        carried(h, 0, T, u2p, sweep)


def ring(n, h, v, bh, c, wh, oh, ends, corners, here, to):
    one = lambda r: pl.ds(r, 1)
    wh[n, mid(), :] = v[h, pl.ds(0, T), :]
    for r, (outside, inside) in zip((0, T - 1), ends):
        wh[n, one(8 + r), :] = wh[n, one(8 + r), :] + outside
        oh[n, one(r), :] = oh[n, one(r), :] + inside
    u2h = wh[n, mid(), :]
    w0h = u2h + c
    wh[n, mid(), :] = w0h
    wh[n, one(7), :], wh[n, one(8 + T), :] = corners
    near = (wh[n, left(), :] + wh[n, right(), :]) + oh[n]
    here(u2h)
    to(0.2 * w0h + bh * ((v[h, pl.ds(T, T), :] + c) + near))


def corner_values(bumps, sp, h):
    bump = lambda i, j, k: bumps[h, pl.ds(4 * (2 * i + j) + k, 1), :]
    diag = {
        (i, j): bump(i, j, 3) + sp[h, (0, NB + 1)[i], pl.ds((7, 8 + T)[j], 1), :] for i in range(2) for j in range(2)
    }
    return bump, diag


INNER_X = T - 16


def inner_kernel(w1_in, sp, bumps, vye, vyo, hyl, hyh, u2p, b, ld, w1, out, vyl, vyh, w0, wh, oh, sems):
    del w1_in
    order("u2y", vyl, vyh, vye, vyo)
    one = lambda r: pl.ds(r, 1)
    n = 0
    copies = []
    for h in range(HALVES):
        bump, diag = corner_values(bumps, sp, h)
        for i in range(2):
            for j in range(2):
                e, y, x = bump(i, j, 0), (0, T - 1)[i], (0, T - 1)[j]
                yi, xi = (1, T - 2)[i], (1, T - 2)[j]
                for yy, xx, f in ((y, x, None), (y, xi, b), (yi, x, b)):
                    f = 0.2 if f is None else b[h, yy, one(xx), :]
                    w1[h, yy + 1, one(xx + 8), :] = w1[h, yy + 1, one(xx + 8), :] + f * e
        for i, (v, hy) in enumerate(((vyl, hyl), (vyh, hyh))):
            y = (0, T - 1)[i]
            oh[n] = u2p[h, y + 1, mid(), :] + sp[h, (1, NB)[i], mid(), :]

            def here(u2h, h=h, y=y):
                w1[h, y + 1, mid(), :] = w1[h, y + 1, mid(), :] + b[h, y] * u2h

            def to(value, h=h, i=i):
                w1[h, (0, T + 1)[i], mid(), :] = value

            ring(
                n, h, v, hy[h, pl.ds(2 * T, T), :], sp[h, (0, NB + 1)[i], mid(), :], wh, oh,
                [(bump(i, j, 2), bump(i, j, 0)) for j in range(2)], (diag[i, 0], diag[i, 1]), here, to,
            )
            n += 1

        def last(y, c, near, h=h):
            w0[h, y] = 0.2 * c + b[h, y, pl.ds(8, INNER_X), :] * (ld[h, y, pl.ds(8, INNER_X), :] + near)

        step = T // 4
        for q in range(4):
            carried(h, q * step, (q + 1) * step, w1, last, 8, INNER_X)
            copies.append(
                pltpu.make_async_copy(
                    w0.at[h, pl.ds(q * step, step)],
                    out.at[pl.ds(q * step, step), pl.ds(8, INNER_X), pl.ds(h * LANES, LANES)],
                    sems.at[h, q],
                )
            )
            copies[-1].start()
    for c in copies:
        c.wait()


def last_kernel(w1_in, out_in, sp, bumps, vxe, vxo, hxl, hxh, u2p, b, ld, w1, out, vxl, vxh, w0, wh, sh, oh, sems):
    del w1_in, out_in
    order("u2x", vxl, vxh, vxe, vxo)
    stride = (NB + 2) * PC
    sp2, b2 = sp.reshape(HALVES * stride, LANES), b.reshape(HALVES * T * T, LANES)
    w12, u2p2 = w1.reshape(HALVES * PLANE, LANES), u2p.reshape(HALVES * PLANE, LANES)
    n = 0
    copies = []
    for h in range(HALVES):
        bump, diag = corner_values(bumps, sp, h)
        for j, (v, hx) in enumerate(((vxl, hxl), (vxh, hxh))):
            x, xo = (0, T - 1)[j], (-1, T)[j]
            for k in range(R):
                sh[n, 0, rows(k, NB, R), :] = sp2[rows(h * stride + PC + 8 + xo, NB, PC), :]
                sh[n, 1, rows(k, NB, R), :] = sp2[rows(h * stride + PC + 8 + x, NB, PC), :]
            oh[n] = u2p2[column(h, x), :] + sh[n, 1]

            def here(u2h, h=h, x=x):
                at = column(h, x)
                w12[at, :] = w12[at, :] + b2[rows(h * T * T + x, T, T), :] * u2h

            def to(value, h=h, xo=xo):
                w12[column(h, xo), :] = value

            ring(
                n, h, v, hx[h, pl.ds(2 * T, T), :], sh[n, 0], wh, oh,
                [(bump(i, j, 1), bump(i, j, 0)) for i in range(2)], (diag[0, j], diag[1, j]), here, to,
            )
            n += 1

        for j, x in enumerate((0, T - 8)):

            def sweep(k, c, h=h, j=j, x=x):
                y = pl.multiple_of(k * 8, 8)
                tile = (h, pl.ds(y, 8), pl.ds(x, 8))
                near = near_tile(w1, h, y, x)
                w0[h, j, pl.ds(y, 8)] = 0.2 * w1[h, pl.ds(y + 1, 8), pl.ds(8 + x, 8)] + b[tile] * (ld[tile] + near)
                return c

            lax.fori_loop(0, T // 8, sweep, 0, unroll=2)
            copies.append(
                pltpu.make_async_copy(
                    w0.at[h, j], out.at[:, pl.ds(x, 8), pl.ds(h * LANES, LANES)], sems.at[h, j]
                )
            )
            copies[-1].start()
    for c in copies:
        c.wait()


def vmem(*shape):
    return pltpu.VMEM(shape, F)


V = pl.BlockSpec(memory_space=pltpu.VMEM)
H = pl.BlockSpec(memory_space=pltpu.HBM)


def exchange(name, even, odd):
    axis = AXIS[name]
    size = lax.axis_size(axis)
    up = [(i, (i + 1) % size) for i in range(size)]
    if name not in SWAPPED:
        return lax.ppermute(odd, axis, up), lax.ppermute(even, axis, [(b, a) for a, b in up])
    pairs = [[p for a, b in up[k::2] for p in ((a, b), (b, a))] for k in range(2)]
    return lax.ppermute(even, axis, pairs[0]), lax.ppermute(odd, axis, pairs[1])


def estimate(flops, size):
    return pl.CostEstimate(flops=flops, bytes_accessed=size, transcendentals=0)


def per_device(load_terms, start_values, reaction_rate):
    tile, padded = (HALVES, T, T, LANES), (HALVES, PR, PC, LANES)
    coarse = (HALVES * NB * NB, LANES)
    edge = (HALVES, 3 * T, LANES)
    part = vmem(HALVES * NB * T, LANES)
    inputs = tuple(
        pltpu.with_memory_space_constraint(v, pltpu.HBM) for v in (load_terms, start_values, reaction_rate)
    )
    strip, line = vmem(HALVES, 2, T, 8, LANES), vmem(HALVES, 2, 1, T, LANES)
    pyl, pyh, pye, pyo = pl.pallas_call(
        row_edges,
        in_specs=[H] * 3,
        out_specs=[V] * 4,
        out_shape=[vmem(*edge)] * 4,
        scratch_shapes=[vmem(HALVES, 2, 2, PC, LANES), line, line, pltpu.SemaphoreType.DMA((HALVES, 2, 3))],
        compiler_params=pltpu.CompilerParams(vmem_limit_bytes=4 * MIB),
        name="rowedges",
    )(*inputs)
    hye, hyo = exchange("r1y", pye, pyo)
    pxl, pxh, pxe, pxo = pl.pallas_call(
        column_edges,
        in_specs=[H] * 3,
        out_specs=[V] * 4,
        out_shape=[vmem(*edge)] * 4,
        scratch_shapes=[vmem(HALVES, 2, T + 2, 8, LANES), strip, strip, pltpu.SemaphoreType.DMA((HALVES, 2, 3))],
        compiler_params=pltpu.CompilerParams(vmem_limit_bytes=8 * MIB),
        name="columnedges",
    )(*inputs)
    hxe, hxo = exchange("r1x", pxe, pxo)
    u1p, b, ld, m, mo, kxe, kxo = pl.pallas_call(
        first_kernel,
        in_specs=[H] * 3,
        out_specs=[V] * 7,
        out_shape=[vmem(*padded)] + [vmem(*tile)] * 3 + [vmem(*coarse)] + [vmem(HALVES, KX, LANES)] * 2,
        scratch_shapes=[vmem(*padded), part]
        + [vmem(HALVES, KX, LANES)] * 2
        + [pltpu.SemaphoreType.DMA((3, HALVES, CHUNKS))],
        compiler_params=pltpu.CompilerParams(vmem_limit_bytes=12 * MIB),
        cost_estimate=estimate(10**7, 12 * MIB),
        name="first",
    )(*inputs)
    gme, gmo = exchange("massx", kxe, kxo)
    outer = vmem(HALVES, 2 * T, LANES)
    u2p, part_sums = pl.pallas_call(
        bulk_kernel,
        in_specs=[V] * 4,
        out_specs=[V] * 2,
        out_shape=[vmem(*padded), part],
        compiler_params=pltpu.CompilerParams(vmem_limit_bytes=4 * MIB),
        cost_estimate=estimate(10**7, 12 * MIB),
        name="bulk",
    )(u1p, b, ld, m)
    _, u2p, _, lp, own, qxl, qxh, qxe, qxo, vxe, vxo, vye, vyo, hxl, hxh, hyl, hyh = pl.pallas_call(
        second_kernel,
        in_specs=[V] * 14,
        out_specs=[V] * 17,
        out_shape=[vmem(*padded)] * 2
        + [part, vmem(*coarse), vmem(HALVES, 2, NB, LANES)]
        + [vmem(HALVES, QX, LANES)] * 4
        + [outer] * 4
        + [vmem(*edge)] * 4,
        scratch_shapes=[outer] * 4,
        input_output_aliases={0: 0, 1: 1, 2: 2},
        compiler_params=pltpu.CompilerParams(vmem_limit_bytes=8 * MIB),
        name="second",
    )(u1p, u2p, part_sums, b, ld, m, pxl, pxh, pyl, pyh, hxe, hxo, hye, hyo)
    gxe, gxo = exchange("r2x", qxe, qxo)
    vxe, vxo = exchange("u2x", vxe, vxo)
    mx, kye, kyo = pl.pallas_call(
        mass_kernel,
        in_specs=[V] * 3,
        out_specs=[V] * 3,
        out_shape=[vmem(HALVES, NB, CW, LANES)] + [vmem(HALVES, KY, LANES)] * 2,
        scratch_shapes=[vmem(HALVES, KX, LANES)] * 2 + [vmem(HALVES, KY, LANES)] * 2,
        compiler_params=pltpu.CompilerParams(vmem_limit_bytes=8 * MIB),
        name="mass",
    )(mo, gme, gmo)
    gke, gko = exchange("massy", kye, kyo)
    lx, s0, s1, qye, qyo = pl.pallas_call(
        third_kernel,
        in_specs=[V] * 8,
        out_specs=[V] * 5,
        out_shape=[vmem(HALVES, NB, CW, LANES)]
        + [vmem(HALVES, CW, LANES)] * 2
        + [vmem(HALVES, QY, LANES)] * 2,
        scratch_shapes=[vmem(HALVES, QX, LANES)] * 2 + [vmem(HALVES, QY, LANES)] * 2,
        compiler_params=pltpu.CompilerParams(vmem_limit_bytes=8 * MIB),
        name="third",
    )(lp, own, qxl, qxh, gxe, gxo, hxl, hxh)
    gye, gyo = exchange("r2y", qye, qyo)
    vye, vyo = exchange("u2y", vye, vyo)
    grid = vmem(HALVES, CR, CW, LANES)
    bc = pl.pallas_call(
        rate_kernel,
        in_specs=[V] * 3,
        out_specs=V,
        out_shape=grid,
        scratch_shapes=[vmem(HALVES, KY, LANES)] * 2,
        compiler_params=pltpu.CompilerParams(vmem_limit_bytes=8 * MIB),
        name="rate",
    )(mx, gke, gko)
    wide = vmem(HALVES, CR, CW + 16, LANES)
    u3 = pl.pallas_call(
        ahead_kernel,
        in_specs=[V] * 3,
        out_specs=V,
        out_shape=vmem(*padded),
        compiler_params=pltpu.CompilerParams(vmem_limit_bytes=4 * MIB),
        name="ahead",
    )(u2p, b, ld)
    w1, sp, bumps = pl.pallas_call(
        coarse_kernel,
        in_specs=[V] * 14,
        out_specs=[V] * 3,
        out_shape=[vmem(*padded), vmem(HALVES, NB + 2, PC, LANES), vmem(HALVES, 16, LANES)],
        scratch_shapes=[vmem(HALVES, QY, LANES)] * 2 + [grid, wide, wide, grid],
        input_output_aliases={13: 0},
        compiler_params=pltpu.CompilerParams(vmem_limit_bytes=8 * MIB),
        cost_estimate=estimate(10**7, 4 * MIB),
        name="coarse",
    )(lx, bc, s0, s1, gye, gyo, hxl, hxh, hyl, hyh, pxl, pxh, b, u3)
    result = jax.ShapeDtypeStruct(load_terms.shape, F)
    sides = [vmem(4, PC, LANES), vmem(4, T, LANES)]
    w1, partial = pl.pallas_call(
        inner_kernel,
        in_specs=[V] * 10,
        out_specs=[V, H],
        out_shape=[vmem(*padded), result],
        scratch_shapes=[outer] * 2
        + [vmem(HALVES, T, INNER_X, LANES)]
        + sides
        + [pltpu.SemaphoreType.DMA((HALVES, 4))],
        input_output_aliases={0: 0},
        compiler_params=pltpu.CompilerParams(vmem_limit_bytes=12 * MIB),
        cost_estimate=estimate(10**7, 4 * MIB),
        name="inner",
    )(w1, sp, bumps, vye, vyo, hyl, hyh, u2p, b, ld)
    _, corrected = pl.pallas_call(
        last_kernel,
        in_specs=[V, H] + [V] * 9,
        out_specs=[V, H],
        out_shape=[vmem(*padded), result],
        scratch_shapes=[outer] * 2
        + [vmem(HALVES, 2, T, 8, LANES), sides[0], vmem(4, 2, T, LANES), sides[1]]
        + [pltpu.SemaphoreType.DMA((HALVES, 2))],
        input_output_aliases={0: 0, 1: 1},
        compiler_params=pltpu.CompilerParams(vmem_limit_bytes=12 * MIB),
        name="last",
    )(w1, partial, sp, bumps, vxe, vxo, hxl, hxh, u2p, b, ld)
    return corrected


def solution(mesh):
    return jax.shard_map(
        per_device,
        mesh=mesh,
        in_specs=(P("py", "px", None), P("py", "px", None), P("py", "px", None)),
        out_specs=P("py", "px", None),
        check_vma=False,
    )
```

```python
import jax
import jax.numpy as jnp
from jax import lax
from jax.experimental import pallas as pl
from jax.experimental.pallas import tpu as pltpu
from jax.sharding import PartitionSpec as P

F = jnp.float32
T = 64
R = 4
NB = T // R
INNER = 7
DEPTH = INNER
LANES = 128
HALVES = 2
PR, PC = T + 2, T + 16
PLANE = PR * PC
CW = 32
CR = NB + 2 * DEPTH
KX = DEPTH * NB
KY = sum(CW - 2 * i for i in range(1, DEPTH + 1))
QX_S, QX_Q = KX, KX + 16
QX = QX_Q + NB
QY_S, QY_DIAG = KY, KY + CW
QY = QY_DIAG + 8
MIB = 2**20


def rows(start, size, stride=1):
    return pl.ds(start, size, stride=stride)


def mid():
    return pl.ds(8, T)


def left():
    return pl.ds(7, T)


def right():
    return pl.ds(9, T)


def around(ref, h, y):
    return (ref[h, y, mid(), :] + ref[h, y + 2, mid(), :]) + (
        ref[h, y + 1, left(), :] + ref[h, y + 1, right(), :]
    )


def each_row(body, n=T, unroll=2):
    for h in range(HALVES):
        lax.fori_loop(0, n, lambda y, c, h=h: (body(h, y), c)[1], 0, unroll=unroll)


def carried(h, first, last, src, point, x=0, n=T, unroll=2):
    here_x, left_x, right_x = pl.ds(8 + x, n), pl.ds(7 + x, n), pl.ds(9 + x, n)

    def body(y, c):
        above, here = c
        below = src[h, y + 2, here_x, :]
        point(y, here, (above + below) + (src[h, y + 1, left_x, :] + src[h, y + 1, right_x, :]))
        return here, below

    lax.fori_loop(first, last, body, (src[h, first, here_x, :], src[h, first + 1, here_x, :]), unroll=unroll)


def clear_border(ref):
    for h in range(HALVES):
        ref[h, 0] = jnp.zeros((PC, LANES), F)
        ref[h, PR - 1] = jnp.zeros((PC, LANES), F)
        for x in (0, PC - 8):
            ref[h, pl.ds(1, T), pl.ds(x, 8), :] = jnp.zeros((T, 8, LANES), F)


def column(h, x):
    return rows(h * PLANE + PC + 8 + x, T, PC)


AXIS = {"r1x": "px", "massx": "px", "r2x": "px", "u2x": "px", "r1y": "py", "massy": "py", "r2y": "py"}
SWAPPED = ("r1x", "massx", "r2x", "u2x", "r1y", "massy", "r2y")


def is_even(axis):
    return lax.rem(lax.axis_index(axis), 2) == 0


def order(name, first, second, a, b):
    even = is_even(AXIS[name]) if name in SWAPPED else False
    n = first.shape[1]
    for h in range(HALVES):
        for r in range(0, n, T):
            part = pl.ds(r, min(T, n - r))
            va, vb = a[h, part, :], b[h, part, :]
            first[h, part, :] = va if even is False else jnp.where(even, vb, va)
            second[h, part, :] = vb if even is False else jnp.where(even, va, vb)


def block_sums(part, out):
    n = HALVES * NB * NB

    def body(j, c):
        total = part[rows(j * 4 * T, T, R), :]
        for k in range(1, R):
            total = total + part[rows(j * 4 * T + k, T, R), :]
        out[pl.ds(j * T, T), :] = total * (1.0 / R)
        return c

    lax.fori_loop(0, n // T, body, 0)


def column_edges(load_h, u_h, m_h, pxl, pxh, pxe, pxo, uc, lc, mc, sems):
    copies = []
    for h in range(HALVES):
        lanes = pl.ds(h * LANES, LANES)
        for i in range(2):
            x = (0, T - 8)[i]
            for n, (src, dst) in enumerate(
                (
                    (u_h.at[:, pl.ds(x, 8), lanes], uc.at[h, i, pl.ds(1, T)]),
                    (load_h.at[:, pl.ds(x, 8), lanes], lc.at[h, i]),
                    (m_h.at[:, pl.ds(x, 8), lanes], mc.at[h, i]),
                )
            ):
                copies.append(pltpu.make_async_copy(src, dst, sems.at[h, i, n]))
    for c in copies:
        c.start()
    for h in range(HALVES):
        for i in range(2):
            uc[h, i, 0] = jnp.zeros((8, LANES), F)
            uc[h, i, T + 1] = jnp.zeros((8, LANES), F)
    for c in copies:
        c.wait()
    uc2 = uc.reshape(HALVES * 2 * (T + 2) * 8, LANES)
    lc2, mc2 = lc.reshape(HALVES * 2 * T * 8, LANES), mc.reshape(HALVES * 2 * T * 8, LANES)
    for h in range(HALVES):
        for i in range(2):
            px = (pxl, pxh)[i]
            ub, lb = (h * 2 + i) * (T + 2) * 8, (h * 2 + i) * T * 8
            x, xi = (0, 7)[i], (1, 6)[i]
            u = uc2[rows(ub + 8 + x, T, 8), :]
            bb = 0.8 / (4.0 + mc2[rows(lb + x, T, 8), :])
            near = uc2[rows(ub + 8 + xi, T, 8), :] + (uc2[rows(ub + x, T, 8), :] + uc2[rows(ub + 16 + x, T, 8), :])
            px[h, pl.ds(0, T), :] = u
            px[h, pl.ds(T, T), :] = 0.2 * u + bb * (lc2[rows(lb + x, T, 8), :] + near)
            px[h, pl.ds(2 * T, T), :] = bb
    order("r1x", pxe, pxo, pxl, pxh)


def row_edges(load_h, u_h, m_h, pyl, pyh, pye, pyo, ur, lr, mr, sems):
    copies = []
    for h in range(HALVES):
        lanes = pl.ds(h * LANES, LANES)
        for i in range(2):
            y, yy = (0, T - 1)[i], (0, T - 2)[i]
            for n, (src, dst) in enumerate(
                (
                    (u_h.at[pl.ds(yy, 2), :, lanes], ur.at[h, i, :, mid(), :]),
                    (load_h.at[pl.ds(y, 1), :, lanes], lr.at[h, i]),
                    (m_h.at[pl.ds(y, 1), :, lanes], mr.at[h, i]),
                )
            ):
                copies.append(pltpu.make_async_copy(src, dst, sems.at[h, i, n]))
    for c in copies:
        c.start()
    for h in range(HALVES):
        for i in range(2):
            for k in range(2):
                ur[h, i, k, pl.ds(0, 8), :] = jnp.zeros((8, LANES), F)
                ur[h, i, k, pl.ds(8 + T, 8), :] = jnp.zeros((8, LANES), F)
    for c in copies:
        c.wait()
    for h in range(HALVES):
        for k in range(2):
            py = (pyl, pyh)[k]
            u = ur[h, k, k, mid(), :]
            bb = 0.8 / (4.0 + mr[h, k, 0])
            near = ur[h, k, 1 - k, mid(), :] + (ur[h, k, k, left(), :] + ur[h, k, k, right(), :])
            py[h, pl.ds(0, T), :] = u
            py[h, pl.ds(T, T), :] = 0.2 * u + bb * (lr[h, k, 0] + near)
            py[h, pl.ds(2 * T, T), :] = bb
    order("r1y", pye, pyo, pyl, pyh)


CHUNKS = 4


def first_kernel(load_h, u_h, m_h, u1p, b, ld, m, mo, kxe, kxo, up, part, kxl, kxh, sems):
    step = T // CHUNKS
    copies = {}
    for h in range(HALVES):
        lanes = pl.ds(h * LANES, LANES)
        for q in range(CHUNKS):
            y = pl.ds(q * step, step)
            copies[h, q] = [
                pltpu.make_async_copy(m_h.at[y, :, lanes], m.at[h, y], sems.at[0, h, q]),
                pltpu.make_async_copy(
                    u_h.at[y, :, lanes], up.at[h, pl.ds(q * step + 1, step), pl.ds(8, T), :], sems.at[1, h, q]
                ),
                pltpu.make_async_copy(load_h.at[y, :, lanes], ld.at[h, y], sems.at[2, h, q]),
            ]
            for c in copies[h, q]:
                c.start()
    clear_border(up)

    for h in range(HALVES):

        def sweep(y, c, h=h):
            bb = 0.8 / (4.0 + m[h, y])
            b[h, y] = bb
            u1p[h, y + 1, mid(), :] = 0.2 * up[h, y + 1, mid(), :] + bb * (ld[h, y] + around(up, h, y))
            return c

        def sums(y, c, h=h):
            part[pl.ds(pl.multiple_of((h * NB + y) * T, T), T), :] = (m[h, R * y] + m[h, R * y + 1]) + (
                m[h, R * y + 2] + m[h, R * y + 3]
            )
            return c

        for q in range(CHUNKS):
            for c in copies[h, q]:
                c.wait()
            lax.fori_loop(q * step // R, (q + 1) * step // R, sums, 0, unroll=2)
            lax.fori_loop(max(q * step - 1, 0), T if q == CHUNKS - 1 else (q + 1) * step - 1, sweep, 0, unroll=2 if q else 1)
    block_sums(part, mo)
    for h in range(HALVES):
        for first, q in ((0, kxl), (NB - DEPTH, kxh)):
            for k in range(DEPTH):
                q[h, pl.ds(k * NB, NB), :] = mo[rows(h * NB * NB + first + k, NB, NB), :]
    order("massx", kxe, kxo, kxl, kxh)


def spread_x(inner, low, high, ext):
    ext2 = ext.reshape(HALVES * NB * CW, LANES)
    for h in range(HALVES):
        for y in range(NB):
            ext[h, y, pl.ds(8, NB), :] = inner[pl.ds(h * NB * NB + y * NB, NB), :]
        for c, g in ((1, low), (8 + NB, high)):
            for k in range(DEPTH):
                ext2[rows(h * NB * CW + c + k, NB, CW), :] = g[h, pl.ds(k * NB, NB), :]


def wedge(i):
    return i, CW - 2 * i, sum(CW - 2 * k for k in range(1, i))


def cut_wedges(ext, h, low, high):
    for i in range(1, DEPTH + 1):
        c, n, at = wedge(i)
        low[h, pl.ds(at, n), :] = ext[h, i - 1, pl.ds(c, n), :]
        high[h, pl.ds(at, n), :] = ext[h, NB - i, pl.ds(c, n), :]


def mass_kernel(mo, gme, gmo, vyl, vyh, mx, kye, kyo, gml, gmh, kyl, kyh):
    order("massx", gml, gmh, gme, gmo)
    spread_x(mo, gml, gmh, mx)
    for h in range(HALVES):
        cut_wedges(mx, h, kyl, kyh)
        for k, v in ((kyl, vyl), (kyh, vyh)):
            k[h, pl.ds(KY, 2 * T), :] = v[h]
    order("massy", kye, kyo, kyl, kyh)


def bulk_kernel(u1p, b, ld, m, u2p, part):
    clear_border(u2p)
    for h in range(HALVES):

        def sweep(y, c, near, h=h):
            u2p[h, y + 1, mid(), :] = 0.2 * c + b[h, y] * (ld[h, y] + near)

        carried(h, 0, T, u1p, sweep)
    for h in range(HALVES):

        def sums(y, c, h=h):
            above, here = c
            total = None
            for k in range(R):
                r = R * y + k
                below = u2p[h, r + 2, mid(), :]
                near = (above + below) + (u2p[h, r + 1, left(), :] + u2p[h, r + 1, right(), :])
                d = (ld[h, r] + near) - (4.0 + m[h, r]) * here
                total = d if total is None else total + d
                above, here = here, below
            part[pl.ds(pl.multiple_of((h * NB + y) * T, T), T), :] = total
            return above, here

        lax.fori_loop(0, NB, sums, (u2p[h, 0, mid(), :], u2p[h, 1, mid(), :]))


def defect_rows(h, y, u2p, ld, m, part):
    total = None
    for k in range(R):
        c = R * y + k
        d = (ld[h, c] + around(u2p, h, c)) - (4.0 + m[h, c]) * u2p[h, c + 1, mid(), :]
        total = d if total is None else total + d
    part[pl.ds(pl.multiple_of((h * NB + y) * T, T), T), :] = total


def near_tile(ref, h, y, x):
    return (ref[h, pl.ds(y, 8), pl.ds(x + 8, 8), :] + ref[h, pl.ds(y + 2, 8), pl.ds(x + 8, 8), :]) + (
        ref[h, pl.ds(y + 1, 8), pl.ds(x + 7, 8), :] + ref[h, pl.ds(y + 1, 8), pl.ds(x + 9, 8), :]
    )


def second_kernel(
    u1p_in, u2p_in, part_in, b, ld, m, pxl, pxh, pyl, pyh, hxe, hxo, hye, hyo,
    u1p, u2p, part, lp, own, qxl, qxh, qxe, qxo, vxe, vxo, vyl, vyh, hxl, hxh, hyl, hyh,
    vxl, vxh,
):
    del u1p_in, u2p_in, part_in
    order("r1x", hxl, hxh, hxe, hxo)
    order("r1y", hyl, hyh, hye, hyo)
    u1p2 = u1p.reshape(HALVES * PLANE, LANES)
    U, A, B = pl.ds(0, T), pl.ds(T, T), pl.ds(2 * T, T)
    for h in range(HALVES):
        for x, p, g in ((0, pxl, hxl), (T - 1, pxh, hxh)):
            inner = column(h, x)
            outer = column(h, -1 if x == 0 else T)
            u1p2[inner, :] = u1p2[inner, :] + p[h, B, :] * g[h, U, :]
            u1p2[outer, :] = g[h, A, :] + g[h, B, :] * p[h, U, :]
        for y, p, g in ((0, pyl, hyl), (T - 1, pyh, hyh)):
            u1p[h, y + 1, mid(), :] = u1p[h, y + 1, mid(), :] + p[h, B, :] * g[h, U, :]
            u1p[h, 0 if y == 0 else T + 1, mid(), :] = g[h, A, :] + g[h, B, :] * p[h, U, :]

    for h in range(HALVES):
        for y in (0, 1, T - 2, T - 1):
            u2p[h, y + 1, mid(), :] = 0.2 * u1p[h, y + 1, mid(), :] + b[h, y] * (ld[h, y] + around(u1p, h, y))

    def sweep(j, c):
        y = pl.multiple_of(j * 8, 8)
        for h in range(HALVES):
            for x in (0, T - 8):
                here = (h, pl.ds(y + 1, 8), pl.ds(8 + x, 8))
                tile = (h, pl.ds(y, 8), pl.ds(x, 8))
                u2p[here] = 0.2 * u1p[here] + b[tile] * (ld[tile] + near_tile(u1p, h, y, x))
        return c

    lax.fori_loop(0, T // 8, sweep, 0)

    def sums(j, c):
        y = pl.multiple_of(j * 8, 8)
        for h in range(HALVES):
            for x in (0, T - 8):
                here = (h, pl.ds(y + 1, 8), pl.ds(8 + x, 8))
                tile = (h, pl.ds(y, 8), pl.ds(x, 8))
                d = (ld[tile] + near_tile(u2p, h, y, x)) - (4.0 + m[tile]) * u2p[here]
                for k in range(2):
                    at = pl.multiple_of((h * NB + 2 * j + k) * T, T) + x
                    part[pl.ds(at, 8), :] = (d[R * k] + d[R * k + 1]) + (d[R * k + 2] + d[R * k + 3])
        return c

    lax.fori_loop(0, T // 8, sums, 0)
    for h in range(HALVES):
        for y in (0, NB - 1):
            defect_rows(h, y, u2p, ld, m, part)
    block_sums(part, lp)

    u2p2, ld2 = u2p.reshape(HALVES * PLANE, LANES), ld.reshape(HALVES * T * T, LANES)
    for h in range(HALVES):
        for x, first, s, q, v in ((0, 0, 0, qxl, vxl), (T - 1, NB - DEPTH, 8, qxh, vxh)):
            for k in range(DEPTH):
                q[h, pl.ds(k * NB, NB), :] = lp[rows(h * NB * NB + first + k, NB, NB), :]
            for i, y in enumerate((0, T - 1)):
                total = None
                for k in range(R):
                    e = u2p2[rows(h * PLANE + (y + 1) * PC + 8 + R * s + k, 8, R), :]
                    total = e if total is None else total + e
                q[h, pl.ds(QX_S + 8 * i, 8), :] = total
                own[h, i, pl.ds(s, 8), :] = total
                free = QX_S + 8 * i + (7 if x == 0 else 0)
                q[h, pl.ds(free, 1), :] = u2p[h, y + 1, pl.ds(8 + x, 1), :]
            total = None
            for k in range(R):
                e = u2p2[rows(h * PLANE + (k + 1) * PC + 8 + x, NB, R * PC), :]
                total = e if total is None else total + e
            q[h, pl.ds(QX_Q, NB), :] = total * (1.0 / R)
            v[h, pl.ds(0, T), :] = u2p2[column(h, x), :]
            v[h, pl.ds(T, T), :] = ld2[rows(h * T * T + x, T, T), :] + u2p2[column(h, 1 if x == 0 else T - 2), :]
        for y, inside, v in ((0, 1, vyl), (T - 1, T - 2, vyh)):
            v[h, pl.ds(0, T), :] = u2p[h, y + 1, mid(), :]
            v[h, pl.ds(T, T), :] = ld[h, y] + u2p[h, inside + 1, mid(), :]
    order("r2x", qxe, qxo, qxl, qxh)
    order("u2x", vxe, vxo, vxl, vxh)


def third_kernel(lp, own, qxl, qxh, gxe, gxo, hxl, hxh, lx, s0, s1, qye, qyo, gxl, gxh, qyl, qyh):
    order("r2x", gxl, gxh, gxe, gxo)
    lx2 = lx.reshape(HALVES * NB * CW, LANES)
    spread_x(lp, gxl, gxh, lx)
    for h in range(HALVES):
        for c, ref in ((8, gxl), (7, qxl), (7 + NB, gxh), (8 + NB, qxh)):
            col = rows(h * NB * CW + c, NB, CW)
            lx2[col, :] = lx2[col, :] + ref[h, pl.ds(QX_Q, NB), :]
        for i, s in enumerate((s0, s1)):
            for c, ref in ((0, gxl), (24, gxh)):
                s[h, pl.ds(c, 8), :] = ref[h, pl.ds(QX_S + 8 * i, 8), :]
            s[h, pl.ds(8, NB), :] = own[h, i]
        cut_wedges(lx, h, qyl, qyh)
        for i, s, q in ((0, s0, qyl), (1, s1, qyh)):
            y = i * (T - 1)
            q[h, pl.ds(QY_S, CW), :] = s[h]
            for j, (g1, g2) in enumerate(((hxl, gxl), (hxh, gxh))):
                q[h, pl.ds(QY_DIAG + 3 * j, 1), :] = g1[h, pl.ds(y, 1), :]
                q[h, pl.ds(QY_DIAG + 3 * j + 1, 1), :] = g1[h, pl.ds(2 * T + y, 1), :]
                q[h, pl.ds(QY_DIAG + 3 * j + 2, 1), :] = g2[h, pl.ds(QX_S + 8 * i + 7 * j, 1), :]
            q[h, pl.ds(QY_DIAG + 6, 2), :] = jnp.zeros((2, LANES), F)
    order("r2y", qye, qyo, qyl, qyh)


def rate_kernel(mx, gke, gko, bc, vyl, vyh, gkl, gkh):
    order("massy", gkl, gkh, gke, gko)
    for h in range(HALVES):
        for k, v in ((gkl, vyl), (gkh, vyh)):
            v[h] = k[h, pl.ds(KY, 2 * T), :]
        for i in range(1, DEPTH + 1):
            c, n, at = wedge(i)
            for r, gk in ((DEPTH - i, gkl), (DEPTH + NB - 1 + i, gkh)):
                bc[h, r, pl.ds(c, n), :] = 0.8 / (4.0 + gk[h, pl.ds(at, n), :])
        for y in range(NB):
            bc[h, DEPTH + y] = 0.8 / (4.0 + mx[h, y])


def coarse_kernel(
    lx, bc, s0, s1, gye, gyo, hxl, hxh, hyl, hyh, pxl, pxh, b, w1_in,
    w1, sp, bumps, gyl, gyh, lg, ca, cb, cv,
):
    del w1_in
    order("r2y", gyl, gyh, gye, gyo)
    one = lambda r: pl.ds(r, 1)
    for h in range(HALVES):
        for i in range(1, DEPTH + 1):
            c, n, at = wedge(i)
            for r, g in ((DEPTH - i, gyl), (DEPTH + NB - 1 + i, gyh)):
                lg[h, r, pl.ds(c, n), :] = g[h, pl.ds(at, n), :]
        for y in range(NB):
            lg[h, DEPTH + y] = lx[h, y]
        quarter = 1.0 / R
        for r, v in (
            (DEPTH - 1, s0[h]),
            (DEPTH, gyl[h, pl.ds(QY_S, CW), :]),
            (DEPTH + NB - 1, gyh[h, pl.ds(QY_S, CW), :]),
            (DEPTH + NB, s1[h]),
        ):
            lg[h, r] = lg[h, r] + quarter * v

    for h in range(HALVES):
        for j, (px, hx) in enumerate(((pxl, hxl), (pxh, hxh))):
            for i, (hy, gy) in enumerate(((hyl, gyl), (hyh, gyh))):
                y, x = (0, T - 1)[i], (0, T - 1)[j]
                ua, ba = px[h, one(y), :], px[h, one(2 * T + y), :]
                ux, bx = hx[h, one(y), :], hx[h, one(2 * T + y), :]
                uy, by = hy[h, one(x), :], hy[h, one(2 * T + x), :]
                ud, bd = gy[h, one(QY_DIAG + 3 * j), :], gy[h, one(QY_DIAG + 3 * j + 1), :]
                ea, ed = ba * (bx + by) * ud, bd * (bx + by) * ua
                ex, ey = bx * (ba + bd) * uy, by * (ba + bd) * ux
                ya, yo = (DEPTH, DEPTH - 1) if i == 0 else (DEPTH + NB - 1, DEPTH + NB)
                xa, xo = (8, 7) if j == 0 else (7 + NB, 8 + NB)
                for yy, xx, e, bb, e1, e2 in (
                    (ya, xa, ea, ba, ex, ey),
                    (ya, xo, ex, bx, ea, ed),
                    (yo, xa, ey, by, ea, ed),
                    (yo, xo, ed, bd, ex, ey),
                ):
                    lg[h, yy, one(xx), :] = lg[h, yy, one(xx), :] + quarter * (
                        (2.0 - 0.8 / bb) * e + (e1 + e2)
                    )
                at = 4 * (2 * i + j)
                for k, e in enumerate((ea, ex, ey, ed + gy[h, one(QY_DIAG + 3 * j + 2), :])):
                    bumps[h, one(at + k), :] = e

    own = pl.ds(8, CW)

    def start(h, y):
        v = bc[h, y] * lg[h, y]
        lg[h, y] = v
        ca[h, y, own, :] = v

    each_row(start, CR, unroll=6)
    old, new = ca, cb
    for s in range(1, INNER):

        def inner(y, c, old=old, new=new, end=s == INNER - 1):
            kept = []
            for h in range(HALVES):
                above, here = c[h]
                below = old[h, y + 1, own, :]
                near = (above + below) + (old[h, y, pl.ds(7, CW), :] + old[h, y, pl.ds(9, CW), :])
                value = (0.2 * here + lg[h, y]) + bc[h, y] * near
                if end:
                    cv[h, y] = value
                else:
                    new[h, y, own, :] = value
                kept.append((here, below))
            return tuple(kept)

        lax.fori_loop(
            s, CR - s, inner, tuple((old[h, s - 1, own, :], old[h, s, own, :]) for h in range(HALVES)), unroll=2
        )
        old, new = new, old

    for h in range(HALVES):
        for y in range(NB + 2):
            c = cv[h, y + DEPTH - 1, pl.ds(6, NB + 4), :]
            for k in range(R):
                sp[h, y, rows(k, NB + 4, R), :] = c

    def correct(h, y):
        c = sp[h, y + 1, mid(), :]
        sides = sp[h, y + 1, left(), :] + sp[h, y + 1, right(), :]
        above, below = sp[h, y, mid(), :], sp[h, y + 2, mid(), :]
        base = 0.2 * c
        inside = sides + (c + c)
        for k, near in ((0, sides + (c + above)), (1, inside), (2, inside), (3, sides + (c + below))):
            r = R * y + k
            w1[h, r + 1, mid(), :] = w1[h, r + 1, mid(), :] + (base + b[h, r] * near)

    each_row(correct, NB, unroll=2)


def ahead_kernel(u2p, b, ld, w1):
    for h in range(HALVES):

        def sweep(y, c, near, h=h):
            w1[h, y + 1, mid(), :] = 0.2 * c + b[h, y] * (ld[h, y] + near)

        carried(h, 0, T, u2p, sweep)


def ring(n, h, v, bh, c, wh, oh, ends, corners, here, to):
    one = lambda r: pl.ds(r, 1)
    wh[n, mid(), :] = v[h, pl.ds(0, T), :]
    for r, (outside, inside) in zip((0, T - 1), ends):
        wh[n, one(8 + r), :] = wh[n, one(8 + r), :] + outside
        oh[n, one(r), :] = oh[n, one(r), :] + inside
    u2h = wh[n, mid(), :]
    w0h = u2h + c
    wh[n, mid(), :] = w0h
    wh[n, one(7), :], wh[n, one(8 + T), :] = corners
    near = (wh[n, left(), :] + wh[n, right(), :]) + oh[n]
    here(u2h)
    to(0.2 * w0h + bh * ((v[h, pl.ds(T, T), :] + c) + near))


def corner_values(bumps, sp, h):
    bump = lambda i, j, k: bumps[h, pl.ds(4 * (2 * i + j) + k, 1), :]
    diag = {
        (i, j): bump(i, j, 3) + sp[h, (0, NB + 1)[i], pl.ds((7, 8 + T)[j], 1), :] for i in range(2) for j in range(2)
    }
    return bump, diag


INNER_X = T - 16


def inner_kernel(w1_in, sp, bumps, vyl, vyh, hyl, hyh, u2p, b, ld, w1, w0, wh, oh):
    del w1_in
    one = lambda r: pl.ds(r, 1)
    n = 0
    for h in range(HALVES):
        bump, diag = corner_values(bumps, sp, h)
        for i in range(2):
            for j in range(2):
                e, y, x = bump(i, j, 0), (0, T - 1)[i], (0, T - 1)[j]
                yi, xi = (1, T - 2)[i], (1, T - 2)[j]
                for yy, xx, f in ((y, x, None), (y, xi, b), (yi, x, b)):
                    f = 0.2 if f is None else b[h, yy, one(xx), :]
                    w1[h, yy + 1, one(xx + 8), :] = w1[h, yy + 1, one(xx + 8), :] + f * e
        for i, (v, hy) in enumerate(((vyl, hyl), (vyh, hyh))):
            y = (0, T - 1)[i]
            oh[n] = u2p[h, y + 1, mid(), :] + sp[h, (1, NB)[i], mid(), :]

            def here(u2h, h=h, y=y):
                w1[h, y + 1, mid(), :] = w1[h, y + 1, mid(), :] + b[h, y] * u2h

            def to(value, h=h, i=i):
                w1[h, (0, T + 1)[i], mid(), :] = value

            ring(
                n, h, v, hy[h, pl.ds(2 * T, T), :], sp[h, (0, NB + 1)[i], mid(), :], wh, oh,
                [(bump(i, j, 2), bump(i, j, 0)) for j in range(2)], (diag[i, 0], diag[i, 1]), here, to,
            )
            n += 1

        def last(y, c, near, h=h):
            w0[h, y] = 0.2 * c + b[h, y, pl.ds(8, INNER_X), :] * (ld[h, y, pl.ds(8, INNER_X), :] + near)

        carried(h, 0, T, w1, last, 8, INNER_X, unroll=4)


def last_kernel(w1_in, middle, sp, bumps, vxe, vxo, hxl, hxh, u2p, b, ld, w1, out, vxl, vxh, w0, wh, sh, oh, sems):
    del w1_in
    copies = [
        pltpu.make_async_copy(
            middle.at[h], out.at[:, pl.ds(8, INNER_X), pl.ds(h * LANES, LANES)], sems.at[h, 2]
        )
        for h in range(HALVES)
    ]
    for c in copies:
        c.start()
    order("u2x", vxl, vxh, vxe, vxo)
    stride = (NB + 2) * PC
    sp2, b2 = sp.reshape(HALVES * stride, LANES), b.reshape(HALVES * T * T, LANES)
    w12, u2p2 = w1.reshape(HALVES * PLANE, LANES), u2p.reshape(HALVES * PLANE, LANES)
    n = 0
    for h in range(HALVES):
        bump, diag = corner_values(bumps, sp, h)
        for j, (v, hx) in enumerate(((vxl, hxl), (vxh, hxh))):
            x, xo = (0, T - 1)[j], (-1, T)[j]
            for k in range(R):
                sh[n, 0, rows(k, NB, R), :] = sp2[rows(h * stride + PC + 8 + xo, NB, PC), :]
                sh[n, 1, rows(k, NB, R), :] = sp2[rows(h * stride + PC + 8 + x, NB, PC), :]
            oh[n] = u2p2[column(h, x), :] + sh[n, 1]

            def here(u2h, h=h, x=x):
                at = column(h, x)
                w12[at, :] = w12[at, :] + b2[rows(h * T * T + x, T, T), :] * u2h

            def to(value, h=h, xo=xo):
                w12[column(h, xo), :] = value

            ring(
                n, h, v, hx[h, pl.ds(2 * T, T), :], sh[n, 0], wh, oh,
                [(bump(i, j, 1), bump(i, j, 0)) for i in range(2)], (diag[0, j], diag[1, j]), here, to,
            )
            n += 1

        for j, x in enumerate((0, T - 8)):

            def sweep(k, c, h=h, j=j, x=x):
                y = pl.multiple_of(k * 8, 8)
                tile = (h, pl.ds(y, 8), pl.ds(x, 8))
                near = near_tile(w1, h, y, x)
                w0[h, j, pl.ds(y, 8)] = 0.2 * w1[h, pl.ds(y + 1, 8), pl.ds(8 + x, 8)] + b[tile] * (ld[tile] + near)
                return c

            lax.fori_loop(0, T // 8, sweep, 0, unroll=2)
            copies.append(
                pltpu.make_async_copy(
                    w0.at[h, j], out.at[:, pl.ds(x, 8), pl.ds(h * LANES, LANES)], sems.at[h, j]
                )
            )
            copies[-1].start()
    for c in copies:
        c.wait()


def vmem(*shape):
    return pltpu.VMEM(shape, F)


V = pl.BlockSpec(memory_space=pltpu.VMEM)
H = pl.BlockSpec(memory_space=pltpu.HBM)


def exchange(name, even, odd):
    axis = AXIS[name]
    size = lax.axis_size(axis)
    up = [(i, (i + 1) % size) for i in range(size)]
    if name not in SWAPPED:
        return lax.ppermute(odd, axis, up), lax.ppermute(even, axis, [(b, a) for a, b in up])
    pairs = [[p for a, b in up[k::2] for p in ((a, b), (b, a))] for k in range(2)]
    return lax.ppermute(even, axis, pairs[0]), lax.ppermute(odd, axis, pairs[1])


def estimate(flops, size):
    return pl.CostEstimate(flops=flops, bytes_accessed=size, transcendentals=0)


def per_device(load_terms, start_values, reaction_rate):
    tile, padded = (HALVES, T, T, LANES), (HALVES, PR, PC, LANES)
    coarse = (HALVES * NB * NB, LANES)
    edge = (HALVES, 3 * T, LANES)
    part = vmem(HALVES * NB * T, LANES)
    inputs = tuple(
        pltpu.with_memory_space_constraint(v, pltpu.HBM) for v in (load_terms, start_values, reaction_rate)
    )
    strip, line = vmem(HALVES, 2, T, 8, LANES), vmem(HALVES, 2, 1, T, LANES)
    pyl, pyh, pye, pyo = pl.pallas_call(
        row_edges,
        in_specs=[H] * 3,
        out_specs=[V] * 4,
        out_shape=[vmem(*edge)] * 4,
        scratch_shapes=[vmem(HALVES, 2, 2, PC, LANES), line, line, pltpu.SemaphoreType.DMA((HALVES, 2, 3))],
        compiler_params=pltpu.CompilerParams(vmem_limit_bytes=4 * MIB),
        name="rowedges",
    )(*inputs)
    hye, hyo = exchange("r1y", pye, pyo)
    pxl, pxh, pxe, pxo = pl.pallas_call(
        column_edges,
        in_specs=[H] * 3,
        out_specs=[V] * 4,
        out_shape=[vmem(*edge)] * 4,
        scratch_shapes=[vmem(HALVES, 2, T + 2, 8, LANES), strip, strip, pltpu.SemaphoreType.DMA((HALVES, 2, 3))],
        compiler_params=pltpu.CompilerParams(vmem_limit_bytes=8 * MIB),
        name="columnedges",
    )(*inputs)
    hxe, hxo = exchange("r1x", pxe, pxo)
    u1p, b, ld, m, mo, kxe, kxo = pl.pallas_call(
        first_kernel,
        in_specs=[H] * 3,
        out_specs=[V] * 7,
        out_shape=[vmem(*padded)] + [vmem(*tile)] * 3 + [vmem(*coarse)] + [vmem(HALVES, KX, LANES)] * 2,
        scratch_shapes=[vmem(*padded), part]
        + [vmem(HALVES, KX, LANES)] * 2
        + [pltpu.SemaphoreType.DMA((3, HALVES, CHUNKS))],
        compiler_params=pltpu.CompilerParams(vmem_limit_bytes=12 * MIB),
        cost_estimate=estimate(10**7, 12 * MIB),
        name="first",
    )(*inputs)
    gme, gmo = exchange("massx", kxe, kxo)
    outer = vmem(HALVES, 2 * T, LANES)
    u2p, part_sums = pl.pallas_call(
        bulk_kernel,
        in_specs=[V] * 4,
        out_specs=[V] * 2,
        out_shape=[vmem(*padded), part],
        compiler_params=pltpu.CompilerParams(vmem_limit_bytes=4 * MIB),
        cost_estimate=estimate(10**7, 12 * MIB),
        name="bulk",
    )(u1p, b, ld, m)
    _, u2p, _, lp, own, qxl, qxh, qxe, qxo, vxe, vxo, vyl, vyh, hxl, hxh, hyl, hyh = pl.pallas_call(
        second_kernel,
        in_specs=[V] * 14,
        out_specs=[V] * 17,
        out_shape=[vmem(*padded)] * 2
        + [part, vmem(*coarse), vmem(HALVES, 2, NB, LANES)]
        + [vmem(HALVES, QX, LANES)] * 4
        + [outer] * 4
        + [vmem(*edge)] * 4,
        scratch_shapes=[outer] * 2,
        input_output_aliases={0: 0, 1: 1, 2: 2},
        compiler_params=pltpu.CompilerParams(vmem_limit_bytes=8 * MIB),
        name="second",
    )(u1p, u2p, part_sums, b, ld, m, pxl, pxh, pyl, pyh, hxe, hxo, hye, hyo)
    gxe, gxo = exchange("r2x", qxe, qxo)
    vxe, vxo = exchange("u2x", vxe, vxo)
    mx, kye, kyo = pl.pallas_call(
        mass_kernel,
        in_specs=[V] * 5,
        out_specs=[V] * 3,
        out_shape=[vmem(HALVES, NB, CW, LANES)] + [vmem(HALVES, KY + 2 * T, LANES)] * 2,
        scratch_shapes=[vmem(HALVES, KX, LANES)] * 2 + [vmem(HALVES, KY + 2 * T, LANES)] * 2,
        compiler_params=pltpu.CompilerParams(vmem_limit_bytes=8 * MIB),
        name="mass",
    )(mo, gme, gmo, vyl, vyh)
    gke, gko = exchange("massy", kye, kyo)
    lx, s0, s1, qye, qyo = pl.pallas_call(
        third_kernel,
        in_specs=[V] * 8,
        out_specs=[V] * 5,
        out_shape=[vmem(HALVES, NB, CW, LANES)]
        + [vmem(HALVES, CW, LANES)] * 2
        + [vmem(HALVES, QY, LANES)] * 2,
        scratch_shapes=[vmem(HALVES, QX, LANES)] * 2 + [vmem(HALVES, QY, LANES)] * 2,
        compiler_params=pltpu.CompilerParams(vmem_limit_bytes=8 * MIB),
        name="third",
    )(lp, own, qxl, qxh, gxe, gxo, hxl, hxh)
    gye, gyo = exchange("r2y", qye, qyo)
    grid = vmem(HALVES, CR, CW, LANES)
    bc, vyl, vyh = pl.pallas_call(
        rate_kernel,
        in_specs=[V] * 3,
        out_specs=[V] * 3,
        out_shape=[grid, outer, outer],
        scratch_shapes=[vmem(HALVES, KY + 2 * T, LANES)] * 2,
        compiler_params=pltpu.CompilerParams(vmem_limit_bytes=8 * MIB),
        name="rate",
    )(mx, gke, gko)
    wide = vmem(HALVES, CR, CW + 16, LANES)
    u3 = pl.pallas_call(
        ahead_kernel,
        in_specs=[V] * 3,
        out_specs=V,
        out_shape=vmem(*padded),
        compiler_params=pltpu.CompilerParams(vmem_limit_bytes=4 * MIB),
        name="ahead",
    )(u2p, b, ld)
    w1, sp, bumps = pl.pallas_call(
        coarse_kernel,
        in_specs=[V] * 14,
        out_specs=[V] * 3,
        out_shape=[vmem(*padded), vmem(HALVES, NB + 2, PC, LANES), vmem(HALVES, 16, LANES)],
        scratch_shapes=[vmem(HALVES, QY, LANES)] * 2 + [grid, wide, wide, grid],
        input_output_aliases={13: 0},
        compiler_params=pltpu.CompilerParams(vmem_limit_bytes=8 * MIB),
        cost_estimate=estimate(10**7, 4 * MIB),
        name="coarse",
    )(lx, bc, s0, s1, gye, gyo, hxl, hxh, hyl, hyh, pxl, pxh, b, u3)
    result = jax.ShapeDtypeStruct(load_terms.shape, F)
    sides = [vmem(4, PC, LANES), vmem(4, T, LANES)]
    w1, middle = pl.pallas_call(
        inner_kernel,
        in_specs=[V] * 10,
        out_specs=[V, V],
        out_shape=[vmem(*padded), vmem(HALVES, T, INNER_X, LANES)],
        scratch_shapes=sides,
        input_output_aliases={0: 0},
        compiler_params=pltpu.CompilerParams(vmem_limit_bytes=12 * MIB),
        cost_estimate=estimate(10**7, 4 * MIB),
        name="inner",
    )(w1, sp, bumps, vyl, vyh, hyl, hyh, u2p, b, ld)
    _, corrected = pl.pallas_call(
        last_kernel,
        in_specs=[V] * 11,
        out_specs=[V, H],
        out_shape=[vmem(*padded), result],
        scratch_shapes=[outer] * 2
        + [vmem(HALVES, 2, T, 8, LANES), sides[0], vmem(4, 2, T, LANES), sides[1]]
        + [pltpu.SemaphoreType.DMA((HALVES, 3))],
        input_output_aliases={0: 0},
        compiler_params=pltpu.CompilerParams(vmem_limit_bytes=12 * MIB),
        name="last",
    )(w1, middle, sp, bumps, vxe, vxo, hxl, hxh, u2p, b, ld)
    return corrected


def solution(mesh):
    return jax.shard_map(
        per_device,
        mesh=mesh,
        in_specs=(P("py", "px", None), P("py", "px", None), P("py", "px", None)),
        out_specs=P("py", "px", None),
        check_vma=False,
    )
```
